32 devices in a mesh: row: 4 (over y, x), col: 4 (over z), head: 2 (over core).
Axes of the slice: x: 2, y: 2, z: 4, core: 2. Of those that a mesh axis runs over, the one named last changes fastest.
Arguments:
- queries: bfloat16 [256, 64, 256], P('row', 'col'), may hold values from -1000 to 1000
- level_zero: bfloat16 [256, 64, 256], P('row', 'col', 'head'), may hold values from -6 to 6
- level_one: bfloat16 [128, 32, 256], P('row', 'col', 'head'), may hold values from -6 to 6
- level_two: bfloat16 [64, 16, 256], P('row', 'col', 'head'), may hold values from -6 to 6
- level_three: bfloat16 [32, 8, 256], P('row', 'col', 'head'), may hold values from -6 to 6
- tile_lists: int32 [16, 4, 4, 8], P('row', 'col'), may hold values from 0 to 63, as said below
- samples: int32 [256, 64, 128], P('row', 'col', 'head'), may hold values from 0 to 133168895, as said below
- logit_weight: bfloat16 [256, 128], P(None, 'head'), may hold values from -1 to 1
- logit_bias: float32 [128], P('head'), may hold values from -3 to 3
- output_weight: bfloat16 [256, 256], replicated, may hold values from -0.375 to 0.375
- output_bias: float32 [256], replicated, may hold values from -3 to 3
- norm_gain: float32 [256], P('head'), may hold values from 0.5 to 1.5
- norm_shift: float32 [256], P('head'), may hold values from -3 to 3
Outputs:
- updated_queries: bfloat16 [256, 64, 256], P('row', 'col', 'head')
The draws below stay inside these ranges and needn't reach their ends.
Inputs may be any that keep to these rules, and one draw needn't show every extreme that they name: `tile_lists`: entries are tile numbers r * 4 + c. Over all lists of the query blocks that one device holds, at one level, at most 2 entries name tiles that one device holds; at each level some device is named exactly 2 times by the lists of every device. A tile may be listed more than once. `samples`: slot is below 8; at level l, pos_row and pos_col are below (16 / 2^l - 1) * 256.
All inputs are finite; a program needn't handle non-finite values.
Results may differ from the reference program's by a relative error of at most 0.004.
Values may be sent and summed in bfloat16 or wider, within the bound.
No kernel may reach another device: no remote copies, remote signals or barrier semaphores. Data moves between devices by JAX's collectives and lax.ppermute only.
A program may use at most 128 MiB of HBM per device.

```python
import math
import jax
import jax.numpy as jnp
from jax import lax

D = 256
HEADS = 8
LEVELS = 4
POINTS = 4
TILE = 16
K = 8
TR = 4
TC = 1
ROWS = 256
COLS = 64
N_ROW = 4
N_COL = 4


def attend_columns(key):
    raw_draw = jax.random.normal(jax.random.fold_in(key, 701), (D, HEADS * LEVELS * POINTS), jnp.float32)
    return (jnp.clip(raw_draw, -5.0, 5.0) / math.sqrt(D)).astype(jnp.bfloat16)


def draw_logit_weight(key, part):
    return attend_columns(key)


def draw_queries(key, part):
    height = TR * TILE * N_ROW
    width_all = TC * TILE * N_COL
    base_draw = jax.random.normal(jax.random.fold_in(key, 1), (height, width_all, D), jnp.float32)
    base_draw = jnp.clip(base_draw, -6.0, 6.0)
    return base_draw.astype(jnp.bfloat16)


def draw_samples(key, part):
    height = TR * TILE * N_ROW
    width_all = TC * TILE * N_COL
    lane_count = HEADS * LEVELS * POINTS
    lane_level = jnp.arange(lane_count, dtype=jnp.int32) // POINTS % LEVELS
    pos_limit = (TILE // jnp.left_shift(jnp.int32(1), lane_level) - 1) * 256
    full_shape = (height, width_all, lane_count)
    slot_draw = jax.random.randint(jax.random.fold_in(key, 21), full_shape, 0, K)
    row_draw = jax.random.randint(jax.random.fold_in(key, 22), full_shape, 0, jnp.broadcast_to(pos_limit, full_shape))
    col_draw = jax.random.randint(jax.random.fold_in(key, 23), full_shape, 0, jnp.broadcast_to(pos_limit, full_shape))
    return (slot_draw * 16777216 + row_draw * 4096 + col_draw).astype(jnp.int32)


def draw_tile_lists(key, part):
    peer_count = N_ROW * N_COL
    local_tiles = TR * TC
    requests = local_tiles * K
    capacity = max(2, (requests + peer_count - 1) // peer_count)
    slot_count = peer_count * capacity
    hot_owner = jax.random.randint(jax.random.fold_in(key, 31), (LEVELS,), 0, peer_count)

    def one_list(device_num, level_num):
        sub_key = jax.random.fold_in(jax.random.fold_in(key, 32), device_num * LEVELS + level_num)
        scores = jax.random.permutation(jax.random.fold_in(sub_key, 1), slot_count).astype(jnp.int32)
        forced = jnp.arange(slot_count, dtype=jnp.int32) // capacity == hot_owner[level_num]
        scores = jnp.where(forced, -1, scores)
        ranking = jnp.argsort(scores, stable=True)
        chosen = ranking[:requests]
        chosen = chosen[jax.random.permutation(jax.random.fold_in(sub_key, 2), requests)]
        owner_dev = chosen.astype(jnp.int32) // capacity
        local_index = jax.random.randint(jax.random.fold_in(sub_key, 3), (requests,), 0, local_tiles)
        tile_row = owner_dev // N_COL * TR + local_index // TC
        tile_col = owner_dev % N_COL * TC + local_index % TC
        return (tile_row * (TC * N_COL) + tile_col).astype(jnp.int32)
    device_grid = jnp.arange(peer_count, dtype=jnp.int32)
    level_grid = jnp.arange(LEVELS, dtype=jnp.int32)
    tile_ids = jax.vmap(lambda device_num: jax.vmap(lambda level_num: one_list(device_num, level_num))(level_grid))(device_grid)
    tile_ids = tile_ids.reshape(N_ROW, N_COL, LEVELS, TR, TC, K)
    return tile_ids.transpose(0, 3, 1, 4, 2, 5).reshape(TR * N_ROW, TC * N_COL, LEVELS, K)


def levels(rng, dims, split, least, largest):
    gain = 1.0
    for position, shards_of in split:
        heights = jax.random.uniform(jax.random.fold_in(jax.random.fold_in(rng, 6), position), (shards_of,), jnp.float32, least / len(split), largest / len(split))
        gain = gain * jnp.repeat(jnp.exp(heights), dims[position] // shards_of).reshape((-1,) + (1,) * (len(dims) - 1 - position))
    return gain


def scatter_about(key, shape, deviation, most, cuts=(), kind=jnp.bfloat16):
    values = jax.random.normal(key, shape, jnp.float32) * deviation
    if len(cuts) > 0:
        values = levels(key, shape, cuts, -0.22, 0.18) * values
    return jnp.clip(values, min=-most, max=most).astype(kind)


def setup_inputs(seed: int = 0) -> dict:
    key_list = jax.random.split(jax.random.key(seed), 14)
    queries = draw_queries(jax.random.fold_in(key_list[13], 71), 0)
    level_zero = scatter_about(key_list[1], (ROWS, COLS, D), 1.0, 6.0, ((0, 4), (1, 4), (2, 2)))
    level_one = scatter_about(key_list[2], (ROWS // 2, COLS // 2, D), 1.0, 6.0, ((0, 4), (1, 4), (2, 2)))
    level_two = scatter_about(key_list[3], (ROWS // 4, COLS // 4, D), 1.0, 6.0, ((0, 4), (1, 4), (2, 2)))
    level_three = scatter_about(key_list[4], (ROWS // 8, COLS // 8, D), 1.0, 6.0, ((0, 4), (1, 4), (2, 2)))
    tile_lists = draw_tile_lists(jax.random.fold_in(key_list[13], 71), 0)
    samples = draw_samples(jax.random.fold_in(key_list[13], 71), 0)
    logit_weight = draw_logit_weight(jax.random.fold_in(key_list[13], 71), 0)
    logit_bias = scatter_about(key_list[8], (HEADS * LEVELS * POINTS,), 0.5, 3.0, ((0, 2),), jnp.float32)
    output_weight = scatter_about(key_list[9], (D, D), D ** -0.5, 0.375)
    output_bias = scatter_about(key_list[10], (D,), 0.5, 3.0, (), jnp.float32)
    norm_gain = jnp.clip(1.0 + 0.1 * jax.random.normal(key_list[11], (D,), jnp.float32), 0.5, 1.5)
    norm_shift = scatter_about(key_list[12], (D,), 0.5, 3.0, ((0, 2),), jnp.float32)
    return dict(queries=queries, level_zero=level_zero, level_one=level_one, level_two=level_two, level_three=level_three, tile_lists=tile_lists, samples=samples, logit_weight=logit_weight, logit_bias=logit_bias, output_weight=output_weight, output_bias=output_bias, norm_gain=norm_gain, norm_shift=norm_shift)


def to_blocks(source, grid_rows, grid_cols, tile_side):
    channels = source.shape[2]
    shaped = source.reshape(grid_rows, tile_side, grid_cols, tile_side, channels)
    return shaped.transpose(0, 2, 1, 3, 4).reshape(grid_rows * grid_cols, tile_side * tile_side, channels)

def reference(queries, level_zero, level_one, level_two, level_three, tile_lists, samples, logit_weight, logit_bias, output_weight, output_bias, norm_gain, norm_shift):
    grid_rows = tile_lists.shape[0]
    grid_cols = tile_lists.shape[1]
    head_dim = D // HEADS
    pixels = TILE * TILE
    hits = POINTS * 4
    tile_sets = []
    for level_num, level_array in enumerate((level_zero, level_one, level_two, level_three)):
        tile_side = TILE // 2 ** level_num
        blocks_here = to_blocks(level_array, grid_rows, grid_cols, tile_side)
        tile_sets.append(blocks_here.reshape(grid_rows * grid_cols, tile_side * tile_side, HEADS, head_dim))
    query_blocks = to_blocks(queries, grid_rows, grid_cols, TILE)
    sample_blocks = to_blocks(samples, grid_rows, grid_cols, TILE)
    list_blocks = tile_lists.reshape(grid_rows * grid_cols, LEVELS, K)
    earlier = jnp.arange(hits, dtype=jnp.int32)[None, :] < jnp.arange(hits, dtype=jnp.int32)[:, None]

    def one_block(operands):
        query_blk, sample_blk, list_blk = operands
        logits = jnp.dot(query_blk, logit_weight, preferred_element_type=jnp.float32) + logit_bias
        attend = jax.nn.softmax(logits.reshape(pixels, HEADS, LEVELS * POINTS), axis=-1)
        attend = attend.reshape(pixels, HEADS, LEVELS, POINTS)
        packed = sample_blk.reshape(pixels, HEADS, LEVELS, POINTS)
        slot_index = packed // 16777216
        pos_row = packed // 4096 % 4096
        pos_col = packed % 4096
        frac_row = (pos_row % 256).astype(jnp.float32) / 256.0
        frac_col = (pos_col % 256).astype(jnp.float32) / 256.0
        running = jnp.zeros((pixels, HEADS, head_dim), jnp.float32)
        for level_num in range(LEVELS):
            tile_side = TILE // 2 ** level_num
            chosen = tile_sets[level_num][list_blk[level_num]]
            flat_values = chosen.reshape(K * tile_side * tile_side, HEADS, head_dim).transpose(1, 0, 2)
            base_index = slot_index[:, :, level_num] * tile_side * tile_side + pos_row[:, :, level_num] // 256 * tile_side + pos_col[:, :, level_num] // 256
            lvl_row = frac_row[:, :, level_num]
            lvl_col = frac_col[:, :, level_num]
            attend_lvl = attend[:, :, level_num]
            targets = jnp.stack([base_index, base_index + 1, base_index + tile_side, base_index + tile_side + 1], axis=3).reshape(pixels, HEADS, hits)
            corner_weights = jnp.stack([attend_lvl * (1.0 - lvl_row) * (1.0 - lvl_col), attend_lvl * (1.0 - lvl_row) * lvl_col, attend_lvl * lvl_row * (1.0 - lvl_col), attend_lvl * lvl_row * lvl_col], axis=3).reshape(pixels, HEADS, hits)
            same_pixel = targets[:, :, :, None] == targets[:, :, None, :]
            combined = lax.optimization_barrier(jnp.sum(jnp.where(same_pixel, corner_weights[:, :, None, :], 0.0), axis=3))
            repeated = jnp.any(same_pixel & earlier, axis=3)
            rounded = lax.optimization_barrier(combined.astype(jnp.bfloat16)).astype(jnp.float32)
            pixel_weight = jnp.where(repeated, 0.0, rounded)
            lookup = targets.transpose(1, 0, 2).reshape(HEADS, pixels * hits)
            picked = jnp.take_along_axis(flat_values, lookup[:, :, None], axis=1).astype(jnp.float32)
            picked = picked.reshape(HEADS, pixels, hits, head_dim)
            running = running + jnp.einsum('qhn,hqnd->qhd', pixel_weight, picked, precision=lax.Precision.HIGHEST)
        attn_out = running.reshape(pixels, D).astype(jnp.bfloat16)
        pre_norm = query_blk.astype(jnp.float32) + jnp.dot(attn_out, output_weight, preferred_element_type=jnp.float32) + output_bias
        row_mean = lax.optimization_barrier(jnp.mean(pre_norm, axis=1, keepdims=True))
        centered = pre_norm - row_mean
        variance = lax.optimization_barrier(jnp.mean(centered * centered, axis=1, keepdims=True))
        return (centered * lax.rsqrt(variance + 1e-05) * norm_gain + norm_shift).astype(jnp.bfloat16)
    updated = lax.map(one_block, (query_blocks, sample_blocks, list_blocks))
    updated = updated.reshape(grid_rows, grid_cols, TILE, TILE, D).transpose(0, 2, 1, 3, 4)
    return updated.reshape(grid_rows * TILE, grid_cols * TILE, D)
```

```python
import functools
import jax
import jax.numpy as jnp
from jax import lax
from jax.experimental import pallas as pl
from jax.experimental.pallas import tpu as pltpu
from jax.sharding import PartitionSpec as P

LEVELS = 4
POINTS = 4
ANY = pl.ANY
SMEM = pltpu.SMEM
VMEM = pltpu.VMEM


def to_blocks(source, tile_rows, tile_cols, tile_side):
    channels = source.shape[2]
    shaped = source.reshape(tile_rows, tile_side, tile_cols, tile_side, channels)
    return shaped.transpose(0, 2, 1, 3, 4).reshape(
        tile_rows * tile_cols, tile_side * tile_side, channels
    )


def hat(position, center):
    return jnp.maximum(1.0 - jnp.abs(position - center), 0.0)


def iota(shape, dim):
    return lax.broadcasted_iota(jnp.int32, shape, dim)


def prep_kernel(heads, query_ref, weight_ref, bias_ref, out_ref):
    logits = lax.dot_general(
        weight_ref[...], query_ref[...], (((1,), (1,)), ((), ())), preferred_element_type=jnp.float32
    )
    logits = logits + bias_ref[...]
    lanes = LEVELS * POINTS
    for head in range(heads):
        part = logits[head * lanes : (head + 1) * lanes, :]
        part = jnp.exp(part - jnp.max(part, axis=0, keepdims=True))
        out_ref[head * lanes : (head + 1) * lanes, :] = part / jnp.sum(part, axis=0, keepdims=True)


def select_kernel(dims, ids_ref, zero_ref, one_ref, two_ref, three_ref, out_ref, sem):
    peers, capacity, sizes = dims
    refs = (zero_ref, one_ref, two_ref)

    def copies(peer, make):
        base = 0
        for level in range(LEVELS - 1):
            size = sizes[level]
            for slot in range(capacity):
                index = jnp.maximum(ids_ref[peer, level * capacity + slot], 0)
                make(refs[level].at[index], out_ref.at[peer, base : base + size, :])
                base += size
        make(three_ref, out_ref.at[peer, base : base + three_ref.shape[0], :])

    def start(peer, carry):
        copies(peer, lambda src, dst: pltpu.make_async_copy(src, dst, sem).start())
        return carry

    def finish(peer, carry):
        copies(peer, lambda src, dst: pltpu.make_async_copy(src, dst, sem).wait())
        return carry

    lax.fori_loop(0, peers, start, 0)
    lax.fori_loop(0, peers, finish, 0)


def attend_kernel(
    dims,
    request_ref,
    fetched_ref,
    attend_ref,
    sample_ref,
    rowid_ref,
    out_ref,
    tile0,
    tile1,
    tile2,
    tile3,
    left0,
    left1,
    left2,
    weight0,
    weight1,
    weight2,
    code_ref,
    row_ref,
    col_ref,
    sem,
):
    peers, capacity, sizes, sides, per_block, heads, head_dim, blocks = dims
    block = pl.program_id(0)
    pixels = out_ref.shape[0]
    channels = heads * head_dim
    tiles = (tile0, tile1, tile2)
    small = tile3.shape[1]
    base3 = capacity * sum(sizes[:3])

    @pl.when(block == 0)
    def _():
        def start(peer, carry):
            base = 0
            for level in range(LEVELS - 1):
                size = sizes[level]
                for slot in range(capacity):
                    request = request_ref[peer, level * capacity + slot]

                    @pl.when(request >= 0)
                    def _(level=level, base=base, size=size, request=request):
                        here = request // per_block
                        pltpu.make_async_copy(
                            fetched_ref.at[peer, base : base + size, :],
                            tiles[level].at[here, request % per_block],
                            sem.at[level, here],
                        ).start()

                    base += size
            return carry

        pltpu.make_async_copy(
            fetched_ref.at[:, base3 : base3 + small, :], tile3, sem.at[LEVELS - 1, 0]
        ).start()
        lax.fori_loop(0, peers, start, 0)
        left0[...] = jnp.zeros_like(left0)
        weight2[...] = jnp.zeros_like(weight2)
        pltpu.make_async_copy(
            fetched_ref.at[:, base3 : base3 + small, :], tile3, sem.at[LEVELS - 1, 0]
        ).wait()
        flat = tile3[...].reshape(peers * small, channels)
        chosen = (rowid_ref[...] == iota((rowid_ref.shape[0], peers * small), 1)).astype(jnp.bfloat16)
        picked = jnp.dot(chosen, flat, preferred_element_type=jnp.float32)
        left2[:, 128:] = picked.T.astype(jnp.bfloat16)

    packed = sample_ref[...]
    level_of = iota(packed.shape, 0) // POINTS % LEVELS
    slot = packed >> 24
    pos_row = (packed >> 12) & 4095
    pos_col = packed & 4095
    half = lax.shift_right_logical(jnp.full_like(packed, sides[0] * 128), level_of)
    upper = (pos_row >= half) & (level_of < 2)
    code_ref[...] = slot + jnp.where(upper, per_block, 0)
    row_ref[...] = (pos_row - jnp.where(upper, half, 0)).astype(jnp.float32) * (1.0 / 256.0)
    col_ref[...] = pos_col.astype(jnp.float32) * (1.0 / 256.0)

    for level in range(LEVELS - 1):
        pltpu.make_async_copy(tiles[level].at[block], tiles[level].at[block], sem.at[level, block]).wait()

    side0, side1 = sides[0], sides[1]
    half0, half1 = side0 // 2, side1 // 2
    for line in range(side0):
        piece = tile0[block, :, line * side0 : (line + 1) * side0, :]
        turned = piece.reshape(per_block * side0, channels).T
        for group in range(2):
            offset = line - group * half0
            if 0 <= offset <= half0:
                for head in range(heads):
                    left0[
                        head,
                        offset * head_dim : (offset + 1) * head_dim,
                        group * per_block * side0 : (group + 1) * per_block * side0,
                    ] = turned[head * head_dim : (head + 1) * head_dim, :]
    wide1 = tile1[block].astype(jnp.float32)
    for offset in range(half1 + 1):
        first = wide1[:, offset * side1 : (offset + 1) * side1, :]
        other = min(half1 + offset, side1 - 1)
        second = wide1[:, other * side1 : (other + 1) * side1, :]
        both = jnp.concatenate(
            [first.reshape(per_block * side1, channels), second.reshape(per_block * side1, channels)], axis=0
        )
        turned = both.T.astype(jnp.bfloat16)
        for head in range(heads):
            left1[head, offset * head_dim : (offset + 1) * head_dim, :] = turned[
                head * head_dim : (head + 1) * head_dim, :
            ]
    left2[:, :128] = tile2[block].reshape(per_block * sizes[2], channels).T
    weight2[128:, :] = jnp.zeros_like(weight2[128:, :])

    for head in range(heads):
        total = jnp.zeros((head_dim, pixels), jnp.float32)
        for level in range(2):
            side = sides[level]
            left = (left0, left1)[level]
            weight = (weight0, weight1)[level]
            reach = side // 2 + 1
            for point in range(POINTS):
                row = (head * LEVELS + level) * POINTS + point
                line = slice(row, row + 1)
                code = code_ref[line, :]
                across = attend_ref[line, :] * hat(
                    col_ref[line, :], (iota((16, pixels), 0) % side).astype(jnp.float32)
                )
                step = 16 // side
                for index in range(0, 2 * per_block, step):
                    wanted = index + iota((16, pixels), 0) // side
                    weight[point, index * side : (index + step) * side, :] = jnp.where(
                        code == wanted, across, 0.0
                    ).astype(jnp.bfloat16)
                product = jnp.dot(left[head], weight[point], preferred_element_type=jnp.float32)
                down = row_ref[line, :]
                for offset in range(reach):
                    total = total + product[offset * head_dim : (offset + 1) * head_dim, :] * hat(
                        down, float(offset)
                    )
        side = sides[2]
        size = sizes[2]
        place = iota((size, pixels), 0)
        parts = []
        codes = []
        for point in range(POINTS):
            row = (head * LEVELS + 2) * POINTS + point
            line = slice(row, row + 1)
            parts.append(
                attend_ref[line, :]
                * hat(row_ref[line, :], (place // side).astype(jnp.float32))
                * hat(col_ref[line, :], (place % side).astype(jnp.float32))
            )
            codes.append(code_ref[line, :])
        for index in range(per_block):
            mixed = jnp.zeros((size, pixels), jnp.float32)
            for point in range(POINTS):
                mixed = mixed + jnp.where(codes[point] == index, parts[point], 0.0)
            weight2[index * size : (index + 1) * size, :] = mixed.astype(jnp.bfloat16)
        side = sides[3]
        size = sizes[3]
        deep = per_block * size
        place = iota((deep, pixels), 0)
        mixed = jnp.zeros((deep, pixels), jnp.float32)
        for point in range(POINTS):
            row = (head * LEVELS + 3) * POINTS + point
            line = slice(row, row + 1)
            value = (
                attend_ref[line, :]
                * hat(row_ref[line, :], (place % size // side).astype(jnp.float32))
                * hat(col_ref[line, :], (place % side).astype(jnp.float32))
            )
            mixed = mixed + jnp.where(code_ref[line, :] == place // size, value, 0.0)
        weight2[pl.ds(pl.multiple_of(128 + block * deep, deep), deep), :] = mixed.astype(jnp.bfloat16)
        total = total + jnp.dot(
            left2[head * head_dim : (head + 1) * head_dim, :], weight2[...], preferred_element_type=jnp.float32
        )
        out_ref[:, head * head_dim : (head + 1) * head_dim] = total.T.astype(jnp.bfloat16)


def norm_kernel(
    count, head_ref, query_ref, own_ref, other_ref, weight_ref, bias_ref, gain_ref, shift_ref, out_ref
):
    own_head = head_ref[0]
    channels = out_ref.shape[1]
    own_rows = weight_ref[pl.ds(pl.multiple_of(own_head * channels, channels), channels), :]
    other_rows = weight_ref[pl.ds(pl.multiple_of((1 - own_head) * channels, channels), channels), :]
    pre = query_ref[...].astype(jnp.float32) + bias_ref[...]
    pre = pre + jnp.dot(own_ref[...], own_rows, preferred_element_type=jnp.float32)
    pre = pre + jnp.dot(other_ref[...], other_rows, preferred_element_type=jnp.float32)
    centered = pre - jnp.mean(pre, axis=1, keepdims=True)
    variance = jnp.mean(centered * centered, axis=1, keepdims=True)
    own = jnp.where(own_head == 0, centered[:, :channels], centered[:, channels:])
    out_ref[...] = (own * lax.rsqrt(variance + 1e-05) * gain_ref[...] + shift_ref[...]).astype(jnp.bfloat16)


def on_device(
    queries,
    level_zero,
    level_one,
    level_two,
    level_three,
    tile_lists,
    samples,
    logit_weight,
    logit_bias,
    output_weight,
    output_bias,
    norm_gain,
    norm_shift,
):
    level_blocks = (level_zero, level_one, level_two, level_three)
    row_count = lax.axis_size("row")
    col_count = lax.axis_size("col")
    peers = row_count * col_count
    tile_rows, tile_cols, level_count, per_block = tile_lists.shape
    blocks = tile_rows * tile_cols
    requests = blocks * per_block
    capacity = max(2, (requests + peers - 1) // peers)
    grid_cols = tile_cols * col_count
    channels = level_zero.shape[2]
    width_all = queries.shape[2]
    lanes = samples.shape[2]
    heads = lanes // (LEVELS * POINTS)
    head_dim = channels // heads
    sides = tuple(block.shape[0] // tile_rows for block in level_blocks)
    sizes = tuple(side * side for side in sides)
    pixels = sizes[0]
    tile_sets = [
        to_blocks(level_blocks[level], tile_rows, tile_cols, sides[level]) for level in range(level_count)
    ]

    wanted = tile_lists.reshape(blocks, level_count, per_block).transpose(1, 0, 2).reshape(level_count, requests)
    grid_row = wanted // grid_cols
    grid_col = wanted % grid_cols
    owner = grid_row // tile_rows * col_count + grid_col // tile_cols
    local = grid_row % tile_rows * tile_cols + grid_col % tile_cols
    order = jnp.arange(requests, dtype=jnp.int32)
    earlier = (owner[:, :, None] == owner[:, None, :]) & (order[None, None, :] < order[None, :, None])
    rank = jnp.sum(earlier.astype(jnp.int32), axis=2)
    device = jnp.arange(peers, dtype=jnp.int32)
    slot = jnp.arange(capacity, dtype=jnp.int32)
    hit = (owner[None, :, None, :] == device[:, None, None, None]) & (
        rank[None, :, None, :] == slot[None, None, :, None]
    )
    table = jnp.sum(jnp.where(hit, 1 + order * blocks + local[:, None, :], 0), axis=3) - 1
    table = table.reshape(peers, level_count * capacity)
    asked = jnp.where(table >= 0, table % blocks, -1)
    request = jnp.where(table >= 0, table // blocks, -1)
    received = lax.all_to_all(asked, ("row", "col"), split_axis=0, concat_axis=0, tiled=True)

    small = blocks * sizes[3]
    pack = capacity * sum(sizes[:3]) + small
    packs = pl.pallas_call(
        functools.partial(select_kernel, (peers, capacity, sizes)),
        out_shape=jax.ShapeDtypeStruct((peers, pack, channels), jnp.bfloat16),
        in_specs=[pl.BlockSpec(memory_space=SMEM)] + [pl.BlockSpec(memory_space=VMEM)] * 4,
        out_specs=pl.BlockSpec(memory_space=ANY),
        scratch_shapes=[pltpu.SemaphoreType.DMA],
        name="select",
    )(received, tile_sets[0], tile_sets[1], tile_sets[2], tile_sets[3].reshape(small, channels))
    fetched = lax.all_to_all(packs, ("row", "col"), split_axis=0, concat_axis=0, tiled=True)

    queries_blocked = to_blocks(queries, tile_rows, tile_cols, sides[0]).reshape(blocks * pixels, width_all)
    samples_turned = to_blocks(samples, tile_rows, tile_cols, sides[0]).reshape(blocks * pixels, lanes).T
    attend = pl.pallas_call(
        functools.partial(prep_kernel, heads),
        out_shape=jax.ShapeDtypeStruct((lanes, blocks * pixels), jnp.float32),
        grid=(blocks,),
        in_specs=[
            pl.BlockSpec((pixels, width_all), lambda i: (i, 0)),
            pl.BlockSpec((lanes, width_all), lambda i: (0, 0)),
            pl.BlockSpec((lanes, 1), lambda i: (0, 0)),
        ],
        out_specs=pl.BlockSpec((lanes, pixels), lambda i: (0, i)),
        name="prep",
    )(queries_blocked, logit_weight.T, logit_bias.reshape(lanes, 1))

    rowid = (owner[3] * small + local[3] * sizes[3])[:, None] + jnp.arange(sizes[3], dtype=jnp.int32)
    rowid = rowid.reshape(requests * sizes[3], 1)
    depth0 = 2 * per_block * sides[0]
    depth1 = 2 * per_block * sides[1]
    dims = (peers, capacity, sizes, sides, per_block, heads, head_dim, blocks)
    attn = pl.pallas_call(
        functools.partial(attend_kernel, dims),
        out_shape=jax.ShapeDtypeStruct((blocks * pixels, channels), jnp.bfloat16),
        grid=(blocks,),
        in_specs=[
            pl.BlockSpec(memory_space=SMEM),
            pl.BlockSpec(memory_space=ANY),
            pl.BlockSpec((lanes, pixels), lambda i: (0, i)),
            pl.BlockSpec((lanes, pixels), lambda i: (0, i)),
            pl.BlockSpec((requests * sizes[3], 1), lambda i: (0, 0)),
        ],
        out_specs=pl.BlockSpec((pixels, channels), lambda i: (i, 0)),
        scratch_shapes=[
            VMEM((blocks, per_block, sizes[0], channels), jnp.bfloat16),
            VMEM((blocks, per_block, sizes[1], channels), jnp.bfloat16),
            VMEM((blocks, per_block, sizes[2], channels), jnp.bfloat16),
            VMEM((peers, small, channels), jnp.bfloat16),
            VMEM((heads, (sides[0] // 2 + 1) * head_dim, depth0), jnp.bfloat16),
            VMEM((heads, (sides[1] // 2 + 1) * head_dim, depth1), jnp.bfloat16),
            VMEM((channels, per_block * sizes[2] + requests * sizes[3]), jnp.bfloat16),
            VMEM((POINTS, depth0, pixels), jnp.bfloat16),
            VMEM((POINTS, depth1, pixels), jnp.bfloat16),
            VMEM((per_block * sizes[2] + requests * sizes[3], pixels), jnp.bfloat16),
            VMEM((lanes, pixels), jnp.int32),
            VMEM((lanes, pixels), jnp.float32),
            VMEM((lanes, pixels), jnp.float32),
            pltpu.SemaphoreType.DMA((LEVELS, blocks)),
        ],
        name="attend",
    )(request, fetched, attend, samples_turned, rowid)

    own_head = lax.axis_index("head")
    other = lax.ppermute(attn, "head", [(0, 1), (1, 0)])
    updated = pl.pallas_call(
        functools.partial(norm_kernel, blocks),
        out_shape=jax.ShapeDtypeStruct((blocks * pixels, channels), jnp.bfloat16),
        grid=(blocks,),
        in_specs=[
            pl.BlockSpec(memory_space=SMEM),
            pl.BlockSpec((pixels, width_all), lambda i: (i, 0)),
            pl.BlockSpec((pixels, channels), lambda i: (i, 0)),
            pl.BlockSpec((pixels, channels), lambda i: (i, 0)),
            pl.BlockSpec((width_all, width_all), lambda i: (0, 0)),
            pl.BlockSpec((1, width_all), lambda i: (0, 0)),
            pl.BlockSpec((1, channels), lambda i: (0, 0)),
            pl.BlockSpec((1, channels), lambda i: (0, 0)),
        ],
        out_specs=pl.BlockSpec((pixels, channels), lambda i: (i, 0)),
        name="norm",
    )(
        own_head.reshape(1).astype(jnp.int32),
        queries_blocked,
        attn,
        other,
        output_weight,
        output_bias.reshape(1, width_all),
        norm_gain.reshape(1, channels),
        norm_shift.reshape(1, channels),
    )
    side = sides[0]
    updated = updated.reshape(tile_rows, tile_cols, side, side, channels).transpose(0, 2, 1, 3, 4)
    return updated.reshape(tile_rows * side, tile_cols * side, channels)


def solution(mesh):
    in_specs = (
        P("row", "col", None),
        P("row", "col", "head"),
        P("row", "col", "head"),
        P("row", "col", "head"),
        P("row", "col", "head"),
        P("row", "col", None, None),
        P("row", "col", "head"),
        P(None, "head"),
        P("head"),
        P(),
        P(),
        P("head"),
        P("head"),
    )
    out_specs = P("row", "col", "head")
    return jax.shard_map(
        on_device, mesh=mesh, in_specs=in_specs, out_specs=out_specs, check_vma=False
    )
```

```python
import functools
import jax
import jax.numpy as jnp
import numpy as np
from jax import lax
from jax.experimental import pallas as pl
from jax.experimental.pallas import tpu as pltpu
from jax.sharding import PartitionSpec as P

LEVELS = 4
POINTS = 4
ANY = pl.ANY
SMEM = pltpu.SMEM
VMEM = pltpu.VMEM
SELECT_VMEM = 8 * 1024 * 1024
ATTEND_VMEM = 24 * 1024 * 1024


def to_blocks(source, tile_rows, tile_cols, tile_side):
    channels = source.shape[2]
    shaped = source.reshape(tile_rows, tile_side, tile_cols, tile_side, channels)
    return shaped.transpose(0, 2, 1, 3, 4).reshape(
        tile_rows * tile_cols, tile_side * tile_side, channels
    )


def hat(position, center):
    return jnp.maximum(1.0 - jnp.abs(position - center), 0.0)


def iota(shape, dim):
    return lax.broadcasted_iota(jnp.int32, shape, dim)


def prep_kernel(heads, query_ref, weight_ref, bias_ref, out_ref):
    logits = lax.dot_general(
        weight_ref[...], query_ref[...], (((1,), (1,)), ((), ())), preferred_element_type=jnp.float32
    )
    logits = logits + bias_ref[...]
    lanes = LEVELS * POINTS
    for head in range(heads):
        part = logits[head * lanes : (head + 1) * lanes, :]
        part = jnp.exp(part - jnp.max(part, axis=0, keepdims=True))
        out_ref[head * lanes : (head + 1) * lanes, :] = part / jnp.sum(part, axis=0, keepdims=True)


def select_kernel(dims, ids_ref, zero_ref, one_ref, two_ref, three_ref, out_ref, sem):
    peers, capacity, sizes = dims
    refs = (zero_ref, one_ref, two_ref)

    def copies(peer, make):
        base = 0
        for level in range(LEVELS - 1):
            size = sizes[level]
            for slot in range(capacity):
                index = jnp.maximum(ids_ref[peer, level * capacity + slot], 0)
                make(refs[level].at[index], out_ref.at[peer, base : base + size, :])
                base += size
        make(three_ref, out_ref.at[peer, base : base + three_ref.shape[0], :])

    def start(peer, carry):
        copies(peer, lambda src, dst: pltpu.make_async_copy(src, dst, sem).start())
        return carry

    def finish(peer, carry):
        copies(peer, lambda src, dst: pltpu.make_async_copy(src, dst, sem).wait())
        return carry

    lax.fori_loop(0, peers, start, 0)
    lax.fori_loop(0, peers, finish, 0)


def relay_select_kernel(dims, slot, plan_ref, *refs):
    partners, candidates, capacity, sizes, blocks = dims
    ids = refs[:partners]
    sources = refs[partners : partners + candidates]
    outs = refs[partners + candidates :]
    column = plan_ref[slot, 0]
    for number, source in enumerate(sources):

        @pl.when(plan_ref[slot, 1] == number)
        def _(source=source):
            for partner in range(partners):
                base = 0
                start = 0
                for level in range(LEVELS - 1):
                    size = sizes[level]
                    for rank in range(capacity):
                        index = jnp.maximum(ids[partner][column, level * capacity + rank], 0)
                        outs[partner][base : base + size, :] = source[
                            pl.ds(pl.multiple_of(start + index * size, size), size), :
                        ]
                        base += size
                    start += blocks * size
                small = blocks * sizes[3]
                outs[partner][base : base + small, :] = source[start : start + small, :]


def gather_direct(dims, request_ref, fetched_ref, tiles, tile3, sem):
    peers, capacity, sizes, _, per_block, _, _, _ = dims
    small = tile3.shape[1]
    base3 = capacity * sum(sizes[:3])
    pltpu.make_async_copy(fetched_ref.at[:, base3 : base3 + small, :], tile3, sem.at[LEVELS - 1, 0]).start()

    def start(peer, carry):
        base = 0
        for level in range(LEVELS - 1):
            size = sizes[level]
            for rank in range(capacity):
                fetch_one(
                    request_ref[peer, level * capacity + rank],
                    fetched_ref.at[peer, base : base + size, :],
                    tiles[level],
                    per_block,
                    sem,
                    level,
                )
                base += size
        return carry

    lax.fori_loop(0, peers, start, 0)


def fetch_one(request, source, tile, per_block, sem, level):
    @pl.when(request >= 0)
    def _():
        here = request // per_block
        pltpu.make_async_copy(source, tile.at[here, request % per_block], sem.at[level, here]).start()


def gather_relay(dims, relay, request_ref, plan_ref, asked_ref, blocks_refs, packs_refs, tiles, tile3, sem):
    _, capacity, sizes, _, per_block, _, _, blocks = dims
    rows, columns, partner_of = relay
    small = tile3.shape[1]
    my_row = plan_ref[columns, 0]
    my_column = plan_ref[columns, 1]

    def take_small(owner, source):
        pltpu.make_async_copy(source, tile3.at[owner], sem.at[LEVELS - 1, 0]).start()

    for number, source in enumerate(blocks_refs):
        shift = (number + 1) // 2 * (-1 if number % 2 else 1)
        column = my_column + shift

        @pl.when((column >= 0) & (column < columns))
        def _(source=source, column=column):
            owner = my_row * columns + column
            start = 0
            for level in range(LEVELS - 1):
                size = sizes[level]
                for rank in range(capacity):
                    index = jnp.maximum(asked_ref[owner, level * capacity + rank], 0)
                    fetch_one(
                        request_ref[owner, level * capacity + rank],
                        source.at[pl.ds(pl.multiple_of(start + index * size, size), size), :],
                        tiles[level],
                        per_block,
                        sem,
                        level,
                    )
                start += blocks * size
            take_small(owner, source.at[start : start + small, :])

    for number, source in enumerate(packs_refs):
        slot, partner = divmod(number, rows - 1)
        owner = partner_of(my_row, partner + 1) * columns + plan_ref[slot, 0]
        base = 0
        for level in range(LEVELS - 1):
            size = sizes[level]
            for rank in range(capacity):
                fetch_one(
                    request_ref[owner, level * capacity + rank],
                    source.at[base : base + size, :],
                    tiles[level],
                    per_block,
                    sem,
                    level,
                )
                base += size
        take_small(owner, source.at[base : base + small, :])


def attend_kernel(dims, gather, count, *refs):
    sources = refs[:count]
    (
        attend_ref,
        sample_ref,
        rowid_ref,
        out_ref,
        tile0,
        tile1,
        tile2,
        tile3,
        left0,
        left1,
        left2,
        weight0,
        weight1,
        weight2,
        code_ref,
        row_ref,
        col_ref,
        sem,
    ) = refs[count:]
    peers, _, sizes, sides, per_block, heads, head_dim, _ = dims
    block = pl.program_id(0)
    pixels = out_ref.shape[0]
    channels = heads * head_dim
    tiles = (tile0, tile1, tile2)
    small = tile3.shape[1]
    base2 = per_block * sizes[2]

    @pl.when(block == 0)
    def _():
        gather(sources, tiles, tile3, sem)
        left0[...] = jnp.zeros_like(left0)
        weight2[...] = jnp.zeros_like(weight2)
        pltpu.make_async_copy(tile3, tile3, sem.at[LEVELS - 1, 0]).wait()
        flat = tile3[...].reshape(peers * small, channels)
        chosen = (rowid_ref[...] == iota((rowid_ref.shape[0], peers * small), 1)).astype(jnp.bfloat16)
        picked = jnp.dot(chosen, flat, preferred_element_type=jnp.float32)
        left2[:, base2:] = picked.T.astype(jnp.bfloat16)

    packed = sample_ref[...]
    level_of = iota(packed.shape, 0) // POINTS % LEVELS
    slot = packed >> 24
    pos_row = (packed >> 12) & 4095
    pos_col = packed & 4095
    half = lax.shift_right_logical(jnp.full_like(packed, sides[0] * 128), level_of)
    upper = (pos_row >= half) & (level_of < 2)
    code_ref[...] = slot + jnp.where(upper, per_block, 0)
    row_ref[...] = (pos_row - jnp.where(upper, half, 0)).astype(jnp.float32) * (1.0 / 256.0)
    col_ref[...] = pos_col.astype(jnp.float32) * (1.0 / 256.0)

    for level in range(LEVELS - 1):
        pltpu.make_async_copy(tiles[level].at[block], tiles[level].at[block], sem.at[level, block]).wait()

    side0, side1 = sides[0], sides[1]
    half0, half1 = side0 // 2, side1 // 2
    for line in range(side0):
        piece = tile0[block, :, line * side0 : (line + 1) * side0, :]
        turned = piece.reshape(per_block * side0, channels).T
        for group in range(2):
            offset = line - group * half0
            if 0 <= offset <= half0:
                for head in range(heads):
                    left0[
                        head,
                        offset * head_dim : (offset + 1) * head_dim,
                        group * per_block * side0 : (group + 1) * per_block * side0,
                    ] = turned[head * head_dim : (head + 1) * head_dim, :]
    wide1 = tile1[block].astype(jnp.float32)
    for offset in range(half1 + 1):
        first = wide1[:, offset * side1 : (offset + 1) * side1, :]
        other = min(half1 + offset, side1 - 1)
        second = wide1[:, other * side1 : (other + 1) * side1, :]
        both = jnp.concatenate(
            [first.reshape(per_block * side1, channels), second.reshape(per_block * side1, channels)], axis=0
        )
        turned = both.T.astype(jnp.bfloat16)
        for head in range(heads):
            left1[head, offset * head_dim : (offset + 1) * head_dim, :] = turned[
                head * head_dim : (head + 1) * head_dim, :
            ]
    left2[:, :base2] = tile2[block].reshape(per_block * sizes[2], channels).T
    weight2[base2:, :] = jnp.zeros_like(weight2[base2:, :])

    for head in range(heads):
        total = jnp.zeros((head_dim, pixels), jnp.float32)
        for level in range(2):
            side = sides[level]
            left = (left0, left1)[level]
            weight = (weight0, weight1)[level]
            reach = side // 2 + 1
            for point in range(POINTS):
                row = (head * LEVELS + level) * POINTS + point
                line = slice(row, row + 1)
                code = code_ref[line, :]
                across = attend_ref[line, :] * hat(
                    col_ref[line, :], (iota((16, pixels), 0) % side).astype(jnp.float32)
                )
                step = 16 // side
                for index in range(0, 2 * per_block, step):
                    wanted = index + iota((16, pixels), 0) // side
                    weight[point, index * side : (index + step) * side, :] = jnp.where(
                        code == wanted, across, 0.0
                    ).astype(jnp.bfloat16)
                product = jnp.dot(left[head], weight[point], preferred_element_type=jnp.float32)
                down = row_ref[line, :]
                for offset in range(reach):
                    total = total + product[offset * head_dim : (offset + 1) * head_dim, :] * hat(
                        down, float(offset)
                    )
        side = sides[2]
        size = sizes[2]
        place = iota((size, pixels), 0)
        parts = []
        codes = []
        for point in range(POINTS):
            row = (head * LEVELS + 2) * POINTS + point
            line = slice(row, row + 1)
            parts.append(
                attend_ref[line, :]
                * hat(row_ref[line, :], (place // side).astype(jnp.float32))
                * hat(col_ref[line, :], (place % side).astype(jnp.float32))
            )
            codes.append(code_ref[line, :])
        for index in range(per_block):
            mixed = jnp.zeros((size, pixels), jnp.float32)
            for point in range(POINTS):
                mixed = mixed + jnp.where(codes[point] == index, parts[point], 0.0)
            weight2[index * size : (index + 1) * size, :] = mixed.astype(jnp.bfloat16)
        side = sides[3]
        size = sizes[3]
        deep = per_block * size
        place = iota((deep, pixels), 0)
        mixed = jnp.zeros((deep, pixels), jnp.float32)
        for point in range(POINTS):
            row = (head * LEVELS + 3) * POINTS + point
            line = slice(row, row + 1)
            value = (
                attend_ref[line, :]
                * hat(row_ref[line, :], (place % size // side).astype(jnp.float32))
                * hat(col_ref[line, :], (place % side).astype(jnp.float32))
            )
            mixed = mixed + jnp.where(code_ref[line, :] == place // size, value, 0.0)
        weight2[pl.ds(pl.multiple_of(base2 + block * deep, deep), deep), :] = mixed.astype(jnp.bfloat16)
        total = total + jnp.dot(
            left2[head * head_dim : (head + 1) * head_dim, :], weight2[...], preferred_element_type=jnp.float32
        )
        out_ref[:, head * head_dim : (head + 1) * head_dim] = total.T.astype(jnp.bfloat16)


def norm_kernel(head_ref, query_ref, own_ref, other_ref, weight_ref, bias_ref, gain_ref, shift_ref, out_ref):
    own_head = head_ref[0]
    channels = out_ref.shape[1]
    own_rows = weight_ref[pl.ds(pl.multiple_of(own_head * channels, channels), channels), :]
    other_rows = weight_ref[pl.ds(pl.multiple_of((1 - own_head) * channels, channels), channels), :]
    pre = query_ref[...].astype(jnp.float32) + bias_ref[...]
    pre = pre + jnp.dot(own_ref[...], own_rows, preferred_element_type=jnp.float32)
    pre = pre + jnp.dot(other_ref[...], other_rows, preferred_element_type=jnp.float32)
    centered = pre - jnp.mean(pre, axis=1, keepdims=True)
    variance = jnp.mean(centered * centered, axis=1, keepdims=True)
    own = jnp.where(own_head == 0, centered[:, :channels], centered[:, channels:])
    out_ref[...] = (own * lax.rsqrt(variance + 1e-05) * gain_ref[...] + shift_ref[...]).astype(jnp.bfloat16)


def column_order(column, columns):
    found = []
    for step in range(1, columns):
        found += [(step, side) for side in (-1, 1) if 0 <= column + side * step < columns]
    return found


def relay_tiles(dims, row_count, col_count, pack, flat_sets, asked, request):
    _, capacity, sizes, _, _, heads, head_dim, blocks = dims
    channels = heads * head_dim
    my_row = lax.axis_index("row")
    my_column = lax.axis_index("col")
    power = row_count & (row_count - 1) == 0

    def partner_of(row, number):
        return row ^ number if power else (row + number) % row_count

    def source_of(row, number):
        return row ^ number if power else (row + row_count - number) % row_count

    block = jnp.concatenate(flat_sets, axis=0)
    arrived = {}

    def hop(step):
        for side in (-1, 1):
            pairs = []
            for column in range(col_count):
                if 0 <= column + side * step < col_count:
                    pairs.append((column + side, column))
            held = arrived.get((step - 1, side), block)
            arrived[(step, side)] = lax.ppermute(held, "col", pairs)

    hop(1)
    grid = asked.reshape(row_count, col_count, asked.shape[1])
    ids = []
    for number in range(1, row_count):
        mine = lax.dynamic_index_in_dim(grid, partner_of(my_row, number), 0, keepdims=False)
        ids.append(
            lax.ppermute(mine, "row", [(row, partner_of(row, number)) for row in range(row_count)])
        )

    orders = [[(0, 1)] + column_order(column, col_count) for column in range(col_count)]
    candidates = [sorted({order[slot] for order in orders}) for slot in range(col_count)]
    plan = np.zeros((col_count, col_count, 2), np.int32)
    for column in range(col_count):
        for slot in range(col_count):
            step, side = orders[column][slot]
            plan[column, slot] = (column + side * step, candidates[slot].index(orders[column][slot]))
    plan = lax.dynamic_index_in_dim(jnp.asarray(plan), my_column, 0, keepdims=False)
    place = jnp.stack([my_row, my_column]).astype(jnp.int32)
    plan = jnp.concatenate([plan, place[None, :]], axis=0)

    packs = []
    for slot in range(col_count):
        if slot > 1:
            hop(slot)
        held = [block if slot == 0 else arrived[candidate] for candidate in candidates[slot]]
        sent = pl.pallas_call(
            functools.partial(
                relay_select_kernel, (row_count - 1, len(held), capacity, sizes, blocks), slot
            ),
            out_shape=[jax.ShapeDtypeStruct((pack, channels), jnp.bfloat16)] * (row_count - 1),
            in_specs=[pl.BlockSpec(memory_space=SMEM)] * row_count
            + [pl.BlockSpec(memory_space=VMEM)] * len(held),
            out_specs=[pl.BlockSpec(memory_space=VMEM)] * (row_count - 1),
            compiler_params=pltpu.CompilerParams(vmem_limit_bytes=SELECT_VMEM),
        )(plan, *ids, *held)
        for number in range(1, row_count):
            packs.append(
                lax.ppermute(
                    sent[number - 1], "row", [(row, source_of(row, number)) for row in range(row_count)]
                )
            )

    near = [block]
    for step in range(1, col_count):
        near += [arrived[(step, -1)], arrived[(step, 1)]]
    sources = (request, plan, asked, *near, *packs)
    spaces = (SMEM, SMEM, SMEM) + (ANY,) * (len(near) + len(packs))

    def gather(refs, tiles, tile3, sem):
        gather_relay(
            dims,
            (row_count, col_count, partner_of),
            refs[0],
            refs[1],
            refs[2],
            refs[3 : 3 + len(near)],
            refs[3 + len(near) :],
            tiles,
            tile3,
            sem,
        )

    return gather, sources, spaces


def on_device(
    queries,
    level_zero,
    level_one,
    level_two,
    level_three,
    tile_lists,
    samples,
    logit_weight,
    logit_bias,
    output_weight,
    output_bias,
    norm_gain,
    norm_shift,
):
    level_blocks = (level_zero, level_one, level_two, level_three)
    row_count = lax.axis_size("row")
    col_count = lax.axis_size("col")
    peers = row_count * col_count
    tile_rows, tile_cols, level_count, per_block = tile_lists.shape
    blocks = tile_rows * tile_cols
    requests = blocks * per_block
    capacity = max(2, (requests + peers - 1) // peers)
    grid_cols = tile_cols * col_count
    channels = level_zero.shape[2]
    width_all = queries.shape[2]
    lanes = samples.shape[2]
    heads = lanes // (LEVELS * POINTS)
    head_dim = channels // heads
    sides = tuple(block.shape[0] // tile_rows for block in level_blocks)
    sizes = tuple(side * side for side in sides)
    pixels = sizes[0]
    tile_sets = [
        to_blocks(level_blocks[level], tile_rows, tile_cols, sides[level]) for level in range(level_count)
    ]

    wanted = tile_lists.reshape(blocks, level_count, per_block).transpose(1, 0, 2).reshape(level_count, requests)
    grid_row = wanted // grid_cols
    grid_col = wanted % grid_cols
    owner = grid_row // tile_rows * col_count + grid_col // tile_cols
    local = grid_row % tile_rows * tile_cols + grid_col % tile_cols
    order = jnp.arange(requests, dtype=jnp.int32)
    earlier = (owner[:, :, None] == owner[:, None, :]) & (order[None, None, :] < order[None, :, None])
    rank = jnp.sum(earlier.astype(jnp.int32), axis=2)
    device = jnp.arange(peers, dtype=jnp.int32)
    slot = jnp.arange(capacity, dtype=jnp.int32)
    hit = (owner[None, :, None, :] == device[:, None, None, None]) & (
        rank[None, :, None, :] == slot[None, None, :, None]
    )
    table = jnp.sum(jnp.where(hit, 1 + order * blocks + local[:, None, :], 0), axis=3) - 1
    table = table.reshape(peers, level_count * capacity)
    asked = jnp.where(table >= 0, table % blocks, -1)
    request = jnp.where(table >= 0, table // blocks, -1)
    small = blocks * sizes[3]
    pack = capacity * sum(sizes[:3]) + small
    dims = (peers, capacity, sizes, sides, per_block, heads, head_dim, blocks)
    flat_sets = [
        tile_sets[level].reshape(blocks * sizes[level], channels) for level in range(level_count)
    ]
    if peers * capacity <= requests and col_count > 1:
        gather, sources, spaces = relay_tiles(dims, row_count, col_count, pack, flat_sets, asked, request)
    else:
        received = lax.all_to_all(asked, ("row", "col"), split_axis=0, concat_axis=0, tiled=True)
        packs = pl.pallas_call(
            functools.partial(select_kernel, (peers, capacity, sizes)),
            out_shape=jax.ShapeDtypeStruct((peers, pack, channels), jnp.bfloat16),
            in_specs=[pl.BlockSpec(memory_space=SMEM)] + [pl.BlockSpec(memory_space=VMEM)] * 4,
            out_specs=pl.BlockSpec(memory_space=ANY),
            scratch_shapes=[pltpu.SemaphoreType.DMA],
            name="select",
        )(received, tile_sets[0], tile_sets[1], tile_sets[2], flat_sets[3])
        fetched = lax.all_to_all(packs, ("row", "col"), split_axis=0, concat_axis=0, tiled=True)
        sources = (request, fetched)
        spaces = (SMEM, ANY)

        def gather(refs, tiles, tile3, sem):
            gather_direct(dims, refs[0], refs[1], tiles, tile3, sem)

    queries_blocked = to_blocks(queries, tile_rows, tile_cols, sides[0]).reshape(blocks * pixels, width_all)
    samples_turned = to_blocks(samples, tile_rows, tile_cols, sides[0]).reshape(blocks * pixels, lanes).T
    attend = pl.pallas_call(
        functools.partial(prep_kernel, heads),
        out_shape=jax.ShapeDtypeStruct((lanes, blocks * pixels), jnp.float32),
        grid=(blocks,),
        in_specs=[
            pl.BlockSpec((pixels, width_all), lambda i: (i, 0)),
            pl.BlockSpec((lanes, width_all), lambda i: (0, 0)),
            pl.BlockSpec((lanes, 1), lambda i: (0, 0)),
        ],
        out_specs=pl.BlockSpec((lanes, pixels), lambda i: (0, i)),
        compiler_params=pltpu.CompilerParams(vmem_limit_bytes=SELECT_VMEM),
        name="prep",
    )(queries_blocked, logit_weight.T, logit_bias.reshape(lanes, 1))

    rowid = (owner[3] * small + local[3] * sizes[3])[:, None] + jnp.arange(sizes[3], dtype=jnp.int32)
    rowid = rowid.reshape(requests * sizes[3], 1)
    depth0 = 2 * per_block * sides[0]
    depth1 = 2 * per_block * sides[1]
    attn = pl.pallas_call(
        functools.partial(attend_kernel, dims, gather, len(sources)),
        out_shape=jax.ShapeDtypeStruct((blocks * pixels, channels), jnp.bfloat16),
        grid=(blocks,),
        in_specs=[pl.BlockSpec(memory_space=space) for space in spaces]
        + [
            pl.BlockSpec((lanes, pixels), lambda i: (0, i)),
            pl.BlockSpec((lanes, pixels), lambda i: (0, i)),
            pl.BlockSpec((requests * sizes[3], 1), lambda i: (0, 0)),
        ],
        out_specs=pl.BlockSpec((pixels, channels), lambda i: (i, 0)),
        scratch_shapes=[
            VMEM((blocks, per_block, sizes[0], channels), jnp.bfloat16),
            VMEM((blocks, per_block, sizes[1], channels), jnp.bfloat16),
            VMEM((blocks, per_block, sizes[2], channels), jnp.bfloat16),
            VMEM((peers, small, channels), jnp.bfloat16),
            VMEM((heads, (sides[0] // 2 + 1) * head_dim, depth0), jnp.bfloat16),
            VMEM((heads, (sides[1] // 2 + 1) * head_dim, depth1), jnp.bfloat16),
            VMEM((channels, per_block * sizes[2] + requests * sizes[3]), jnp.bfloat16),
            VMEM((POINTS, depth0, pixels), jnp.bfloat16),
            VMEM((POINTS, depth1, pixels), jnp.bfloat16),
            VMEM((per_block * sizes[2] + requests * sizes[3], pixels), jnp.bfloat16),
            VMEM((lanes, pixels), jnp.int32),
            VMEM((lanes, pixels), jnp.float32),
            VMEM((lanes, pixels), jnp.float32),
            pltpu.SemaphoreType.DMA((LEVELS, blocks)),
        ],
        compiler_params=pltpu.CompilerParams(vmem_limit_bytes=ATTEND_VMEM),
        name="attend",
    )(*sources, attend, samples_turned, rowid)

    own_head = lax.axis_index("head")
    other = lax.ppermute(attn, "head", [(0, 1), (1, 0)])
    updated = pl.pallas_call(
        norm_kernel,
        out_shape=jax.ShapeDtypeStruct((blocks * pixels, channels), jnp.bfloat16),
        grid=(blocks,),
        in_specs=[
            pl.BlockSpec(memory_space=SMEM),
            pl.BlockSpec((pixels, width_all), lambda i: (i, 0)),
            pl.BlockSpec((pixels, channels), lambda i: (i, 0)),
            pl.BlockSpec((pixels, channels), lambda i: (i, 0)),
            pl.BlockSpec((width_all, width_all), lambda i: (0, 0)),
            pl.BlockSpec((1, width_all), lambda i: (0, 0)),
            pl.BlockSpec((1, channels), lambda i: (0, 0)),
            pl.BlockSpec((1, channels), lambda i: (0, 0)),
        ],
        out_specs=pl.BlockSpec((pixels, channels), lambda i: (i, 0)),
        compiler_params=pltpu.CompilerParams(vmem_limit_bytes=SELECT_VMEM),
        name="norm",
    )(
        own_head.reshape(1).astype(jnp.int32),
        queries_blocked,
        attn,
        other,
        output_weight,
        output_bias.reshape(1, width_all),
        norm_gain.reshape(1, channels),
        norm_shift.reshape(1, channels),
    )
    side = sides[0]
    updated = updated.reshape(tile_rows, tile_cols, side, side, channels).transpose(0, 2, 1, 3, 4)
    return updated.reshape(tile_rows * side, tile_cols * side, channels)


def solution(mesh):
    in_specs = (
        P("row", "col", None),
        P("row", "col", "head"),
        P("row", "col", "head"),
        P("row", "col", "head"),
        P("row", "col", "head"),
        P("row", "col", None, None),
        P("row", "col", "head"),
        P(None, "head"),
        P("head"),
        P(),
        P(),
        P("head"),
        P("head"),
    )
    out_specs = P("row", "col", "head")
    return jax.shard_map(on_device, mesh=mesh, in_specs=in_specs, out_specs=out_specs, check_vma=False)
```

```python
import functools
import jax
import jax.numpy as jnp
import numpy as np
from jax import lax
from jax.experimental import pallas as pl
from jax.experimental.pallas import tpu as pltpu
from jax.sharding import PartitionSpec as P

LEVELS = 4
POINTS = 4
ANY = pl.ANY
SMEM = pltpu.SMEM
VMEM = pltpu.VMEM
SELECT_VMEM = 8 * 1024 * 1024
PREP_VMEM = 12 * 1024 * 1024
ATTEND_VMEM = 20 * 1024 * 1024


def to_blocks(source, tile_rows, tile_cols, tile_side):
    channels = source.shape[2]
    shaped = source.reshape(tile_rows, tile_side, tile_cols, tile_side, channels)
    return shaped.transpose(0, 2, 1, 3, 4).reshape(
        tile_rows * tile_cols, tile_side * tile_side, channels
    )


def hat(position, center):
    return jnp.maximum(1.0 - jnp.abs(position - center), 0.0)


def iota(shape, dim):
    return lax.broadcasted_iota(jnp.int32, shape, dim)


def prep_kernel(
    dims,
    query_ref,
    logit_ref,
    bias_ref,
    sample_ref,
    weight0,
    weight1,
    weight2,
    down_ref,
    attend_ref,
    code_ref,
    row_ref,
    col_ref,
):
    _, _, sizes, sides, per_block, heads, _, _ = dims
    block = pl.program_id(0)
    pixels = query_ref.shape[0]
    base2 = per_block * sizes[2]
    logits = lax.dot_general(
        logit_ref[...], query_ref[...], (((1,), (1,)), ((), ())), preferred_element_type=jnp.float32
    )
    logits = logits + bias_ref[...]
    lanes = LEVELS * POINTS
    for head in range(heads):
        part = logits[head * lanes : (head + 1) * lanes, :]
        part = jnp.exp(part - jnp.max(part, axis=0, keepdims=True))
        attend_ref[head * lanes : (head + 1) * lanes, :] = part / jnp.sum(part, axis=0, keepdims=True)

    packed = sample_ref[...]
    level_of = iota(packed.shape, 0) // POINTS % LEVELS
    slot = packed >> 24
    pos_row = (packed >> 12) & 4095
    pos_col = packed & 4095
    half = lax.shift_right_logical(jnp.full_like(packed, sides[0] * 128), level_of)
    upper = (pos_row >= half) & (level_of < 2)
    code_ref[...] = slot + jnp.where(upper, per_block, 0)
    down = (pos_row - jnp.where(upper, half, 0)).astype(jnp.float32) * (1.0 / 256.0)
    row_ref[...] = down
    down_ref[...] = down
    col_ref[...] = pos_col.astype(jnp.float32) * (1.0 / 256.0)

    for head in range(heads):
        for level in range(2):
            side = sides[level]
            weight = (weight0, weight1)[level]
            for point in range(POINTS):
                row = (head * LEVELS + level) * POINTS + point
                line = slice(row, row + 1)
                code = code_ref[line, :]
                across = attend_ref[line, :] * hat(
                    col_ref[line, :], (iota((16, pixels), 0) % side).astype(jnp.float32)
                )
                step = 16 // side
                for index in range(0, 2 * per_block, step):
                    wanted = index + iota((16, pixels), 0) // side
                    weight[0, head, point, index * side : (index + step) * side, :] = jnp.where(
                        code == wanted, across, 0.0
                    ).astype(jnp.bfloat16)
        side = sides[2]
        size = sizes[2]
        place = iota((size, pixels), 0)
        parts = []
        codes = []
        for point in range(POINTS):
            row = (head * LEVELS + 2) * POINTS + point
            line = slice(row, row + 1)
            parts.append(
                attend_ref[line, :]
                * hat(row_ref[line, :], (place // side).astype(jnp.float32))
                * hat(col_ref[line, :], (place % side).astype(jnp.float32))
            )
            codes.append(code_ref[line, :])
        for index in range(per_block):
            mixed = jnp.zeros((size, pixels), jnp.float32)
            for point in range(POINTS):
                mixed = mixed + jnp.where(codes[point] == index, parts[point], 0.0)
            weight2[0, head, index * size : (index + 1) * size, :] = mixed.astype(jnp.bfloat16)
        side = sides[3]
        size = sizes[3]
        deep = per_block * size
        place = iota((deep, pixels), 0)
        mixed = jnp.zeros((deep, pixels), jnp.float32)
        for point in range(POINTS):
            row = (head * LEVELS + 3) * POINTS + point
            line = slice(row, row + 1)
            value = (
                attend_ref[line, :]
                * hat(row_ref[line, :], (place % size // side).astype(jnp.float32))
                * hat(col_ref[line, :], (place % side).astype(jnp.float32))
            )
            mixed = mixed + jnp.where(code_ref[line, :] == place // size, value, 0.0)
        weight2[0, head, base2:, :] = jnp.zeros((weight2.shape[2] - base2, pixels), jnp.bfloat16)
        weight2[0, head, pl.ds(pl.multiple_of(base2 + block * deep, deep), deep), :] = mixed.astype(
            jnp.bfloat16
        )


def select_kernel(dims, ids_ref, zero_ref, one_ref, two_ref, three_ref, out_ref, sem):
    peers, capacity, sizes = dims
    refs = (zero_ref, one_ref, two_ref)

    def copies(peer, make):
        base = 0
        for level in range(LEVELS - 1):
            size = sizes[level]
            for slot in range(capacity):
                index = jnp.maximum(ids_ref[peer, level * capacity + slot], 0)
                make(refs[level].at[index], out_ref.at[peer, base : base + size, :])
                base += size
        make(three_ref, out_ref.at[peer, base : base + three_ref.shape[0], :])

    def start(peer, carry):
        copies(peer, lambda src, dst: pltpu.make_async_copy(src, dst, sem).start())
        return carry

    def finish(peer, carry):
        copies(peer, lambda src, dst: pltpu.make_async_copy(src, dst, sem).wait())
        return carry

    lax.fori_loop(0, peers, start, 0)
    lax.fori_loop(0, peers, finish, 0)


def relay_select_kernel(dims, slot, plan_ref, *refs):
    partners, candidates, capacity, sizes, blocks = dims
    ids = refs[:partners]
    sources = refs[partners : partners + candidates]
    outs = refs[partners + candidates :]
    column = plan_ref[slot, 0]
    for number, source in enumerate(sources):

        @pl.when(plan_ref[slot, 1] == number)
        def _(source=source):
            for partner in range(partners):
                base = 0
                start = 0
                for level in range(LEVELS - 1):
                    size = sizes[level]
                    for rank in range(capacity):
                        index = jnp.maximum(ids[partner][column, level * capacity + rank], 0)
                        outs[partner][base : base + size, :] = source[
                            pl.ds(pl.multiple_of(start + index * size, size), size), :
                        ]
                        base += size
                    start += blocks * size
                small = blocks * sizes[3]
                outs[partner][base : base + small, :] = source[start : start + small, :]


def gather_direct(dims, request_ref, fetched_ref, tiles, tile3, sem):
    peers, capacity, sizes, _, _, _, _, _ = dims
    small = tile3.shape[1]
    base3 = capacity * sum(sizes[:3])
    pltpu.make_async_copy(fetched_ref.at[:, base3 : base3 + small, :], tile3, sem.at[LEVELS - 1]).start()

    def start(peer, carry):
        base = 0
        for level in range(LEVELS - 1):
            size = sizes[level]
            for rank in range(capacity):
                fetch_one(
                    request_ref[peer, level * capacity + rank],
                    fetched_ref.at[peer, base : base + size, :],
                    tiles[level],
                    sem.at[level],
                )
                base += size
        return carry

    lax.fori_loop(0, peers, start, 0)
    for level in range(LEVELS - 1):
        pltpu.make_async_copy(tiles[level], tiles[level], sem.at[level]).wait()
    pltpu.make_async_copy(tile3, tile3, sem.at[LEVELS - 1]).wait()


def fetch_one(request, source, tile, sem):
    @pl.when(request >= 0)
    def _():
        pltpu.make_async_copy(source, tile.at[request], sem).start()


def gather_relay(dims, relay, request_ref, plan_ref, asked_ref, blocks_refs, packs_refs, tiles, tile3):
    _, capacity, sizes, _, _, _, _, blocks = dims
    rows, columns, partner_of = relay
    small = tile3.shape[1]
    my_row = plan_ref[columns, 0]
    my_column = plan_ref[columns, 1]

    def put(owner, level, rank, source, start):
        request = request_ref[owner, level * capacity + rank]
        size = sizes[level]
        tiles[level][jnp.maximum(request, 0)] = source[pl.ds(start, size), :]

    for number, source in enumerate(blocks_refs):
        shift = (number + 1) // 2 * (-1 if number % 2 else 1)
        column = my_column + shift

        @pl.when((column >= 0) & (column < columns))
        def _(source=source, column=column):
            owner = my_row * columns + column
            start = 0
            for level in range(LEVELS - 1):
                size = sizes[level]
                for rank in range(capacity):
                    index = jnp.maximum(asked_ref[owner, level * capacity + rank], 0)
                    put(owner, level, rank, source, pl.multiple_of(start + index * size, size))
                start += blocks * size
            tile3[owner] = source[start : start + small, :]

    for number, source in enumerate(packs_refs):
        slot, partner = divmod(number, rows - 1)
        owner = partner_of(my_row, partner + 1) * columns + plan_ref[slot, 0]
        base = 0
        for level in range(LEVELS - 1):
            for rank in range(capacity):
                put(owner, level, rank, source, base)
                base += sizes[level]
        tile3[owner] = source[base : base + small, :]


def attend_kernel(dims, gather, count, *refs):
    sources = refs[:count]
    (
        weight0,
        weight1,
        weight2,
        down_ref,
        rowid_ref,
        out_ref,
        tile0,
        tile1,
        tile2,
        tile3,
        left0,
        left1,
        left2,
        sem,
    ) = refs[count:]
    peers, _, sizes, sides, per_block, heads, head_dim, _ = dims
    block = pl.program_id(0)
    channels = heads * head_dim
    small = tile3.shape[1]
    base2 = per_block * sizes[2]

    @pl.when(block == 0)
    def _():
        gather(sources, (tile0, tile1, tile2), tile3, sem)
        left0[...] = jnp.zeros_like(left0)
        flat = tile3[...].reshape(peers * small, channels)
        chosen = (rowid_ref[...] == iota((rowid_ref.shape[0], peers * small), 1)).astype(jnp.bfloat16)
        picked = jnp.dot(chosen, flat, preferred_element_type=jnp.float32)
        left2[:, base2:] = picked.T.astype(jnp.bfloat16)

    mine = pl.ds(block * per_block, per_block)
    side0, side1 = sides[0], sides[1]
    half0, half1 = side0 // 2, side1 // 2
    for line in range(side0):
        piece = tile0[mine, line * side0 : (line + 1) * side0, :]
        turned = piece.reshape(per_block * side0, channels).T
        for group in range(2):
            offset = line - group * half0
            if 0 <= offset <= half0:
                for head in range(heads):
                    left0[
                        head,
                        offset * head_dim : (offset + 1) * head_dim,
                        group * per_block * side0 : (group + 1) * per_block * side0,
                    ] = turned[head * head_dim : (head + 1) * head_dim, :]
    wide1 = tile1[mine].astype(jnp.float32)
    for offset in range(half1 + 1):
        first = wide1[:, offset * side1 : (offset + 1) * side1, :]
        other = min(half1 + offset, side1 - 1)
        second = wide1[:, other * side1 : (other + 1) * side1, :]
        both = jnp.concatenate(
            [first.reshape(per_block * side1, channels), second.reshape(per_block * side1, channels)], axis=0
        )
        turned = both.T.astype(jnp.bfloat16)
        for head in range(heads):
            left1[head, offset * head_dim : (offset + 1) * head_dim, :] = turned[
                head * head_dim : (head + 1) * head_dim, :
            ]
    left2[:, :base2] = tile2[mine].reshape(per_block * sizes[2], channels).T

    for head in range(heads):
        total = jnp.dot(
            left2[head * head_dim : (head + 1) * head_dim, :],
            weight2[0, head],
            preferred_element_type=jnp.float32,
        )
        for level in range(2):
            left = (left0, left1)[level]
            weight = (weight0, weight1)[level]
            reach = sides[level] // 2 + 1
            for point in range(POINTS):
                row = (head * LEVELS + level) * POINTS + point
                product = jnp.dot(left[head], weight[0, head, point], preferred_element_type=jnp.float32)
                down = down_ref[row : row + 1, :]
                for offset in range(reach):
                    total = total + product[offset * head_dim : (offset + 1) * head_dim, :] * hat(
                        down, float(offset)
                    )
        out_ref[:, head * head_dim : (head + 1) * head_dim] = total.T.astype(jnp.bfloat16)


def own_kernel(head_ref, query_ref, own_ref, weight_ref, bias_ref, out_ref):
    channels = own_ref.shape[1]
    rows = weight_ref[pl.ds(pl.multiple_of(head_ref[0] * channels, channels), channels), :]
    pre = query_ref[...].astype(jnp.float32) + bias_ref[...]
    out_ref[...] = pre + jnp.dot(own_ref[...], rows, preferred_element_type=jnp.float32)


def norm_kernel(head_ref, pre_ref, other_ref, weight_ref, gain_ref, shift_ref, out_ref):
    own_head = head_ref[0]
    channels = out_ref.shape[1]
    rows = weight_ref[pl.ds(pl.multiple_of((1 - own_head) * channels, channels), channels), :]
    pre = pre_ref[...] + jnp.dot(other_ref[...], rows, preferred_element_type=jnp.float32)
    centered = pre - jnp.mean(pre, axis=1, keepdims=True)
    variance = jnp.mean(centered * centered, axis=1, keepdims=True)
    own = jnp.where(own_head == 0, centered[:, :channels], centered[:, channels:])
    out_ref[...] = (own * lax.rsqrt(variance + 1e-05) * gain_ref[...] + shift_ref[...]).astype(jnp.bfloat16)


def column_order(column, columns):
    found = []
    for step in range(1, columns):
        found += [(step, side) for side in (-1, 1) if 0 <= column + side * step < columns]
    return found


def relay_tiles(dims, row_count, col_count, pack, flat_sets, asked, request):
    _, capacity, sizes, _, _, heads, head_dim, blocks = dims
    channels = heads * head_dim
    my_row = lax.axis_index("row")
    my_column = lax.axis_index("col")
    power = row_count & (row_count - 1) == 0

    def partner_of(row, number):
        return row ^ number if power else (row + number) % row_count

    def source_of(row, number):
        return row ^ number if power else (row + row_count - number) % row_count

    block = jnp.concatenate(flat_sets, axis=0)
    arrived = {}

    def hop(step):
        for side in (-1, 1):
            pairs = []
            for column in range(col_count):
                if 0 <= column + side * step < col_count:
                    pairs.append((column + side, column))
            held = arrived.get((step - 1, side), block)
            arrived[(step, side)] = lax.ppermute(held, "col", pairs)

    grid = asked.reshape(row_count, col_count, asked.shape[1])
    ids = []
    for number in range(1, row_count):
        mine = lax.dynamic_index_in_dim(grid, partner_of(my_row, number), 0, keepdims=False)
        ids.append(
            lax.ppermute(mine, "row", [(row, partner_of(row, number)) for row in range(row_count)])
        )

    hop(1)

    orders = [[(0, 1)] + column_order(column, col_count) for column in range(col_count)]
    candidates = [sorted({order[slot] for order in orders}) for slot in range(col_count)]
    plan = np.zeros((col_count, col_count, 2), np.int32)
    for column in range(col_count):
        for slot in range(col_count):
            step, side = orders[column][slot]
            plan[column, slot] = (column + side * step, candidates[slot].index(orders[column][slot]))
    plan = lax.dynamic_index_in_dim(jnp.asarray(plan), my_column, 0, keepdims=False)
    place = jnp.stack([my_row, my_column]).astype(jnp.int32)
    plan = jnp.concatenate([plan, place[None, :]], axis=0)

    packs = []
    for slot in range(col_count):
        if slot > 1:
            hop(slot)
        held = [block if slot == 0 else arrived[candidate] for candidate in candidates[slot]]
        sent = pl.pallas_call(
            functools.partial(
                relay_select_kernel, (row_count - 1, len(held), capacity, sizes, blocks), slot
            ),
            out_shape=[jax.ShapeDtypeStruct((pack, channels), jnp.bfloat16)] * (row_count - 1),
            in_specs=[pl.BlockSpec(memory_space=SMEM)] * row_count
            + [pl.BlockSpec(memory_space=VMEM)] * len(held),
            out_specs=[pl.BlockSpec(memory_space=VMEM)] * (row_count - 1),
            compiler_params=pltpu.CompilerParams(vmem_limit_bytes=SELECT_VMEM),
        )(plan, *ids, *held)
        for number in range(1, row_count):
            packs.append(
                lax.ppermute(
                    sent[number - 1], "row", [(row, source_of(row, number)) for row in range(row_count)]
                )
            )

    near = [block]
    for step in range(1, col_count):
        near += [arrived[(step, -1)], arrived[(step, 1)]]
    sources = (request, plan, asked, *near, *packs)
    spaces = (SMEM, SMEM, SMEM) + (VMEM,) * (len(near) + len(packs))

    def gather(refs, tiles, tile3, sem):
        gather_relay(
            dims,
            (row_count, col_count, partner_of),
            refs[0],
            refs[1],
            refs[2],
            refs[3 : 3 + len(near)],
            refs[3 + len(near) :],
            tiles,
            tile3,
        )

    return gather, sources, spaces


def on_device(
    queries,
    level_zero,
    level_one,
    level_two,
    level_three,
    tile_lists,
    samples,
    logit_weight,
    logit_bias,
    output_weight,
    output_bias,
    norm_gain,
    norm_shift,
):
    level_blocks = (level_zero, level_one, level_two, level_three)
    row_count = lax.axis_size("row")
    col_count = lax.axis_size("col")
    peers = row_count * col_count
    tile_rows, tile_cols, level_count, per_block = tile_lists.shape
    blocks = tile_rows * tile_cols
    requests = blocks * per_block
    capacity = max(2, (requests + peers - 1) // peers)
    grid_cols = tile_cols * col_count
    channels = level_zero.shape[2]
    width_all = queries.shape[2]
    lanes = samples.shape[2]
    heads = lanes // (LEVELS * POINTS)
    head_dim = channels // heads
    sides = tuple(block.shape[0] // tile_rows for block in level_blocks)
    sizes = tuple(side * side for side in sides)
    pixels = sizes[0]
    tile_sets = [
        to_blocks(level_blocks[level], tile_rows, tile_cols, sides[level]) for level in range(level_count)
    ]

    wanted = tile_lists.reshape(blocks, level_count, per_block).transpose(1, 0, 2).reshape(level_count, requests)
    grid_row = wanted // grid_cols
    grid_col = wanted % grid_cols
    owner = grid_row // tile_rows * col_count + grid_col // tile_cols
    local = grid_row % tile_rows * tile_cols + grid_col % tile_cols
    order = jnp.arange(requests, dtype=jnp.int32)
    earlier = (owner[:, :, None] == owner[:, None, :]) & (order[None, None, :] < order[None, :, None])
    rank = jnp.sum(earlier.astype(jnp.int32), axis=2)
    device = jnp.arange(peers, dtype=jnp.int32)
    slot = jnp.arange(capacity, dtype=jnp.int32)
    hit = (owner[None, :, None, :] == device[:, None, None, None]) & (
        rank[None, :, None, :] == slot[None, None, :, None]
    )
    table = jnp.sum(jnp.where(hit, 1 + order * blocks + local[:, None, :], 0), axis=3) - 1
    table = table.reshape(peers, level_count * capacity)
    asked = jnp.where(table >= 0, table % blocks, -1)
    request = jnp.where(table >= 0, table // blocks, -1)
    small = blocks * sizes[3]
    pack = capacity * sum(sizes[:3]) + small
    dims = (peers, capacity, sizes, sides, per_block, heads, head_dim, blocks)
    flat_sets = [
        tile_sets[level].reshape(blocks * sizes[level], channels) for level in range(level_count)
    ]
    if peers * capacity <= requests and col_count > 1:
        gather, sources, spaces = relay_tiles(dims, row_count, col_count, pack, flat_sets, asked, request)
    else:
        received = lax.all_to_all(asked, ("row", "col"), split_axis=0, concat_axis=0, tiled=True)
        packs = pl.pallas_call(
            functools.partial(select_kernel, (peers, capacity, sizes)),
            out_shape=jax.ShapeDtypeStruct((peers, pack, channels), jnp.bfloat16),
            in_specs=[pl.BlockSpec(memory_space=SMEM)] + [pl.BlockSpec(memory_space=VMEM)] * 4,
            out_specs=pl.BlockSpec(memory_space=ANY),
            scratch_shapes=[pltpu.SemaphoreType.DMA],
            name="select",
        )(received, tile_sets[0], tile_sets[1], tile_sets[2], flat_sets[3])
        fetched = lax.all_to_all(packs, ("row", "col"), split_axis=0, concat_axis=0, tiled=True)
        sources = (request, fetched)
        spaces = (SMEM, ANY)

        def gather(refs, tiles, tile3, sem):
            gather_direct(dims, refs[0], refs[1], tiles, tile3, sem)

    queries_blocked = to_blocks(queries, tile_rows, tile_cols, sides[0]).reshape(blocks * pixels, width_all)
    samples_turned = to_blocks(samples, tile_rows, tile_cols, sides[0]).reshape(blocks * pixels, lanes).T
    depth0 = 2 * per_block * sides[0]
    depth1 = 2 * per_block * sides[1]
    depth2 = per_block * sizes[2] + requests * sizes[3]
    shape0 = (heads, POINTS, depth0, pixels)
    shape1 = (heads, POINTS, depth1, pixels)
    shape2 = (heads, depth2, pixels)
    weight_specs = [
        pl.BlockSpec((1, *shape0), lambda i: (i, 0, 0, 0, 0)),
        pl.BlockSpec((1, *shape1), lambda i: (i, 0, 0, 0, 0)),
        pl.BlockSpec((1, *shape2), lambda i: (i, 0, 0, 0)),
        pl.BlockSpec((lanes, pixels), lambda i: (0, i)),
    ]
    weights = pl.pallas_call(
        functools.partial(prep_kernel, dims),
        out_shape=[
            jax.ShapeDtypeStruct((blocks, *shape0), jnp.bfloat16),
            jax.ShapeDtypeStruct((blocks, *shape1), jnp.bfloat16),
            jax.ShapeDtypeStruct((blocks, *shape2), jnp.bfloat16),
            jax.ShapeDtypeStruct((lanes, blocks * pixels), jnp.float32),
        ],
        grid=(blocks,),
        in_specs=[
            pl.BlockSpec((pixels, width_all), lambda i: (i, 0)),
            pl.BlockSpec((lanes, width_all), lambda i: (0, 0)),
            pl.BlockSpec((lanes, 1), lambda i: (0, 0)),
            pl.BlockSpec((lanes, pixels), lambda i: (0, i)),
        ],
        out_specs=weight_specs,
        scratch_shapes=[
            VMEM((lanes, pixels), jnp.float32),
            VMEM((lanes, pixels), jnp.int32),
            VMEM((lanes, pixels), jnp.float32),
            VMEM((lanes, pixels), jnp.float32),
        ],
        compiler_params=pltpu.CompilerParams(vmem_limit_bytes=PREP_VMEM),
        name="prep",
    )(queries_blocked, logit_weight.T, logit_bias.reshape(lanes, 1), samples_turned)

    rowid = (owner[3] * small + local[3] * sizes[3])[:, None] + jnp.arange(sizes[3], dtype=jnp.int32)
    rowid = rowid.reshape(requests * sizes[3], 1)
    attn = pl.pallas_call(
        functools.partial(attend_kernel, dims, gather, len(sources)),
        out_shape=jax.ShapeDtypeStruct((blocks * pixels, channels), jnp.bfloat16),
        grid=(blocks,),
        in_specs=[pl.BlockSpec(memory_space=space) for space in spaces]
        + weight_specs
        + [pl.BlockSpec((requests * sizes[3], 1), lambda i: (0, 0))],
        out_specs=pl.BlockSpec((pixels, channels), lambda i: (i, 0)),
        scratch_shapes=[
            VMEM((requests, sizes[0], channels), jnp.bfloat16),
            VMEM((requests, sizes[1], channels), jnp.bfloat16),
            VMEM((requests, sizes[2], channels), jnp.bfloat16),
            VMEM((peers, small, channels), jnp.bfloat16),
            VMEM((heads, (sides[0] // 2 + 1) * head_dim, depth0), jnp.bfloat16),
            VMEM((heads, (sides[1] // 2 + 1) * head_dim, depth1), jnp.bfloat16),
            VMEM((channels, depth2), jnp.bfloat16),
            pltpu.SemaphoreType.DMA((LEVELS,)),
        ],
        compiler_params=pltpu.CompilerParams(vmem_limit_bytes=ATTEND_VMEM),
        name="attend",
    )(*sources, *weights, rowid)

    own_head = lax.axis_index("head").reshape(1).astype(jnp.int32)
    other = lax.ppermute(attn, "head", [(0, 1), (1, 0)])
    wide_spec = pl.BlockSpec((pixels, width_all), lambda i: (i, 0))
    slim_spec = pl.BlockSpec((pixels, channels), lambda i: (i, 0))
    matrix_spec = pl.BlockSpec((width_all, width_all), lambda i: (0, 0))
    pre = pl.pallas_call(
        own_kernel,
        out_shape=jax.ShapeDtypeStruct((blocks * pixels, width_all), jnp.float32),
        grid=(blocks,),
        in_specs=[
            pl.BlockSpec(memory_space=SMEM),
            wide_spec,
            slim_spec,
            matrix_spec,
            pl.BlockSpec((1, width_all), lambda i: (0, 0)),
        ],
        out_specs=wide_spec,
        compiler_params=pltpu.CompilerParams(vmem_limit_bytes=SELECT_VMEM),
        name="own",
    )(own_head, queries_blocked, attn, output_weight, output_bias.reshape(1, width_all))
    updated = pl.pallas_call(
        norm_kernel,
        out_shape=jax.ShapeDtypeStruct((blocks * pixels, channels), jnp.bfloat16),
        grid=(blocks,),
        in_specs=[
            pl.BlockSpec(memory_space=SMEM),
            wide_spec,
            slim_spec,
            matrix_spec,
            pl.BlockSpec((1, channels), lambda i: (0, 0)),
            pl.BlockSpec((1, channels), lambda i: (0, 0)),
        ],
        out_specs=slim_spec,
        compiler_params=pltpu.CompilerParams(vmem_limit_bytes=SELECT_VMEM),
        name="norm",
    )(
        own_head,
        pre,
        other,
        output_weight,
        norm_gain.reshape(1, channels),
        norm_shift.reshape(1, channels),
    )
    side = sides[0]
    updated = updated.reshape(tile_rows, tile_cols, side, side, channels).transpose(0, 2, 1, 3, 4)
    return updated.reshape(tile_rows * side, tile_cols * side, channels)


def solution(mesh):
    in_specs = (
        P("row", "col", None),
        P("row", "col", "head"),
        P("row", "col", "head"),
        P("row", "col", "head"),
        P("row", "col", "head"),
        P("row", "col", None, None),
        P("row", "col", "head"),
        P(None, "head"),
        P("head"),
        P(),
        P(),
        P("head"),
        P("head"),
    )
    out_specs = P("row", "col", "head")
    return jax.shard_map(on_device, mesh=mesh, in_specs=in_specs, out_specs=out_specs, check_vma=False)
```

```python
import functools
import jax
import jax.numpy as jnp
from jax import lax
from jax.experimental import pallas as pl
from jax.experimental.pallas import tpu as pltpu
from jax.sharding import PartitionSpec as P

LEVELS = 4
POINTS = 4
ANY = pl.ANY
SMEM = pltpu.SMEM
VMEM = pltpu.VMEM
SELECT_VMEM = 4 * 1024 * 1024
PREP_VMEM = 8 * 1024 * 1024
ATTEND_VMEM = 12 * 1024 * 1024
GROUPS = (2, 4)


def to_blocks(source, tile_rows, tile_cols, tile_side):
    channels = source.shape[2]
    shaped = source.reshape(tile_rows, tile_side, tile_cols, tile_side, channels)
    return shaped.transpose(0, 2, 1, 3, 4).reshape(
        tile_rows * tile_cols, tile_side * tile_side, channels
    )


def hat(position, center):
    return jnp.maximum(1.0 - jnp.abs(position - center), 0.0)


def iota(shape, dim):
    return lax.broadcasted_iota(jnp.int32, shape, dim)


def prep_kernel(
    dims,
    query_hbm,
    logit_hbm,
    bias_hbm,
    sample_hbm,
    weight1,
    weight2,
    attend_ref,
    code_ref,
    down_ref,
    col_ref,
    query_ref,
    logit_ref,
    bias_ref,
    sample_ref,
    sem,
):
    _, _, sizes, sides, per_block, heads, _, blocks = dims
    pixels = sizes[0]
    base2 = per_block * sizes[2]
    lanes = LEVELS * POINTS
    moves = [
        pltpu.make_async_copy(source, target, sem.at[number])
        for number, (source, target) in enumerate(
            (
                (query_hbm, query_ref),
                (logit_hbm, logit_ref),
                (bias_hbm, bias_ref),
                (sample_hbm, sample_ref),
            )
        )
    ]
    for move in moves:
        move.start()
    weight2[...] = jnp.zeros_like(weight2)
    for move in moves:
        move.wait()

    def one(block, carry):
        here = pl.ds(pl.multiple_of(block * pixels, pixels), pixels)
        logits = lax.dot_general(
            query_ref[here, :], logit_ref[...], (((1,), (1,)), ((), ())), preferred_element_type=jnp.float32
        )
        logits = (logits + bias_ref[...]).T
        for head in range(heads):
            part = logits[head * lanes : (head + 1) * lanes, :]
            part = jnp.exp(part - jnp.max(part, axis=0, keepdims=True))
            attend_ref[block, head * lanes : (head + 1) * lanes, :] = part / jnp.sum(
                part, axis=0, keepdims=True
            )
        packed = sample_ref[here, :].T
        level_of = iota(packed.shape, 0) // POINTS % LEVELS
        slot = packed >> 24
        pos_row = (packed >> 12) & 4095
        pos_col = packed & 4095
        deep = jnp.where(level_of == 0, sides[0] * 128, sides[1] * 256 // GROUPS[1])
        group = jnp.where(level_of < 2, pos_row // deep, 0)
        code_ref[block] = slot + group * per_block
        down_ref[block] = (pos_row - group * deep).astype(jnp.float32) * (1.0 / 256.0)
        col_ref[block] = pos_col.astype(jnp.float32) * (1.0 / 256.0)

        for head in range(heads):
            hot_rows(1, block, head, sides, per_block, attend_ref, code_ref, col_ref, weight1)
            side = sides[2]
            size = sizes[2]
            place = iota((size, pixels), 0)
            parts = []
            codes = []
            for point in range(POINTS):
                row = (head * LEVELS + 2) * POINTS + point
                line = slice(row, row + 1)
                parts.append(
                    attend_ref[block, line, :]
                    * hat(down_ref[block, line, :], (place // side).astype(jnp.float32))
                    * hat(col_ref[block, line, :], (place % side).astype(jnp.float32))
                )
                codes.append(code_ref[block, line, :])
            for index in range(per_block):
                mixed = jnp.zeros((size, pixels), jnp.float32)
                for point in range(POINTS):
                    mixed = mixed + jnp.where(codes[point] == index, parts[point], 0.0)
                weight2[block, head, index * size : (index + 1) * size, :] = mixed.astype(jnp.bfloat16)
            side = sides[3]
            size = sizes[3]
            depth = per_block * size
            place = iota((depth, pixels), 0)
            mixed = jnp.zeros((depth, pixels), jnp.float32)
            for point in range(POINTS):
                row = (head * LEVELS + 3) * POINTS + point
                line = slice(row, row + 1)
                value = (
                    attend_ref[block, line, :]
                    * hat(down_ref[block, line, :], (place % size // side).astype(jnp.float32))
                    * hat(col_ref[block, line, :], (place % side).astype(jnp.float32))
                )
                mixed = mixed + jnp.where(code_ref[block, line, :] == place // size, value, 0.0)
            weight2[block, head, pl.ds(pl.multiple_of(base2 + block * depth, depth), depth), :] = mixed.astype(
                jnp.bfloat16
            )
        return carry

    lax.fori_loop(0, blocks, one, 0)


def hot_rows(level, block, head, sides, per_block, attend_ref, code_ref, col_ref, weight):
    side = sides[level]
    pixels = attend_ref.shape[2]
    step = 16 // side
    for point in range(POINTS):
        row = (head * LEVELS + level) * POINTS + point
        line = slice(row, row + 1)
        code = code_ref[block, line, :]
        across = attend_ref[block, line, :] * hat(
            col_ref[block, line, :], (iota((16, pixels), 0) % side).astype(jnp.float32)
        )
        for index in range(0, GROUPS[level] * per_block, step):
            wanted = index + iota((16, pixels), 0) // side
            weight[block, head, point, index * side : (index + step) * side, :] = jnp.where(
                code == wanted, across, 0.0
            ).astype(jnp.bfloat16)


def hot_kernel(dims, attend_ref, code_ref, col_ref, weight0):
    _, _, _, sides, per_block, heads, _, blocks = dims

    def one(block, carry):
        for head in range(heads):
            hot_rows(0, block, head, sides, per_block, attend_ref, code_ref, col_ref, weight0)
        return carry

    lax.fori_loop(0, blocks, one, 0)


def select_kernel(dims, ids_ref, zero_ref, one_ref, two_ref, three_ref, out_ref, sem):
    peers, capacity, sizes = dims
    refs = (zero_ref, one_ref, two_ref)

    def copies(peer, make):
        base = 0
        for level in range(LEVELS - 1):
            size = sizes[level]
            for slot in range(capacity):
                index = jnp.maximum(ids_ref[peer, level * capacity + slot], 0)
                make(refs[level].at[index], out_ref.at[peer, base : base + size, :])
                base += size
        make(three_ref, out_ref.at[peer, base : base + three_ref.shape[0], :])

    def start(peer, carry):
        copies(peer, lambda src, dst: pltpu.make_async_copy(src, dst, sem).start())
        return carry

    def finish(peer, carry):
        copies(peer, lambda src, dst: pltpu.make_async_copy(src, dst, sem).wait())
        return carry

    lax.fori_loop(0, peers, start, 0)
    lax.fori_loop(0, peers, finish, 0)


def pick(values, my_column):
    chosen = jnp.int32(values[0])
    for column in range(1, len(values)):
        chosen = jnp.where(my_column == column, values[column], chosen)
    return chosen


def relay_select_kernel(dims, order, place_ref, ids_ref, request_ref, *refs):
    partners, candidates, capacity, sizes, blocks = dims
    sources = refs[:candidates]
    outs = refs[candidates:]
    columns, numbers = order
    column = pick(columns, place_ref[1])
    which = pick(numbers, place_ref[1])
    for number, source in enumerate(sources):

        @pl.when(which == number)
        def _(source=source):
            for partner in range(partners):
                base = 0
                start = 0
                for level in range(LEVELS - 1):
                    size = sizes[level]
                    for rank in range(capacity):
                        index = jnp.maximum(ids_ref[partner + 1, column, level * capacity + rank], 0)
                        outs[partner][base : base + size, :] = source[
                            pl.ds(pl.multiple_of(start + index * size, size), size), :
                        ]
                        base += size
                    start += blocks * size
                small = blocks * sizes[3]
                outs[partner][base : base + small, :] = source[start : start + small, :]


def gather_direct(dims, request_ref, fetched_ref, tiles, tile3, sem):
    peers, capacity, sizes, _, _, _, _, _ = dims
    small = tile3.shape[1]
    base3 = capacity * sum(sizes[:3])
    pltpu.make_async_copy(fetched_ref.at[:, base3 : base3 + small, :], tile3, sem.at[LEVELS - 1]).start()

    def start(peer, carry):
        base = 0
        for level in range(LEVELS - 1):
            size = sizes[level]
            for rank in range(capacity):
                fetch_one(
                    request_ref[peer, level * capacity + rank],
                    fetched_ref.at[peer, base : base + size, :],
                    tiles[level],
                    sem.at[level],
                )
                base += size
        return carry

    lax.fori_loop(0, peers, start, 0)
    for level in range(LEVELS - 1):
        pltpu.make_async_copy(tiles[level], tiles[level], sem.at[level]).wait()
    pltpu.make_async_copy(tile3, tile3, sem.at[LEVELS - 1]).wait()


def fetch_one(request, source, tile, sem):
    @pl.when(request >= 0)
    def _():
        pltpu.make_async_copy(source, tile.at[request], sem).start()


def gather_relay(dims, relay, request_ref, place_ref, ids_ref, blocks_refs, packs_refs, tiles, tile3):
    _, capacity, sizes, _, _, _, _, blocks = dims
    rows, columns, partner_of, met = relay
    small = tile3.shape[1]
    my_row = place_ref[0]
    my_column = place_ref[1]

    def put(owner, level, rank, source, start):
        request = request_ref[owner, level * capacity + rank]
        size = sizes[level]
        tiles[level][jnp.maximum(request, 0)] = source[pl.ds(start, size), :]

    for number, source in enumerate(blocks_refs):
        shift = (number + 1) // 2 * (-1 if number % 2 else 1)
        column = my_column + shift

        @pl.when((column >= 0) & (column < columns))
        def _(source=source, column=column):
            owner = my_row * columns + column
            start = 0
            for level in range(LEVELS - 1):
                size = sizes[level]
                for rank in range(capacity):
                    index = jnp.maximum(ids_ref[0, column, level * capacity + rank], 0)
                    put(owner, level, rank, source, pl.multiple_of(start + index * size, size))
                start += blocks * size
            tile3[owner] = source[start : start + small, :]

    for number, source in enumerate(packs_refs):
        slot, partner = divmod(number, rows - 1)
        owner = partner_of(my_row, partner + 1) * columns + pick(met[slot], my_column)
        base = 0
        for level in range(LEVELS - 1):
            for rank in range(capacity):
                put(owner, level, rank, source, base)
                base += sizes[level]
        tile3[owner] = source[base : base + small, :]


def attend_kernel(dims, grid, gather, count, *refs):
    sources = refs[:count]
    (
        weight0,
        weight1,
        weight2,
        down_ref,
        lists_ref,
        out_ref,
        tile0,
        tile1,
        tile2,
        tile3,
        left0,
        left1,
        left2,
        sem,
    ) = refs[count:]
    peers, capacity, sizes, sides, per_block, heads, head_dim, blocks = dims
    pixels = sizes[0]
    channels = heads * head_dim
    small = tile3.shape[1]
    base2 = per_block * sizes[2]
    side0, side1 = sides[0], sides[1]

    gather(sources, (tile0, tile1, tile2), tile3, sem)
    left0[...] = jnp.zeros_like(left0)
    flat = tile3[...].reshape(peers * small, channels)
    size3 = sizes[3]
    wide = blocks * per_block * size3
    lane = iota((1, wide), 1)
    target = lane % size3
    tile_rows, tile_cols, grid_cols, col_count, capacity = grid
    for request in range(blocks * per_block):
        block, entry = divmod(request, per_block)
        tile = lists_ref[block // tile_cols, block % tile_cols, LEVELS - 1, entry]
        tile_row = tile // grid_cols
        tile_col = tile % grid_cols
        owner = tile_row // tile_rows * col_count + tile_col // tile_cols
        first = owner * small + (tile_row % tile_rows * tile_cols + tile_col % tile_cols) * size3
        target = target + jnp.where(lane // size3 == request, first, 0)
    chosen = (iota((peers * small, wide), 0) == target).astype(jnp.bfloat16)
    picked = lax.dot_general(flat, chosen, (((0,), (0,)), ((), ())), preferred_element_type=jnp.float32)
    left2[:, base2:] = picked.astype(jnp.bfloat16)

    def one(block, carry):
        mine = pl.ds(block * per_block, per_block)
        reach0 = side0 // GROUPS[0]
        for line in range(side0):
            piece = tile0[mine, line * side0 : (line + 1) * side0, :]
            turned = piece.reshape(per_block * side0, channels).T
            for group in range(GROUPS[0]):
                offset = line - group * reach0
                if 0 <= offset <= reach0:
                    for head in range(heads):
                        left0[
                            head,
                            offset * head_dim : (offset + 1) * head_dim,
                            group * per_block * side0 : (group + 1) * per_block * side0,
                        ] = turned[head * head_dim : (head + 1) * head_dim, :]
        wide1 = tile1[mine].astype(jnp.float32)
        reach1 = side1 // GROUPS[1]
        for offset in range(reach1 + 1):
            stack = []
            for group in range(GROUPS[1]):
                line = min(group * reach1 + offset, side1 - 1)
                stack.append(
                    wide1[:, line * side1 : (line + 1) * side1, :].reshape(per_block * side1, channels)
                )
            turned = jnp.concatenate(stack, axis=0).astype(jnp.bfloat16).T
            for head in range(heads):
                left1[head, offset * head_dim : (offset + 1) * head_dim, :] = turned[
                    head * head_dim : (head + 1) * head_dim, :
                ]
        left2[:, :base2] = tile2[mine].reshape(per_block * sizes[2], channels).T

        for head in range(heads):
            total = jnp.dot(
                left2[head * head_dim : (head + 1) * head_dim, :],
                weight2[block, head],
                preferred_element_type=jnp.float32,
            )
            for level in range(2):
                left = (left0, left1)[level]
                weight = (weight0, weight1)[level]
                for point in range(POINTS):
                    row = (head * LEVELS + level) * POINTS + point
                    product = jnp.dot(left[head], weight[block, head, point], preferred_element_type=jnp.float32)
                    down = down_ref[block, row : row + 1, :]
                    for offset in range(sides[level] // GROUPS[level] + 1):
                        total = total + product[offset * head_dim : (offset + 1) * head_dim, :] * hat(
                            down, float(offset)
                        )
            out_ref[
                pl.ds(pl.multiple_of(block * pixels, pixels), pixels), head * head_dim : (head + 1) * head_dim
            ] = total.T.astype(jnp.bfloat16)
        return carry

    lax.fori_loop(0, blocks, one, 0)


def own_kernel(head_ref, query_ref, own_ref, weight_ref, bias_ref, out_ref):
    channels = own_ref.shape[1]
    rows = weight_ref[pl.ds(pl.multiple_of(head_ref[0] * channels, channels), channels), :]
    pre = query_ref[...].astype(jnp.float32) + bias_ref[...]
    out_ref[...] = pre + jnp.dot(own_ref[...], rows, preferred_element_type=jnp.float32)


def norm_kernel(head_ref, pre_ref, other_ref, weight_ref, gain_ref, shift_ref, out_ref):
    own_head = head_ref[0]
    channels = out_ref.shape[1]
    rows = weight_ref[pl.ds(pl.multiple_of((1 - own_head) * channels, channels), channels), :]
    pre = pre_ref[...] + jnp.dot(other_ref[...], rows, preferred_element_type=jnp.float32)
    centered = pre - jnp.mean(pre, axis=1, keepdims=True)
    variance = jnp.mean(centered * centered, axis=1, keepdims=True)
    own = jnp.where(own_head == 0, centered[:, :channels], centered[:, channels:])
    out_ref[...] = (own * lax.rsqrt(variance + 1e-05) * gain_ref[...] + shift_ref[...]).astype(jnp.bfloat16)


def column_order(column, columns):
    found = []
    for step in range(1, columns):
        found += [(step, side) for side in (-1, 1) if 0 <= column + side * step < columns]
    return found


def tables(lists, grid):
    tile_rows, tile_cols, grid_cols, col_count, _ = grid
    count, blocks, level_count, per_block = lists.shape
    requests = blocks * per_block
    wanted = lists.transpose(0, 2, 1, 3).reshape(count, level_count, requests)
    grid_row = wanted // grid_cols
    grid_col = wanted % grid_cols
    owner = grid_row // tile_rows * col_count + grid_col // tile_cols
    local = grid_row % tile_rows * tile_cols + grid_col % tile_cols
    order = jnp.arange(requests, dtype=jnp.int32)
    earlier = (owner[..., :, None] == owner[..., None, :]) & (order[None, :] < order[:, None])
    rank = jnp.sum(earlier.astype(jnp.int32), axis=3)
    return owner, local, rank


def entries(owner, rank, owners, capacity, value):
    slot = jnp.arange(capacity, dtype=jnp.int32)
    hit = (owner[:, None, :, None, :] == owners[None, :, None, None, None]) & (
        rank[:, None, :, None, :] == slot[None, None, None, :, None]
    )
    found = jnp.sum(jnp.where(hit, 1 + value[:, None, :, None, :], 0), axis=4) - 1
    return found.reshape(owner.shape[0], owners.shape[0], -1)


def relay_tiles(dims, row_count, col_count, pack, flat_sets, lists, grid):
    peers, capacity, sizes, _, per_block, heads, head_dim, blocks = dims
    channels = heads * head_dim
    my_row = lax.axis_index("row")
    my_column = lax.axis_index("col")
    power = row_count & (row_count - 1) == 0

    def partner_of(row, number):
        return row ^ number if power else (row + number) % row_count

    def source_of(row, number):
        return row ^ number if power else (row + row_count - number) % row_count

    gathered = [lists]
    for number in range(1, row_count):
        gathered.append(
            lax.ppermute(lists, "row", [(row, partner_of(row, number)) for row in range(row_count)])
        )
    block = jnp.concatenate(flat_sets, axis=0)
    arrived = {}

    def hop(step):
        for side in (-1, 1):
            pairs = []
            for column in range(col_count):
                if 0 <= column + side * step < col_count:
                    pairs.append((column + side, column))
            held = arrived.get((step - 1, side), block)
            arrived[(step, side)] = lax.ppermute(held, "col", pairs)

    hop(1)
    place = jnp.stack([my_row, my_column]).astype(jnp.int32)
    owner, local, rank = tables(jnp.stack(gathered).reshape(row_count, blocks, LEVELS, per_block), grid)
    row_owners = my_row * col_count + jnp.arange(col_count, dtype=jnp.int32)
    ids = entries(owner, rank, row_owners, capacity, local)
    order = jnp.broadcast_to(jnp.arange(blocks * per_block, dtype=jnp.int32), owner[:1].shape)
    request = entries(owner[:1], rank[:1], jnp.arange(peers, dtype=jnp.int32), capacity, order)[0]

    orders = [[(0, 1)] + column_order(column, col_count) for column in range(col_count)]
    candidates = [sorted({order[slot] for order in orders}) for slot in range(col_count)]
    met = []
    packs = []
    for slot in range(col_count):
        if slot > 1:
            hop(slot)
        columns = [column + order[slot][0] * order[slot][1] for column, order in enumerate(orders)]
        numbers = [candidates[slot].index(order[slot]) for order in orders]
        met.append(columns)
        held = [block if slot == 0 else arrived[candidate] for candidate in candidates[slot]]
        sent = pl.pallas_call(
            functools.partial(
                relay_select_kernel, (row_count - 1, len(held), capacity, sizes, blocks), (columns, numbers)
            ),
            out_shape=[jax.ShapeDtypeStruct((pack, channels), jnp.bfloat16)] * (row_count - 1),
            in_specs=[pl.BlockSpec(memory_space=SMEM)] * 3 + [pl.BlockSpec(memory_space=VMEM)] * len(held),
            out_specs=[pl.BlockSpec(memory_space=VMEM)] * (row_count - 1),
            compiler_params=pltpu.CompilerParams(vmem_limit_bytes=SELECT_VMEM),
        )(place, ids, request, *held)
        for number in range(1, row_count):
            packs.append(
                lax.ppermute(
                    sent[number - 1], "row", [(row, source_of(row, number)) for row in range(row_count)]
                )
            )

    near = [block]
    for step in range(1, col_count):
        near += [arrived[(step, -1)], arrived[(step, 1)]]
    sources = (request, place, ids, *near, *packs)
    spaces = (SMEM, SMEM, SMEM) + (VMEM,) * (len(near) + len(packs))

    def gather(refs, tiles, tile3, sem):
        gather_relay(
            dims,
            (row_count, col_count, partner_of, met),
            refs[0],
            refs[1],
            refs[2],
            refs[3 : 3 + len(near)],
            refs[3 + len(near) :],
            tiles,
            tile3,
        )

    return gather, sources, spaces


def direct_tiles(dims, pack, tile_sets, flat_sets, lists, grid):
    peers, capacity, sizes, _, per_block, heads, head_dim, blocks = dims
    channels = heads * head_dim
    owner, local, rank = tables(lists.reshape(1, blocks, LEVELS, per_block), grid)
    owners = jnp.arange(peers, dtype=jnp.int32)
    order = jnp.broadcast_to(jnp.arange(blocks * per_block, dtype=jnp.int32), owner.shape)
    asked = entries(owner, rank, owners, capacity, local)[0]
    request = entries(owner, rank, owners, capacity, order)[0]
    received = lax.all_to_all(asked, ("row", "col"), split_axis=0, concat_axis=0, tiled=True)
    packs = pl.pallas_call(
        functools.partial(select_kernel, (peers, capacity, sizes)),
        out_shape=jax.ShapeDtypeStruct((peers, pack, channels), jnp.bfloat16),
        in_specs=[pl.BlockSpec(memory_space=SMEM)] + [pl.BlockSpec(memory_space=VMEM)] * 4,
        out_specs=pl.BlockSpec(memory_space=ANY),
        scratch_shapes=[pltpu.SemaphoreType.DMA],
        name="select",
    )(received, tile_sets[0], tile_sets[1], tile_sets[2], flat_sets[3])
    fetched = lax.all_to_all(packs, ("row", "col"), split_axis=0, concat_axis=0, tiled=True)

    def gather(refs, tiles, tile3, sem):
        gather_direct(dims, refs[0], refs[1], tiles, tile3, sem)

    return gather, (request, fetched), (SMEM, ANY)


def on_device(
    queries,
    level_zero,
    level_one,
    level_two,
    level_three,
    tile_lists,
    samples,
    logit_weight,
    logit_bias,
    output_weight,
    output_bias,
    norm_gain,
    norm_shift,
):
    level_blocks = (level_zero, level_one, level_two, level_three)
    row_count = lax.axis_size("row")
    col_count = lax.axis_size("col")
    peers = row_count * col_count
    tile_rows, tile_cols, level_count, per_block = tile_lists.shape
    blocks = tile_rows * tile_cols
    requests = blocks * per_block
    capacity = max(2, (requests + peers - 1) // peers)
    grid_cols = tile_cols * col_count
    channels = level_zero.shape[2]
    width_all = queries.shape[2]
    lanes = samples.shape[2]
    heads = lanes // (LEVELS * POINTS)
    head_dim = channels // heads
    sides = tuple(block.shape[0] // tile_rows for block in level_blocks)
    sizes = tuple(side * side for side in sides)
    pixels = sizes[0]
    tile_sets = [
        to_blocks(level_blocks[level], tile_rows, tile_cols, sides[level]) for level in range(level_count)
    ]

    small = blocks * sizes[3]
    pack = capacity * sum(sizes[:3]) + small
    dims = (peers, capacity, sizes, sides, per_block, heads, head_dim, blocks)
    grid = (tile_rows, tile_cols, grid_cols, col_count, capacity)
    flat_sets = [
        tile_sets[level].reshape(blocks * sizes[level], channels) for level in range(level_count)
    ]
    if peers * capacity <= requests and col_count > 1:
        gather, sources, spaces = relay_tiles(
            dims, row_count, col_count, pack, flat_sets, tile_lists, grid
        )
    else:
        gather, sources, spaces = direct_tiles(
            dims, pack, tile_sets, flat_sets, tile_lists, grid
        )

    queries_blocked = to_blocks(queries, tile_rows, tile_cols, sides[0]).reshape(blocks * pixels, width_all)
    samples_blocked = to_blocks(samples, tile_rows, tile_cols, sides[0]).reshape(blocks * pixels, lanes)
    depth0 = GROUPS[0] * per_block * sides[0]
    depth1 = GROUPS[1] * per_block * sides[1]
    depth2 = per_block * sizes[2] + requests * sizes[3]
    whole = pl.BlockSpec(memory_space=VMEM)
    turned = (blocks, lanes, pixels)
    weight1, weight2, attend, code, down, col = pl.pallas_call(
        functools.partial(prep_kernel, dims),
        out_shape=[
            jax.ShapeDtypeStruct((blocks, heads, POINTS, depth1, pixels), jnp.bfloat16),
            jax.ShapeDtypeStruct((blocks, heads, depth2, pixels), jnp.bfloat16),
            jax.ShapeDtypeStruct(turned, jnp.float32),
            jax.ShapeDtypeStruct(turned, jnp.int32),
            jax.ShapeDtypeStruct(turned, jnp.float32),
            jax.ShapeDtypeStruct(turned, jnp.float32),
        ],
        in_specs=[pl.BlockSpec(memory_space=pltpu.HBM)] * 4,
        out_specs=[whole] * 6,
        scratch_shapes=[
            VMEM((blocks * pixels, width_all), jnp.bfloat16),
            VMEM((lanes, width_all), jnp.bfloat16),
            VMEM((1, lanes), jnp.float32),
            VMEM((blocks * pixels, lanes), jnp.int32),
            pltpu.SemaphoreType.DMA((4,)),
        ],
        compiler_params=pltpu.CompilerParams(vmem_limit_bytes=PREP_VMEM),
        name="prep",
    )(queries_blocked, logit_weight.T, logit_bias.reshape(1, lanes), samples_blocked)
    weight0 = pl.pallas_call(
        functools.partial(hot_kernel, dims),
        out_shape=jax.ShapeDtypeStruct((blocks, heads, POINTS, depth0, pixels), jnp.bfloat16),
        in_specs=[whole] * 3,
        out_specs=whole,
        compiler_params=pltpu.CompilerParams(vmem_limit_bytes=PREP_VMEM),
        name="hot",
    )(attend, code, col)

    attn = pl.pallas_call(
        functools.partial(attend_kernel, dims, grid, gather, len(sources)),
        out_shape=jax.ShapeDtypeStruct((blocks * pixels, channels), jnp.bfloat16),
        in_specs=[pl.BlockSpec(memory_space=space) for space in spaces]
        + [whole] * 4
        + [pl.BlockSpec(memory_space=SMEM)],
        out_specs=whole,
        scratch_shapes=[
            VMEM((requests, sizes[0], channels), jnp.bfloat16),
            VMEM((requests, sizes[1], channels), jnp.bfloat16),
            VMEM((requests, sizes[2], channels), jnp.bfloat16),
            VMEM((peers, small, channels), jnp.bfloat16),
            VMEM((heads, (sides[0] // GROUPS[0] + 1) * head_dim, depth0), jnp.bfloat16),
            VMEM((heads, (sides[1] // GROUPS[1] + 1) * head_dim, depth1), jnp.bfloat16),
            VMEM((channels, depth2), jnp.bfloat16),
            pltpu.SemaphoreType.DMA((LEVELS,)),
        ],
        compiler_params=pltpu.CompilerParams(vmem_limit_bytes=ATTEND_VMEM),
        name="attend",
    )(*sources, weight0, weight1, weight2, down, tile_lists)

    own_head = lax.axis_index("head").reshape(1).astype(jnp.int32)
    other = lax.ppermute(attn, "head", [(0, 1), (1, 0)])
    wide_spec = pl.BlockSpec((pixels, width_all), lambda i: (i, 0))
    slim_spec = pl.BlockSpec((pixels, channels), lambda i: (i, 0))
    matrix_spec = pl.BlockSpec((width_all, width_all), lambda i: (0, 0))
    pre = pl.pallas_call(
        own_kernel,
        out_shape=jax.ShapeDtypeStruct((blocks * pixels, width_all), jnp.float32),
        grid=(blocks,),
        in_specs=[
            pl.BlockSpec(memory_space=SMEM),
            wide_spec,
            slim_spec,
            matrix_spec,
            pl.BlockSpec((1, width_all), lambda i: (0, 0)),
        ],
        out_specs=wide_spec,
        compiler_params=pltpu.CompilerParams(vmem_limit_bytes=SELECT_VMEM),
        name="own",
    )(own_head, queries_blocked, attn, output_weight, output_bias.reshape(1, width_all))
    updated = pl.pallas_call(
        norm_kernel,
        out_shape=jax.ShapeDtypeStruct((blocks * pixels, channels), jnp.bfloat16),
        grid=(blocks,),
        in_specs=[
            pl.BlockSpec(memory_space=SMEM),
            wide_spec,
            slim_spec,
            matrix_spec,
            pl.BlockSpec((1, channels), lambda i: (0, 0)),
            pl.BlockSpec((1, channels), lambda i: (0, 0)),
        ],
        out_specs=slim_spec,
        compiler_params=pltpu.CompilerParams(vmem_limit_bytes=SELECT_VMEM),
        name="norm",
    )(
        own_head,
        pre,
        other,
        output_weight,
        norm_gain.reshape(1, channels),
        norm_shift.reshape(1, channels),
    )
    side = sides[0]
    updated = updated.reshape(tile_rows, tile_cols, side, side, channels).transpose(0, 2, 1, 3, 4)
    return updated.reshape(tile_rows * side, tile_cols * side, channels)


def solution(mesh):
    in_specs = (
        P("row", "col", None),
        P("row", "col", "head"),
        P("row", "col", "head"),
        P("row", "col", "head"),
        P("row", "col", "head"),
        P("row", "col", None, None),
        P("row", "col", "head"),
        P(None, "head"),
        P("head"),
        P(),
        P(),
        P("head"),
        P("head"),
    )
    out_specs = P("row", "col", "head")
    return jax.shard_map(on_device, mesh=mesh, in_specs=in_specs, out_specs=out_specs, check_vma=False)
```

```python
import functools
import jax
import jax.numpy as jnp
from jax import lax
from jax.experimental import pallas as pl
from jax.experimental.pallas import tpu as pltpu
from jax.sharding import PartitionSpec as P

LEVELS = 4
POINTS = 4
ANY = pl.ANY
SMEM = pltpu.SMEM
VMEM = pltpu.VMEM
SELECT_VMEM = 4 * 1024 * 1024
PREP_VMEM = 8 * 1024 * 1024
ATTEND_VMEM = 12 * 1024 * 1024
GROUPS = (2, 4)


def to_blocks(source, tile_rows, tile_cols, tile_side):
    channels = source.shape[2]
    shaped = source.reshape(tile_rows, tile_side, tile_cols, tile_side, channels)
    return shaped.transpose(0, 2, 1, 3, 4).reshape(
        tile_rows * tile_cols, tile_side * tile_side, channels
    )


def hat(position, center):
    return jnp.maximum(1.0 - jnp.abs(position - center), 0.0)


def iota(shape, dim):
    return lax.broadcasted_iota(jnp.int32, shape, dim)


def prep_kernel(
    dims,
    query_hbm,
    logit_hbm,
    bias_hbm,
    sample_hbm,
    weight1,
    weight2,
    attend_ref,
    code_ref,
    down_ref,
    col_ref,
    query_ref,
    logit_ref,
    bias_ref,
    sample_ref,
    sem,
):
    _, _, sizes, sides, per_block, heads, _, blocks = dims
    pixels = sizes[0]
    base2 = per_block * sizes[2]
    lanes = LEVELS * POINTS
    moves = [
        pltpu.make_async_copy(source, target, sem.at[number])
        for number, (source, target) in enumerate(
            (
                (query_hbm, query_ref),
                (logit_hbm, logit_ref),
                (bias_hbm, bias_ref),
                (sample_hbm, sample_ref),
            )
        )
    ]
    for move in moves:
        move.start()
    weight2[...] = jnp.zeros_like(weight2)
    for move in moves:
        move.wait()

    def one(block, carry):
        here = pl.ds(pl.multiple_of(block * pixels, pixels), pixels)
        logits = lax.dot_general(
            query_ref[here, :], logit_ref[...], (((1,), (1,)), ((), ())), preferred_element_type=jnp.float32
        )
        logits = (logits + bias_ref[...]).T
        for head in range(heads):
            part = logits[head * lanes : (head + 1) * lanes, :]
            part = jnp.exp(part - jnp.max(part, axis=0, keepdims=True))
            attend_ref[block, head * lanes : (head + 1) * lanes, :] = part / jnp.sum(
                part, axis=0, keepdims=True
            )
        packed = sample_ref[here, :].T
        level_of = iota(packed.shape, 0) // POINTS % LEVELS
        slot = packed >> 24
        pos_row = (packed >> 12) & 4095
        pos_col = packed & 4095
        deep = jnp.where(level_of == 0, sides[0] * 256 // GROUPS[0], sides[1] * 256 // GROUPS[1])
        group = jnp.zeros_like(packed)
        for bound in range(1, max(GROUPS)):
            group = group + jnp.where(pos_row >= bound * deep, 1, 0)
        group = jnp.where(level_of < 2, group, 0)
        code_ref[block] = slot + group * per_block
        down_ref[block] = (pos_row - group * deep).astype(jnp.float32) * (1.0 / 256.0)
        col_ref[block] = pos_col.astype(jnp.float32) * (1.0 / 256.0)

        for head in range(heads):
            hot_rows(1, block, head, sides, per_block, attend_ref, code_ref, col_ref, weight1)
            side = sides[2]
            size = sizes[2]
            place = iota((size, pixels), 0)
            parts = []
            codes = []
            for point in range(POINTS):
                row = (head * LEVELS + 2) * POINTS + point
                line = slice(row, row + 1)
                parts.append(
                    attend_ref[block, line, :]
                    * hat(down_ref[block, line, :], (place // side).astype(jnp.float32))
                    * hat(col_ref[block, line, :], (place % side).astype(jnp.float32))
                )
                codes.append(code_ref[block, line, :])
            for index in range(per_block):
                mixed = jnp.zeros((size, pixels), jnp.float32)
                for point in range(POINTS):
                    mixed = mixed + jnp.where(codes[point] == index, parts[point], 0.0)
                weight2[block, head, index * size : (index + 1) * size, :] = mixed.astype(jnp.bfloat16)
            side = sides[3]
            size = sizes[3]
            depth = per_block * size
            step = 8 // size
            place = iota((8, pixels), 0)
            parts = []
            codes = []
            for point in range(POINTS):
                row = (head * LEVELS + 3) * POINTS + point
                line = slice(row, row + 1)
                parts.append(
                    attend_ref[block, line, :]
                    * hat(down_ref[block, line, :], (place % size // side).astype(jnp.float32))
                    * hat(col_ref[block, line, :], (place % side).astype(jnp.float32))
                )
                codes.append(code_ref[block, line, :] - place // size)
            stack = []
            for index in range(0, per_block, step):
                mixed = jnp.zeros((8, pixels), jnp.float32)
                for point in range(POINTS):
                    mixed = mixed + jnp.where(codes[point] == index, parts[point], 0.0)
                stack.append(mixed)
            mixed = jnp.concatenate(stack, axis=0)
            weight2[block, head, pl.ds(pl.multiple_of(base2 + block * depth, depth), depth), :] = mixed.astype(
                jnp.bfloat16
            )
        return carry

    lax.fori_loop(0, blocks, one, 0)


def hot_rows(level, block, head, sides, per_block, attend_ref, code_ref, col_ref, weight):
    side = sides[level]
    pixels = attend_ref.shape[2]
    step = 16 // side
    for point in range(POINTS):
        row = (head * LEVELS + level) * POINTS + point
        line = slice(row, row + 1)
        code = code_ref[block, line, :]
        across = attend_ref[block, line, :] * hat(
            col_ref[block, line, :], (iota((16, pixels), 0) % side).astype(jnp.float32)
        )
        for index in range(0, GROUPS[level] * per_block, step):
            wanted = index + iota((16, pixels), 0) // side
            weight[block, head, point, index * side : (index + step) * side, :] = jnp.where(
                code == wanted, across, 0.0
            ).astype(jnp.bfloat16)


def hot_kernel(dims, attend_ref, code_ref, col_ref, weight0):
    _, _, _, sides, per_block, heads, _, blocks = dims

    def one(block, carry):
        for head in range(heads):
            hot_rows(0, block, head, sides, per_block, attend_ref, code_ref, col_ref, weight0)
        return carry

    lax.fori_loop(0, blocks, one, 0)


def select_kernel(dims, ids_ref, zero_ref, one_ref, two_ref, three_ref, out_ref, sem):
    peers, capacity, sizes = dims
    refs = (zero_ref, one_ref, two_ref)

    def copies(peer, make):
        base = 0
        for level in range(LEVELS - 1):
            size = sizes[level]
            for slot in range(capacity):
                index = jnp.maximum(ids_ref[peer, level * capacity + slot], 0)
                make(refs[level].at[index], out_ref.at[peer, base : base + size, :])
                base += size
        make(three_ref, out_ref.at[peer, base : base + three_ref.shape[0], :])

    def start(peer, carry):
        copies(peer, lambda src, dst: pltpu.make_async_copy(src, dst, sem).start())
        return carry

    def finish(peer, carry):
        copies(peer, lambda src, dst: pltpu.make_async_copy(src, dst, sem).wait())
        return carry

    lax.fori_loop(0, peers, start, 0)
    lax.fori_loop(0, peers, finish, 0)


def pick(values, my_column):
    chosen = jnp.int32(values[0])
    for column in range(1, len(values)):
        chosen = jnp.where(my_column == column, values[column], chosen)
    return chosen


def relay_select_kernel(dims, order, place_ref, request_ref, asked_ref, *refs):
    partners, candidates, capacity, sizes, blocks = dims
    ids = refs[:partners]
    sources = refs[partners : partners + candidates]
    outs = refs[partners + candidates :]
    columns, numbers = order
    column = pick(columns, place_ref[1])
    which = pick(numbers, place_ref[1])
    for number, source in enumerate(sources):

        @pl.when(which == number)
        def _(source=source):
            for partner in range(partners):
                base = 0
                start = 0
                for level in range(LEVELS - 1):
                    size = sizes[level]
                    for rank in range(capacity):
                        index = jnp.maximum(ids[partner][column, level * capacity + rank], 0)
                        outs[partner][base : base + size, :] = source[
                            pl.ds(pl.multiple_of(start + index * size, size), size), :
                        ]
                        base += size
                    start += blocks * size
                small = blocks * sizes[3]
                outs[partner][base : base + small, :] = source[start : start + small, :]


def gather_direct(dims, request_ref, fetched_ref, tiles, tile3, sem):
    peers, capacity, sizes, _, _, _, _, _ = dims
    small = tile3.shape[1]
    base3 = capacity * sum(sizes[:3])
    pltpu.make_async_copy(fetched_ref.at[:, base3 : base3 + small, :], tile3, sem.at[LEVELS - 1]).start()

    def start(peer, carry):
        base = 0
        for level in range(LEVELS - 1):
            size = sizes[level]
            for rank in range(capacity):
                fetch_one(
                    request_ref[peer, level * capacity + rank],
                    fetched_ref.at[peer, base : base + size, :],
                    tiles[level],
                    sem.at[level],
                )
                base += size
        return carry

    lax.fori_loop(0, peers, start, 0)
    for level in range(LEVELS - 1):
        pltpu.make_async_copy(tiles[level], tiles[level], sem.at[level]).wait()
    pltpu.make_async_copy(tile3, tile3, sem.at[LEVELS - 1]).wait()


def fetch_one(request, source, tile, sem):
    @pl.when(request >= 0)
    def _():
        pltpu.make_async_copy(source, tile.at[request], sem).start()


def gather_relay(dims, relay, request_ref, place_ref, asked_ref, near_refs, packs_refs, tiles, tile3):
    _, capacity, sizes, _, _, _, _, blocks = dims
    rows, columns, partner_of = relay
    small = tile3.shape[1]
    my_row = place_ref[0]
    my_column = place_ref[1]

    def put(owner, level, rank, source, start):
        request = request_ref[owner, level * capacity + rank]
        size = sizes[level]
        tiles[level][jnp.maximum(request, 0)] = source[pl.ds(start, size), :]

    for name, source in zip(NEAR, near_refs, strict=True):
        held = [-1] * columns
        for buffers, owners in SLOTS:
            for column in range(columns):
                if buffers[column] == name:
                    held[column] = owners[column]
        column = pick(held, my_column)

        @pl.when(column >= 0)
        def _(source=source, column=column):
            owner = my_row * columns + column
            start = 0
            for level in range(LEVELS - 1):
                size = sizes[level]
                for rank in range(capacity):
                    index = jnp.maximum(asked_ref[owner, level * capacity + rank], 0)
                    put(owner, level, rank, source, pl.multiple_of(start + index * size, size))
                start += blocks * size
            tile3[owner] = source[start : start + small, :]

    for number, source in enumerate(packs_refs):
        slot, partner = divmod(number, rows - 1)
        owner = partner_of(my_row, partner + 1) * columns + pick(SLOTS[slot][1], my_column)
        base = 0
        for level in range(LEVELS - 1):
            for rank in range(capacity):
                put(owner, level, rank, source, base)
                base += sizes[level]
        tile3[owner] = source[base : base + small, :]


def attend_kernel(dims, grid, gather, count, *refs):
    sources = refs[:count]
    (
        weight0,
        weight1,
        weight2,
        down_ref,
        lists_ref,
        out_ref,
        tile0,
        tile1,
        tile2,
        tile3,
        left0,
        left1,
        left2,
        sem,
    ) = refs[count:]
    peers, capacity, sizes, sides, per_block, heads, head_dim, blocks = dims
    pixels = sizes[0]
    channels = heads * head_dim
    small = tile3.shape[1]
    base2 = per_block * sizes[2]
    side0, side1 = sides[0], sides[1]

    gather(sources, (tile0, tile1, tile2), tile3, sem)
    left0[...] = jnp.zeros_like(left0)
    flat = tile3[...].reshape(peers * small, channels)
    size3 = sizes[3]
    wide = blocks * per_block * size3
    lane = iota((1, wide), 1)
    target = lane % size3
    tile_rows, tile_cols, grid_cols, col_count, capacity = grid
    for request in range(blocks * per_block):
        block, entry = divmod(request, per_block)
        tile = lists_ref[block // tile_cols, block % tile_cols, LEVELS - 1, entry]
        tile_row = tile // grid_cols
        tile_col = tile % grid_cols
        owner = tile_row // tile_rows * col_count + tile_col // tile_cols
        first = owner * small + (tile_row % tile_rows * tile_cols + tile_col % tile_cols) * size3
        target = target + jnp.where(lane // size3 == request, first, 0)
    chosen = (iota((peers * small, wide), 0) == target).astype(jnp.bfloat16)
    picked = lax.dot_general(flat, chosen, (((0,), (0,)), ((), ())), preferred_element_type=jnp.float32)
    left2[:, base2:] = picked.astype(jnp.bfloat16)

    def one(block, carry):
        mine = pl.ds(block * per_block, per_block)
        reach0 = side0 // GROUPS[0]
        for line in range(side0):
            piece = tile0[mine, line * side0 : (line + 1) * side0, :]
            turned = piece.reshape(per_block * side0, channels).T
            for group in range(GROUPS[0]):
                offset = line - group * reach0
                if 0 <= offset <= reach0:
                    for head in range(heads):
                        left0[
                            head,
                            offset * head_dim : (offset + 1) * head_dim,
                            group * per_block * side0 : (group + 1) * per_block * side0,
                        ] = turned[head * head_dim : (head + 1) * head_dim, :]
        wide1 = tile1[mine].astype(jnp.float32)
        reach1 = side1 // GROUPS[1]
        for offset in range(reach1 + 1):
            stack = []
            for group in range(GROUPS[1]):
                line = min(group * reach1 + offset, side1 - 1)
                stack.append(
                    wide1[:, line * side1 : (line + 1) * side1, :].reshape(per_block * side1, channels)
                )
            turned = jnp.concatenate(stack, axis=0).astype(jnp.bfloat16).T
            for head in range(heads):
                left1[head, offset * head_dim : (offset + 1) * head_dim, :] = turned[
                    head * head_dim : (head + 1) * head_dim, :
                ]
        left2[:, :base2] = tile2[mine].reshape(per_block * sizes[2], channels).T

        for head in range(heads):
            total = jnp.dot(
                left2[head * head_dim : (head + 1) * head_dim, :],
                weight2[block, head],
                preferred_element_type=jnp.float32,
            )
            for level in range(2):
                left = (left0, left1)[level]
                weight = (weight0, weight1)[level]
                for point in range(POINTS):
                    row = (head * LEVELS + level) * POINTS + point
                    product = jnp.dot(left[head], weight[block, head, point], preferred_element_type=jnp.float32)
                    down = down_ref[block, row : row + 1, :]
                    for offset in range(sides[level] // GROUPS[level] + 1):
                        total = total + product[offset * head_dim : (offset + 1) * head_dim, :] * hat(
                            down, float(offset)
                        )
            out_ref[
                pl.ds(pl.multiple_of(block * pixels, pixels), pixels), head * head_dim : (head + 1) * head_dim
            ] = total.T.astype(jnp.bfloat16)
        return carry

    lax.fori_loop(0, blocks, one, 0)


def own_kernel(head_ref, query_ref, own_ref, weight_ref, bias_ref, out_ref):
    channels = own_ref.shape[1]
    rows = weight_ref[pl.ds(pl.multiple_of(head_ref[0] * channels, channels), channels), :]
    pre = query_ref[...].astype(jnp.float32) + bias_ref[...]
    out_ref[...] = pre + jnp.dot(own_ref[...], rows, preferred_element_type=jnp.float32)


def norm_kernel(head_ref, pre_ref, other_ref, weight_ref, gain_ref, shift_ref, out_ref):
    own_head = head_ref[0]
    channels = out_ref.shape[1]
    rows = weight_ref[pl.ds(pl.multiple_of((1 - own_head) * channels, channels), channels), :]
    pre = pre_ref[...] + jnp.dot(other_ref[...], rows, preferred_element_type=jnp.float32)
    centered = pre - jnp.mean(pre, axis=1, keepdims=True)
    variance = jnp.mean(centered * centered, axis=1, keepdims=True)
    own = jnp.where(own_head == 0, centered[:, :channels], centered[:, channels:])
    out_ref[...] = (own * lax.rsqrt(variance + 1e-05) * gain_ref[...] + shift_ref[...]).astype(jnp.bfloat16)


def tables(lists, grid):
    tile_rows, tile_cols, grid_cols, col_count, _ = grid
    count, blocks, level_count, per_block = lists.shape
    requests = blocks * per_block
    wanted = lists.transpose(0, 2, 1, 3).reshape(count, level_count, requests)
    grid_row = wanted // grid_cols
    grid_col = wanted % grid_cols
    owner = grid_row // tile_rows * col_count + grid_col // tile_cols
    local = grid_row % tile_rows * tile_cols + grid_col % tile_cols
    order = jnp.arange(requests, dtype=jnp.int32)
    earlier = (owner[..., :, None] == owner[..., None, :]) & (order[None, :] < order[:, None])
    rank = jnp.sum(earlier.astype(jnp.int32), axis=3)
    return owner, local, rank


def entries(owner, rank, owners, capacity, value):
    slot = jnp.arange(capacity, dtype=jnp.int32)
    hit = (owner[:, None, :, None, :] == owners[None, :, None, None, None]) & (
        rank[:, None, :, None, :] == slot[None, None, None, :, None]
    )
    found = jnp.sum(jnp.where(hit, 1 + value[:, None, :, None, :], 0), axis=4) - 1
    return found.reshape(owner.shape[0], owners.shape[0], -1)


LINE = 4
STEPS = (
    ("first", None, ((0, 1), (1, 0), (2, 3), (3, 2))),
    ("cross", None, ((1, 2), (2, 1))),
    ("out", "cross", ((1, 0), (2, 3))),
    ("over", "first", ((1, 2), (2, 1))),
    ("last", "over", ((1, 0), (2, 3))),
)
NEAR = ("own", "first", "cross", "out", "over", "last")
SLOTS = (
    (("own",) * 4, (0, 1, 2, 3)),
    (("first",) * 4, (1, 0, 3, 2)),
    (("out", "cross", "cross", "out"), (2, 2, 1, 1)),
    (("last", "over", "over", "last"), (3, 3, 0, 0)),
)


def relay_tiles(dims, row_count, col_count, pack, flat_sets, lists, grid):
    peers, capacity, sizes, _, per_block, heads, head_dim, blocks = dims
    channels = heads * head_dim
    my_row = lax.axis_index("row")
    my_column = lax.axis_index("col")
    power = row_count & (row_count - 1) == 0

    def partner_of(row, number):
        return row ^ number if power else (row + number) % row_count

    def source_of(row, number):
        return row ^ number if power else (row + row_count - number) % row_count

    held = {"own": jnp.concatenate(flat_sets, axis=0)}

    def move(name):
        source, pairs = {step[0]: step[1:] for step in STEPS}[name]
        held[name] = lax.ppermute(held[source or "own"], "col", pairs)

    move("first")
    move("cross")
    place = jnp.stack([my_row, my_column]).astype(jnp.int32)
    owner, local, rank = tables(lists.reshape(1, blocks, LEVELS, per_block), grid)
    order = jnp.arange(blocks * per_block, dtype=jnp.int32)
    code = entries(owner, rank, jnp.arange(peers, dtype=jnp.int32), capacity, order * blocks + local)[0]
    asked = jnp.where(code >= 0, code % blocks, -1)
    request = jnp.where(code >= 0, code // blocks, -1)
    by_row = asked.reshape(row_count, col_count, asked.shape[1])
    ids = []
    for number in range(1, row_count):
        mine = jnp.sum(
            jnp.where(
                (jnp.arange(row_count) == partner_of(my_row, number))[:, None, None], by_row, 0
            ),
            axis=0,
        )
        ids.append(
            lax.ppermute(mine, "row", [(row, partner_of(row, number)) for row in range(row_count)])
        )

    packs = []
    for slot, (buffers, columns) in enumerate(SLOTS):
        if slot == 1:
            move("out")
            move("over")
        if slot == 2:
            move("last")
        names = sorted(set(buffers))
        numbers = [names.index(name) for name in buffers]
        sent = pl.pallas_call(
            functools.partial(
                relay_select_kernel, (row_count - 1, len(names), capacity, sizes, blocks), (columns, numbers)
            ),
            out_shape=[jax.ShapeDtypeStruct((pack, channels), jnp.bfloat16)] * (row_count - 1),
            in_specs=[pl.BlockSpec(memory_space=SMEM)] * (row_count + 2)
            + [pl.BlockSpec(memory_space=VMEM)] * len(names),
            out_specs=[pl.BlockSpec(memory_space=VMEM)] * (row_count - 1),
            compiler_params=pltpu.CompilerParams(vmem_limit_bytes=SELECT_VMEM),
        )(place, request, asked, *ids, *[held[name] for name in names])
        for number in range(1, row_count):
            packs.append(
                lax.ppermute(
                    sent[number - 1], "row", [(row, source_of(row, number)) for row in range(row_count)]
                )
            )

    near = [held[name] for name in NEAR]
    sources = (request, place, asked, *near, *packs)
    spaces = (SMEM, SMEM, SMEM) + (VMEM,) * (len(near) + len(packs))

    def gather(refs, tiles, tile3, sem):
        gather_relay(
            dims,
            (row_count, col_count, partner_of),
            refs[0],
            refs[1],
            refs[2],
            refs[3 : 3 + len(near)],
            refs[3 + len(near) :],
            tiles,
            tile3,
        )

    return gather, sources, spaces


def direct_tiles(dims, pack, tile_sets, flat_sets, lists, grid):
    peers, capacity, sizes, _, per_block, heads, head_dim, blocks = dims
    channels = heads * head_dim
    owner, local, rank = tables(lists.reshape(1, blocks, LEVELS, per_block), grid)
    owners = jnp.arange(peers, dtype=jnp.int32)
    order = jnp.broadcast_to(jnp.arange(blocks * per_block, dtype=jnp.int32), owner.shape)
    asked = entries(owner, rank, owners, capacity, local)[0]
    request = entries(owner, rank, owners, capacity, order)[0]
    received = lax.all_to_all(asked, ("row", "col"), split_axis=0, concat_axis=0, tiled=True)
    packs = pl.pallas_call(
        functools.partial(select_kernel, (peers, capacity, sizes)),
        out_shape=jax.ShapeDtypeStruct((peers, pack, channels), jnp.bfloat16),
        in_specs=[pl.BlockSpec(memory_space=SMEM)] + [pl.BlockSpec(memory_space=VMEM)] * 4,
        out_specs=pl.BlockSpec(memory_space=ANY),
        scratch_shapes=[pltpu.SemaphoreType.DMA],
        name="select",
    )(received, tile_sets[0], tile_sets[1], tile_sets[2], flat_sets[3])
    fetched = lax.all_to_all(packs, ("row", "col"), split_axis=0, concat_axis=0, tiled=True)

    def gather(refs, tiles, tile3, sem):
        gather_direct(dims, refs[0], refs[1], tiles, tile3, sem)

    return gather, (request, fetched), (SMEM, ANY)


def on_device(
    queries,
    level_zero,
    level_one,
    level_two,
    level_three,
    tile_lists,
    samples,
    logit_weight,
    logit_bias,
    output_weight,
    output_bias,
    norm_gain,
    norm_shift,
):
    level_blocks = (level_zero, level_one, level_two, level_three)
    row_count = lax.axis_size("row")
    col_count = lax.axis_size("col")
    peers = row_count * col_count
    tile_rows, tile_cols, level_count, per_block = tile_lists.shape
    blocks = tile_rows * tile_cols
    requests = blocks * per_block
    capacity = max(2, (requests + peers - 1) // peers)
    grid_cols = tile_cols * col_count
    channels = level_zero.shape[2]
    width_all = queries.shape[2]
    lanes = samples.shape[2]
    heads = lanes // (LEVELS * POINTS)
    head_dim = channels // heads
    sides = tuple(block.shape[0] // tile_rows for block in level_blocks)
    sizes = tuple(side * side for side in sides)
    pixels = sizes[0]
    tile_sets = [
        to_blocks(level_blocks[level], tile_rows, tile_cols, sides[level]) for level in range(level_count)
    ]

    small = blocks * sizes[3]
    pack = capacity * sum(sizes[:3]) + small
    dims = (peers, capacity, sizes, sides, per_block, heads, head_dim, blocks)
    grid = (tile_rows, tile_cols, grid_cols, col_count, capacity)
    flat_sets = [
        tile_sets[level].reshape(blocks * sizes[level], channels) for level in range(level_count)
    ]
    if peers * capacity <= requests and col_count == LINE:
        gather, sources, spaces = relay_tiles(
            dims, row_count, col_count, pack, flat_sets, tile_lists, grid
        )
    else:
        gather, sources, spaces = direct_tiles(
            dims, pack, tile_sets, flat_sets, tile_lists, grid
        )

    queries_blocked = to_blocks(queries, tile_rows, tile_cols, sides[0]).reshape(blocks * pixels, width_all)
    samples_blocked = to_blocks(samples, tile_rows, tile_cols, sides[0]).reshape(blocks * pixels, lanes)
    depth0 = GROUPS[0] * per_block * sides[0]
    depth1 = GROUPS[1] * per_block * sides[1]
    depth2 = per_block * sizes[2] + requests * sizes[3]
    whole = pl.BlockSpec(memory_space=VMEM)
    turned = (blocks, lanes, pixels)
    weight1, weight2, attend, code, down, col = pl.pallas_call(
        functools.partial(prep_kernel, dims),
        out_shape=[
            jax.ShapeDtypeStruct((blocks, heads, POINTS, depth1, pixels), jnp.bfloat16),
            jax.ShapeDtypeStruct((blocks, heads, depth2, pixels), jnp.bfloat16),
            jax.ShapeDtypeStruct(turned, jnp.float32),
            jax.ShapeDtypeStruct(turned, jnp.int32),
            jax.ShapeDtypeStruct(turned, jnp.float32),
            jax.ShapeDtypeStruct(turned, jnp.float32),
        ],
        in_specs=[pl.BlockSpec(memory_space=pltpu.HBM)] * 4,
        out_specs=[whole] * 6,
        scratch_shapes=[
            VMEM((blocks * pixels, width_all), jnp.bfloat16),
            VMEM((lanes, width_all), jnp.bfloat16),
            VMEM((1, lanes), jnp.float32),
            VMEM((blocks * pixels, lanes), jnp.int32),
            pltpu.SemaphoreType.DMA((4,)),
        ],
        compiler_params=pltpu.CompilerParams(vmem_limit_bytes=PREP_VMEM),
        name="prep",
    )(queries_blocked, logit_weight.T, logit_bias.reshape(1, lanes), samples_blocked)
    weight0 = pl.pallas_call(
        functools.partial(hot_kernel, dims),
        out_shape=jax.ShapeDtypeStruct((blocks, heads, POINTS, depth0, pixels), jnp.bfloat16),
        in_specs=[whole] * 3,
        out_specs=whole,
        compiler_params=pltpu.CompilerParams(vmem_limit_bytes=PREP_VMEM),
        name="hot",
    )(attend, code, col)

    attn = pl.pallas_call(
        functools.partial(attend_kernel, dims, grid, gather, len(sources)),
        out_shape=jax.ShapeDtypeStruct((blocks * pixels, channels), jnp.bfloat16),
        in_specs=[pl.BlockSpec(memory_space=space) for space in spaces]
        + [whole] * 4
        + [pl.BlockSpec(memory_space=SMEM)],
        out_specs=whole,
        scratch_shapes=[
            VMEM((requests, sizes[0], channels), jnp.bfloat16),
            VMEM((requests, sizes[1], channels), jnp.bfloat16),
            VMEM((requests, sizes[2], channels), jnp.bfloat16),
            VMEM((peers, small, channels), jnp.bfloat16),
            VMEM((heads, (sides[0] // GROUPS[0] + 1) * head_dim, depth0), jnp.bfloat16),
            VMEM((heads, (sides[1] // GROUPS[1] + 1) * head_dim, depth1), jnp.bfloat16),
            VMEM((channels, depth2), jnp.bfloat16),
            pltpu.SemaphoreType.DMA((LEVELS,)),
        ],
        compiler_params=pltpu.CompilerParams(vmem_limit_bytes=ATTEND_VMEM),
        name="attend",
    )(*sources, weight0, weight1, weight2, down, tile_lists)

    own_head = lax.axis_index("head").reshape(1).astype(jnp.int32)
    other = lax.ppermute(attn, "head", [(0, 1), (1, 0)])
    wide_spec = pl.BlockSpec((pixels, width_all), lambda i: (i, 0))
    slim_spec = pl.BlockSpec((pixels, channels), lambda i: (i, 0))
    matrix_spec = pl.BlockSpec((width_all, width_all), lambda i: (0, 0))
    pre = pl.pallas_call(
        own_kernel,
        out_shape=jax.ShapeDtypeStruct((blocks * pixels, width_all), jnp.float32),
        grid=(blocks,),
        in_specs=[
            pl.BlockSpec(memory_space=SMEM),
            wide_spec,
            slim_spec,
            matrix_spec,
            pl.BlockSpec((1, width_all), lambda i: (0, 0)),
        ],
        out_specs=wide_spec,
        compiler_params=pltpu.CompilerParams(vmem_limit_bytes=SELECT_VMEM),
        name="own",
    )(own_head, queries_blocked, attn, output_weight, output_bias.reshape(1, width_all))
    updated = pl.pallas_call(
        norm_kernel,
        out_shape=jax.ShapeDtypeStruct((blocks * pixels, channels), jnp.bfloat16),
        grid=(blocks,),
        in_specs=[
            pl.BlockSpec(memory_space=SMEM),
            wide_spec,
            slim_spec,
            matrix_spec,
            pl.BlockSpec((1, channels), lambda i: (0, 0)),
            pl.BlockSpec((1, channels), lambda i: (0, 0)),
        ],
        out_specs=slim_spec,
        compiler_params=pltpu.CompilerParams(vmem_limit_bytes=SELECT_VMEM),
        name="norm",
    )(
        own_head,
        pre,
        other,
        output_weight,
        norm_gain.reshape(1, channels),
        norm_shift.reshape(1, channels),
    )
    side = sides[0]
    updated = updated.reshape(tile_rows, tile_cols, side, side, channels).transpose(0, 2, 1, 3, 4)
    return updated.reshape(tile_rows * side, tile_cols * side, channels)


def solution(mesh):
    in_specs = (
        P("row", "col", None),
        P("row", "col", "head"),
        P("row", "col", "head"),
        P("row", "col", "head"),
        P("row", "col", "head"),
        P("row", "col", None, None),
        P("row", "col", "head"),
        P(None, "head"),
        P("head"),
        P(),
        P(),
        P("head"),
        P("head"),
    )
    out_specs = P("row", "col", "head")
    return jax.shard_map(on_device, mesh=mesh, in_specs=in_specs, out_specs=out_specs, check_vma=False)
```

```python
import functools
import jax
import jax.numpy as jnp
from jax import lax
from jax.experimental import pallas as pl
from jax.experimental.pallas import tpu as pltpu
from jax.sharding import PartitionSpec as P

LEVELS = 4
POINTS = 4
ANY = pl.ANY
SMEM = pltpu.SMEM
VMEM = pltpu.VMEM
SELECT_VMEM = 4 * 1024 * 1024
PREP_VMEM = 8 * 1024 * 1024
ATTEND_VMEM = 12 * 1024 * 1024
GROUPS = (2, 4)


def to_blocks(source, tile_rows, tile_cols, tile_side):
    channels = source.shape[2]
    shaped = source.reshape(tile_rows, tile_side, tile_cols, tile_side, channels)
    return shaped.transpose(0, 2, 1, 3, 4).reshape(
        tile_rows * tile_cols, tile_side * tile_side, channels
    )


def hat(position, center):
    return jnp.maximum(1.0 - jnp.abs(position - center), 0.0)


def iota(shape, dim):
    return lax.broadcasted_iota(jnp.int32, shape, dim)


def prep_kernel(
    dims,
    query_ref,
    logit_ref,
    bias_ref,
    sample_ref,
    weight0,
    weight1,
    weight2,
    down_ref,
    attend_ref,
    code_ref,
    col_ref,
    hot_ref,
):
    _, _, sizes, sides, per_block, heads, _, _ = dims
    block = pl.program_id(0)
    pixels = sizes[0]
    base2 = per_block * sizes[2]
    lanes = LEVELS * POINTS
    logits = lax.dot_general(
        query_ref[...], logit_ref[...], (((1,), (1,)), ((), ())), preferred_element_type=jnp.float32
    )
    logits = (logits + bias_ref[...]).T
    for head in range(heads):
        part = logits[head * lanes : (head + 1) * lanes, :]
        part = jnp.exp(part - jnp.max(part, axis=0, keepdims=True))
        attend_ref[head * lanes : (head + 1) * lanes, :] = part / jnp.sum(part, axis=0, keepdims=True)
    packed = sample_ref[...].T
    level_of = iota(packed.shape, 0) // POINTS % LEVELS
    slot = packed >> 24
    pos_row = (packed >> 12) & 4095
    pos_col = packed & 4095
    deep = jnp.where(level_of == 0, sides[0] * 256 // GROUPS[0], sides[1] * 256 // GROUPS[1])
    group = jnp.zeros_like(packed)
    for bound in range(1, max(GROUPS)):
        group = group + jnp.where(pos_row >= bound * deep, 1, 0)
    group = jnp.where(level_of < 2, group, 0)
    code_ref[...] = slot + group * per_block
    down_ref[0] = (pos_row - group * deep).astype(jnp.float32) * (1.0 / 256.0)
    col_ref[...] = pos_col.astype(jnp.float32) * (1.0 / 256.0)

    def line_of(head, level, point):
        row = (head * LEVELS + level) * POINTS + point
        return slice(row, row + 1)

    def hot_of(head, level, point, rows):
        line = line_of(head, level, point)
        return jnp.where(code_ref[line, :] == iota((rows, pixels), 0), attend_ref[line, :], 0.0)

    weight2[0, :, base2:, :] = jnp.zeros((heads, weight2.shape[2] - base2, pixels), jnp.bfloat16)
    for head in range(heads):
        for level in range(2):
            side = sides[level]
            weight = (weight0, weight1)[level]
            step = 16 // side
            rows = GROUPS[level] * per_block
            for point in range(POINTS):
                hot_ref[point, :rows, :] = hot_of(head, level, point, rows)
                across = hat(
                    col_ref[line_of(head, level, point), :], iota((side, pixels), 0).astype(jnp.float32)
                )
                for index in range(0, rows, step):
                    stack = [hot_ref[point, row : row + 1, :] * across for row in range(index, index + step)]
                    piece = stack[0] if step == 1 else jnp.concatenate(stack, axis=0)
                    weight[0, head, point, index * side : (index + step) * side, :] = piece.astype(
                        jnp.bfloat16
                    )
        for level in (2, 3):
            side = sides[level]
            size = sizes[level]
            step = max(1, 8 // size)
            tall = size * step
            place = iota((tall, pixels), 0)
            parts = []
            for point in range(POINTS):
                line = line_of(head, level, point)
                parts.append(
                    hat(down_ref[0, line, :], (place % size // side).astype(jnp.float32))
                    * hat(col_ref[line, :], (place % side).astype(jnp.float32))
                )
                if step == 1:
                    hot_ref[point, :per_block, :] = hot_of(head, level, point, per_block)
                else:
                    line = line_of(head, level, point)
                    parts[-1] = parts[-1] * attend_ref[line, :]
                    hot_ref[point, :tall, :] = jnp.broadcast_to(
                        code_ref[line, :], (tall, pixels)
                    ).astype(jnp.float32) - (place // size).astype(jnp.float32)
            stack = []
            for index in range(0, per_block, step):
                mixed = jnp.zeros((tall, pixels), jnp.float32)
                for point in range(POINTS):
                    if step == 1:
                        mixed = mixed + hot_ref[point, index : index + 1, :] * parts[point]
                    else:
                        mixed = mixed + jnp.where(hot_ref[point, :tall, :] == float(index), parts[point], 0.0)
                stack.append(mixed)
            if level == 2:
                for index, mixed in enumerate(stack):
                    weight2[0, head, index * tall : (index + 1) * tall, :] = mixed.astype(jnp.bfloat16)
            else:
                depth = per_block * size
                first = pl.multiple_of(base2 + block * depth, depth)
                weight2[0, head, pl.ds(first, depth), :] = jnp.concatenate(stack, axis=0).astype(
                    jnp.bfloat16
                )


def select_kernel(dims, ids_ref, zero_ref, one_ref, two_ref, three_ref, out_ref, sem):
    peers, capacity, sizes = dims
    refs = (zero_ref, one_ref, two_ref)

    def copies(peer, make):
        base = 0
        for level in range(LEVELS - 1):
            size = sizes[level]
            for slot in range(capacity):
                index = jnp.maximum(ids_ref[peer, level * capacity + slot], 0)
                make(refs[level].at[index], out_ref.at[peer, base : base + size, :])
                base += size
        make(three_ref, out_ref.at[peer, base : base + three_ref.shape[0], :])

    def start(peer, carry):
        copies(peer, lambda src, dst: pltpu.make_async_copy(src, dst, sem).start())
        return carry

    def finish(peer, carry):
        copies(peer, lambda src, dst: pltpu.make_async_copy(src, dst, sem).wait())
        return carry

    lax.fori_loop(0, peers, start, 0)
    lax.fori_loop(0, peers, finish, 0)


def pick(values, my_column):
    chosen = jnp.int32(values[0])
    for column in range(1, len(values)):
        chosen = jnp.where(my_column == column, values[column], chosen)
    return chosen


def relay_select_kernel(dims, order, place_ref, request_ref, asked_ref, *refs):
    partners, candidates, capacity, sizes, blocks = dims
    ids = refs[:partners]
    sources = refs[partners : partners + candidates]
    outs = refs[partners + candidates :]
    columns, numbers = order
    column = pick(columns, place_ref[1])
    which = pick(numbers, place_ref[1])
    for number, source in enumerate(sources):

        @pl.when(which == number)
        def _(source=source):
            for partner in range(partners):
                base = 0
                start = 0
                for level in range(LEVELS - 1):
                    size = sizes[level]
                    for rank in range(capacity):
                        index = jnp.maximum(ids[partner][column, level * capacity + rank], 0)
                        outs[partner][base : base + size, :] = source[
                            pl.ds(pl.multiple_of(start + index * size, size), size), :
                        ]
                        base += size
                    start += blocks * size
                small = blocks * sizes[3]
                outs[partner][base : base + small, :] = source[start : start + small, :]


def gather_direct(dims, request_ref, fetched_ref, tiles, tile3, sem):
    peers, capacity, sizes, _, _, _, _, _ = dims
    small = tile3.shape[1]
    base3 = capacity * sum(sizes[:3])
    pltpu.make_async_copy(fetched_ref.at[:, base3 : base3 + small, :], tile3, sem.at[LEVELS - 1]).start()

    def start(peer, carry):
        base = 0
        for level in range(LEVELS - 1):
            size = sizes[level]
            for rank in range(capacity):
                fetch_one(
                    request_ref[peer, level * capacity + rank],
                    fetched_ref.at[peer, base : base + size, :],
                    tiles[level],
                    sem.at[level],
                )
                base += size
        return carry

    lax.fori_loop(0, peers, start, 0)
    for level in range(LEVELS - 1):
        pltpu.make_async_copy(tiles[level], tiles[level], sem.at[level]).wait()
    pltpu.make_async_copy(tile3, tile3, sem.at[LEVELS - 1]).wait()


def fetch_one(request, source, tile, sem):
    @pl.when(request >= 0)
    def _():
        pltpu.make_async_copy(source, tile.at[request], sem).start()


def gather_relay(dims, relay, request_ref, place_ref, asked_ref, near_refs, packs_refs, tiles, tile3):
    _, capacity, sizes, _, _, _, _, blocks = dims
    rows, columns, partner_of = relay
    small = tile3.shape[1]
    my_row = place_ref[0]
    my_column = place_ref[1]

    def put(owner, level, rank, source, start):
        request = request_ref[owner, level * capacity + rank]
        size = sizes[level]
        tiles[level][jnp.maximum(request, 0)] = source[pl.ds(start, size), :]

    for name, source in zip(NEAR, near_refs, strict=True):
        held = [-1] * columns
        for buffers, owners in SLOTS:
            for column in range(columns):
                if buffers[column] == name:
                    held[column] = owners[column]
        column = pick(held, my_column)

        @pl.when(column >= 0)
        def _(source=source, column=column):
            owner = my_row * columns + column
            start = 0
            for level in range(LEVELS - 1):
                size = sizes[level]
                for rank in range(capacity):
                    index = jnp.maximum(asked_ref[owner, level * capacity + rank], 0)
                    put(owner, level, rank, source, pl.multiple_of(start + index * size, size))
                start += blocks * size
            tile3[owner] = source[start : start + small, :]

    for number, source in enumerate(packs_refs):
        slot, partner = divmod(number, rows - 1)
        owner = partner_of(my_row, partner + 1) * columns + pick(SLOTS[slot][1], my_column)
        base = 0
        for level in range(LEVELS - 1):
            for rank in range(capacity):
                put(owner, level, rank, source, base)
                base += sizes[level]
        tile3[owner] = source[base : base + small, :]


def attend_kernel(dims, grid, gather, count, *refs):
    sources = refs[:count]
    (
        weight0,
        weight1,
        weight2,
        down_ref,
        lists_ref,
        out_ref,
        tile0,
        tile1,
        tile2,
        tile3,
        left0,
        left1,
        left2,
        sem,
    ) = refs[count:]
    peers, capacity, sizes, sides, per_block, heads, head_dim, blocks = dims
    pixels = sizes[0]
    channels = heads * head_dim
    small = tile3.shape[1]
    base2 = per_block * sizes[2]
    side0, side1 = sides[0], sides[1]

    gather(sources, (tile0, tile1, tile2), tile3, sem)
    left0[...] = jnp.zeros_like(left0)
    flat = tile3[...].reshape(peers * small, channels)
    size3 = sizes[3]
    wide = blocks * per_block * size3
    lane = iota((1, wide), 1)
    target = lane % size3
    tile_rows, tile_cols, grid_cols, col_count, capacity = grid
    for request in range(blocks * per_block):
        block, entry = divmod(request, per_block)
        tile = lists_ref[block // tile_cols, block % tile_cols, LEVELS - 1, entry]
        tile_row = tile // grid_cols
        tile_col = tile % grid_cols
        owner = tile_row // tile_rows * col_count + tile_col // tile_cols
        first = owner * small + (tile_row % tile_rows * tile_cols + tile_col % tile_cols) * size3
        target = target + jnp.where(lane // size3 == request, first, 0)
    chosen = (iota((peers * small, wide), 0) == target).astype(jnp.bfloat16)
    picked = lax.dot_general(flat, chosen, (((0,), (0,)), ((), ())), preferred_element_type=jnp.float32)
    left2[:, base2:] = picked.astype(jnp.bfloat16)

    def one(block, carry):
        mine = pl.ds(block * per_block, per_block)
        reach0 = side0 // GROUPS[0]
        for line in range(side0):
            piece = tile0[mine, line * side0 : (line + 1) * side0, :]
            turned = piece.reshape(per_block * side0, channels).T
            for group in range(GROUPS[0]):
                offset = line - group * reach0
                if 0 <= offset <= reach0:
                    for head in range(heads):
                        left0[
                            head,
                            offset * head_dim : (offset + 1) * head_dim,
                            group * per_block * side0 : (group + 1) * per_block * side0,
                        ] = turned[head * head_dim : (head + 1) * head_dim, :]
        wide1 = tile1[mine].astype(jnp.float32)
        reach1 = side1 // GROUPS[1]
        for offset in range(reach1 + 1):
            stack = []
            for group in range(GROUPS[1]):
                line = min(group * reach1 + offset, side1 - 1)
                stack.append(
                    wide1[:, line * side1 : (line + 1) * side1, :].reshape(per_block * side1, channels)
                )
            turned = jnp.concatenate(stack, axis=0).astype(jnp.bfloat16).T
            for head in range(heads):
                left1[head, offset * head_dim : (offset + 1) * head_dim, :] = turned[
                    head * head_dim : (head + 1) * head_dim, :
                ]
        left2[:, :base2] = tile2[mine].reshape(per_block * sizes[2], channels).T

        for head in range(heads):
            total = jnp.dot(
                left2[head * head_dim : (head + 1) * head_dim, :],
                weight2[block, head],
                preferred_element_type=jnp.float32,
            )
            for level in range(2):
                left = (left0, left1)[level]
                weight = (weight0, weight1)[level]
                for point in range(POINTS):
                    row = (head * LEVELS + level) * POINTS + point
                    product = jnp.dot(left[head], weight[block, head, point], preferred_element_type=jnp.float32)
                    down = down_ref[block, row : row + 1, :]
                    for offset in range(sides[level] // GROUPS[level] + 1):
                        total = total + product[offset * head_dim : (offset + 1) * head_dim, :] * hat(
                            down, float(offset)
                        )
            out_ref[
                pl.ds(pl.multiple_of(block * pixels, pixels), pixels), head * head_dim : (head + 1) * head_dim
            ] = total.T.astype(jnp.bfloat16)
        return carry

    lax.fori_loop(0, blocks, one, 0)


def own_kernel(head_ref, query_ref, own_ref, weight_ref, bias_ref, out_ref):
    channels = own_ref.shape[1]
    rows = weight_ref[pl.ds(pl.multiple_of(head_ref[0] * channels, channels), channels), :]
    pre = query_ref[...].astype(jnp.float32) + bias_ref[...]
    out_ref[...] = pre + jnp.dot(own_ref[...], rows, preferred_element_type=jnp.float32)


def norm_kernel(head_ref, pre_ref, other_ref, weight_ref, gain_ref, shift_ref, out_ref):
    own_head = head_ref[0]
    channels = out_ref.shape[1]
    rows = weight_ref[pl.ds(pl.multiple_of((1 - own_head) * channels, channels), channels), :]
    pre = pre_ref[...] + jnp.dot(other_ref[...], rows, preferred_element_type=jnp.float32)
    centered = pre - jnp.mean(pre, axis=1, keepdims=True)
    variance = jnp.mean(centered * centered, axis=1, keepdims=True)
    own = jnp.where(own_head == 0, centered[:, :channels], centered[:, channels:])
    out_ref[...] = (own * lax.rsqrt(variance + 1e-05) * gain_ref[...] + shift_ref[...]).astype(jnp.bfloat16)


def tables(lists, grid):
    tile_rows, tile_cols, grid_cols, col_count, _ = grid
    count, blocks, level_count, per_block = lists.shape
    requests = blocks * per_block
    wanted = lists.transpose(0, 2, 1, 3).reshape(count, level_count, requests)
    grid_row = wanted // grid_cols
    grid_col = wanted % grid_cols
    owner = grid_row // tile_rows * col_count + grid_col // tile_cols
    local = grid_row % tile_rows * tile_cols + grid_col % tile_cols
    order = jnp.arange(requests, dtype=jnp.int32)
    earlier = (owner[..., :, None] == owner[..., None, :]) & (order[None, :] < order[:, None])
    rank = jnp.sum(earlier.astype(jnp.int32), axis=3)
    return owner, local, rank


def entries(owner, rank, owners, capacity, value):
    slot = jnp.arange(capacity, dtype=jnp.int32)
    hit = (owner[:, None, :, None, :] == owners[None, :, None, None, None]) & (
        rank[:, None, :, None, :] == slot[None, None, None, :, None]
    )
    found = jnp.sum(jnp.where(hit, 1 + value[:, None, :, None, :], 0), axis=4) - 1
    return found.reshape(owner.shape[0], owners.shape[0], -1)


LINE = 4
SELECT_COST = pl.CostEstimate(flops=500_000_000, bytes_accessed=1_000_000, transcendentals=0)
PREP_COST = pl.CostEstimate(flops=2_000_000_000, bytes_accessed=4_000_000, transcendentals=0)
STEPS = (
    ("first", None, ((0, 1), (1, 0), (2, 3), (3, 2))),
    ("cross", None, ((1, 2), (2, 1))),
    ("out", "cross", ((1, 0), (2, 3))),
    ("over", "first", ((1, 2), (2, 1))),
    ("last", "over", ((1, 0), (2, 3))),
)
NEAR = ("own", "first", "cross", "out", "over", "last")
SLOTS = (
    (("own",) * 4, (0, 1, 2, 3)),
    (("first",) * 4, (1, 0, 3, 2)),
    (("out", "cross", "cross", "out"), (2, 2, 1, 1)),
    (("last", "over", "over", "last"), (3, 3, 0, 0)),
)


def relay_tiles(dims, row_count, col_count, pack, flat_sets, lists, grid):
    peers, capacity, sizes, _, per_block, heads, head_dim, blocks = dims
    channels = heads * head_dim
    my_row = lax.axis_index("row")
    my_column = lax.axis_index("col")
    power = row_count & (row_count - 1) == 0

    def partner_of(row, number):
        return row ^ number if power else (row + number) % row_count

    def source_of(row, number):
        return row ^ number if power else (row + row_count - number) % row_count

    held = {"own": jnp.concatenate(flat_sets, axis=0)}

    def move(name):
        source, pairs = {step[0]: step[1:] for step in STEPS}[name]
        held[name] = lax.ppermute(held[source or "own"], "col", pairs)

    move("first")
    move("cross")
    place = jnp.stack([my_row, my_column]).astype(jnp.int32)
    owner, local, rank = tables(lists.reshape(1, blocks, LEVELS, per_block), grid)
    order = jnp.arange(blocks * per_block, dtype=jnp.int32)
    code = entries(owner, rank, jnp.arange(peers, dtype=jnp.int32), capacity, order * blocks + local)[0]
    asked = jnp.where(code >= 0, code % blocks, -1)
    request = jnp.where(code >= 0, code // blocks, -1)
    by_row = asked.reshape(row_count, col_count, asked.shape[1])
    ids = []
    for number in range(1, row_count):
        mine = jnp.sum(
            jnp.where(
                (jnp.arange(row_count) == partner_of(my_row, number))[:, None, None], by_row, 0
            ),
            axis=0,
        )
        ids.append(
            lax.ppermute(mine, "row", [(row, partner_of(row, number)) for row in range(row_count)])
        )

    packs = []
    for slot, (buffers, columns) in enumerate(SLOTS):
        if slot == 1:
            move("out")
            move("over")
        if slot == 2:
            move("last")
        names = sorted(set(buffers))
        numbers = [names.index(name) for name in buffers]
        sent = pl.pallas_call(
            functools.partial(
                relay_select_kernel, (row_count - 1, len(names), capacity, sizes, blocks), (columns, numbers)
            ),
            out_shape=[jax.ShapeDtypeStruct((pack, channels), jnp.bfloat16)] * (row_count - 1),
            in_specs=[pl.BlockSpec(memory_space=SMEM)] * (row_count + 2)
            + [pl.BlockSpec(memory_space=VMEM)] * len(names),
            out_specs=[pl.BlockSpec(memory_space=VMEM)] * (row_count - 1),
            compiler_params=pltpu.CompilerParams(vmem_limit_bytes=SELECT_VMEM),
            cost_estimate=SELECT_COST,
        )(place, request, asked, *ids, *[held[name] for name in names])
        for number in range(1, row_count):
            packs.append(
                lax.ppermute(
                    sent[number - 1], "row", [(row, source_of(row, number)) for row in range(row_count)]
                )
            )

    near = [held[name] for name in NEAR]
    sources = (request, place, asked, *near, *packs)
    spaces = (SMEM, SMEM, SMEM) + (VMEM,) * (len(near) + len(packs))

    def gather(refs, tiles, tile3, sem):
        gather_relay(
            dims,
            (row_count, col_count, partner_of),
            refs[0],
            refs[1],
            refs[2],
            refs[3 : 3 + len(near)],
            refs[3 + len(near) :],
            tiles,
            tile3,
        )

    return gather, sources, spaces


def direct_tiles(dims, pack, tile_sets, flat_sets, lists, grid):
    peers, capacity, sizes, _, per_block, heads, head_dim, blocks = dims
    channels = heads * head_dim
    owner, local, rank = tables(lists.reshape(1, blocks, LEVELS, per_block), grid)
    owners = jnp.arange(peers, dtype=jnp.int32)
    order = jnp.broadcast_to(jnp.arange(blocks * per_block, dtype=jnp.int32), owner.shape)
    asked = entries(owner, rank, owners, capacity, local)[0]
    request = entries(owner, rank, owners, capacity, order)[0]
    received = lax.all_to_all(asked, ("row", "col"), split_axis=0, concat_axis=0, tiled=True)
    packs = pl.pallas_call(
        functools.partial(select_kernel, (peers, capacity, sizes)),
        out_shape=jax.ShapeDtypeStruct((peers, pack, channels), jnp.bfloat16),
        in_specs=[pl.BlockSpec(memory_space=SMEM)] + [pl.BlockSpec(memory_space=VMEM)] * 4,
        out_specs=pl.BlockSpec(memory_space=ANY),
        scratch_shapes=[pltpu.SemaphoreType.DMA],
        name="select",
    )(received, tile_sets[0], tile_sets[1], tile_sets[2], flat_sets[3])
    fetched = lax.all_to_all(packs, ("row", "col"), split_axis=0, concat_axis=0, tiled=True)

    def gather(refs, tiles, tile3, sem):
        gather_direct(dims, refs[0], refs[1], tiles, tile3, sem)

    return gather, (request, fetched), (SMEM, ANY)


def on_device(
    queries,
    level_zero,
    level_one,
    level_two,
    level_three,
    tile_lists,
    samples,
    logit_weight,
    logit_bias,
    output_weight,
    output_bias,
    norm_gain,
    norm_shift,
):
    level_blocks = (level_zero, level_one, level_two, level_three)
    row_count = lax.axis_size("row")
    col_count = lax.axis_size("col")
    peers = row_count * col_count
    tile_rows, tile_cols, level_count, per_block = tile_lists.shape
    blocks = tile_rows * tile_cols
    requests = blocks * per_block
    capacity = max(2, (requests + peers - 1) // peers)
    grid_cols = tile_cols * col_count
    channels = level_zero.shape[2]
    width_all = queries.shape[2]
    lanes = samples.shape[2]
    heads = lanes // (LEVELS * POINTS)
    head_dim = channels // heads
    sides = tuple(block.shape[0] // tile_rows for block in level_blocks)
    sizes = tuple(side * side for side in sides)
    pixels = sizes[0]
    tile_sets = [
        to_blocks(level_blocks[level], tile_rows, tile_cols, sides[level]) for level in range(level_count)
    ]

    small = blocks * sizes[3]
    pack = capacity * sum(sizes[:3]) + small
    dims = (peers, capacity, sizes, sides, per_block, heads, head_dim, blocks)
    grid = (tile_rows, tile_cols, grid_cols, col_count, capacity)
    flat_sets = [
        tile_sets[level].reshape(blocks * sizes[level], channels) for level in range(level_count)
    ]
    if peers * capacity <= requests and col_count == LINE:
        gather, sources, spaces = relay_tiles(
            dims, row_count, col_count, pack, flat_sets, tile_lists, grid
        )
    else:
        gather, sources, spaces = direct_tiles(
            dims, pack, tile_sets, flat_sets, tile_lists, grid
        )

    queries_blocked = to_blocks(queries, tile_rows, tile_cols, sides[0]).reshape(blocks * pixels, width_all)
    samples_blocked = to_blocks(samples, tile_rows, tile_cols, sides[0]).reshape(blocks * pixels, lanes)
    depth0 = GROUPS[0] * per_block * sides[0]
    depth1 = GROUPS[1] * per_block * sides[1]
    depth2 = per_block * sizes[2] + requests * sizes[3]
    whole = pl.BlockSpec(memory_space=VMEM)
    weights = pl.pallas_call(
        functools.partial(prep_kernel, dims),
        out_shape=[
            jax.ShapeDtypeStruct((blocks, heads, POINTS, depth0, pixels), jnp.bfloat16),
            jax.ShapeDtypeStruct((blocks, heads, POINTS, depth1, pixels), jnp.bfloat16),
            jax.ShapeDtypeStruct((blocks, heads, depth2, pixels), jnp.bfloat16),
            jax.ShapeDtypeStruct((blocks, lanes, pixels), jnp.float32),
        ],
        grid=(blocks,),
        in_specs=[
            pl.BlockSpec((pixels, width_all), lambda i: (i, 0)),
            pl.BlockSpec((lanes, width_all), lambda i: (0, 0)),
            pl.BlockSpec((1, lanes), lambda i: (0, 0)),
            pl.BlockSpec((pixels, lanes), lambda i: (i, 0)),
        ],
        out_specs=[
            pl.BlockSpec((1, heads, POINTS, depth0, pixels), lambda i: (i, 0, 0, 0, 0)),
            pl.BlockSpec((1, heads, POINTS, depth1, pixels), lambda i: (i, 0, 0, 0, 0)),
            pl.BlockSpec((1, heads, depth2, pixels), lambda i: (i, 0, 0, 0)),
            pl.BlockSpec((1, lanes, pixels), lambda i: (i, 0, 0)),
        ],
        scratch_shapes=[
            VMEM((lanes, pixels), jnp.float32),
            VMEM((lanes, pixels), jnp.int32),
            VMEM((lanes, pixels), jnp.float32),
            VMEM((POINTS, max(GROUPS) * per_block, pixels), jnp.float32),
        ],
        compiler_params=pltpu.CompilerParams(vmem_limit_bytes=PREP_VMEM),
        cost_estimate=PREP_COST,
        name="prep",
    )(queries_blocked, logit_weight.T, logit_bias.reshape(1, lanes), samples_blocked)

    attn = pl.pallas_call(
        functools.partial(attend_kernel, dims, grid, gather, len(sources)),
        out_shape=jax.ShapeDtypeStruct((blocks * pixels, channels), jnp.bfloat16),
        in_specs=[pl.BlockSpec(memory_space=space) for space in spaces]
        + [whole] * 4
        + [pl.BlockSpec(memory_space=SMEM)],
        out_specs=whole,
        scratch_shapes=[
            VMEM((requests, sizes[0], channels), jnp.bfloat16),
            VMEM((requests, sizes[1], channels), jnp.bfloat16),
            VMEM((requests, sizes[2], channels), jnp.bfloat16),
            VMEM((peers, small, channels), jnp.bfloat16),
            VMEM((heads, (sides[0] // GROUPS[0] + 1) * head_dim, depth0), jnp.bfloat16),
            VMEM((heads, (sides[1] // GROUPS[1] + 1) * head_dim, depth1), jnp.bfloat16),
            VMEM((channels, depth2), jnp.bfloat16),
            pltpu.SemaphoreType.DMA((LEVELS,)),
        ],
        compiler_params=pltpu.CompilerParams(vmem_limit_bytes=ATTEND_VMEM),
        cost_estimate=PREP_COST,
        name="attend",
    )(*sources, *weights, tile_lists)

    own_head = lax.axis_index("head").reshape(1).astype(jnp.int32)
    other = lax.ppermute(attn, "head", [(0, 1), (1, 0)])
    wide_spec = pl.BlockSpec((pixels, width_all), lambda i: (i, 0))
    slim_spec = pl.BlockSpec((pixels, channels), lambda i: (i, 0))
    matrix_spec = pl.BlockSpec((width_all, width_all), lambda i: (0, 0))
    pre = pl.pallas_call(
        own_kernel,
        out_shape=jax.ShapeDtypeStruct((blocks * pixels, width_all), jnp.float32),
        grid=(blocks,),
        in_specs=[
            pl.BlockSpec(memory_space=SMEM),
            wide_spec,
            slim_spec,
            matrix_spec,
            pl.BlockSpec((1, width_all), lambda i: (0, 0)),
        ],
        out_specs=wide_spec,
        compiler_params=pltpu.CompilerParams(vmem_limit_bytes=SELECT_VMEM),
        name="own",
    )(own_head, queries_blocked, attn, output_weight, output_bias.reshape(1, width_all))
    updated = pl.pallas_call(
        norm_kernel,
        out_shape=jax.ShapeDtypeStruct((blocks * pixels, channels), jnp.bfloat16),
        grid=(blocks,),
        in_specs=[
            pl.BlockSpec(memory_space=SMEM),
            wide_spec,
            slim_spec,
            matrix_spec,
            pl.BlockSpec((1, channels), lambda i: (0, 0)),
            pl.BlockSpec((1, channels), lambda i: (0, 0)),
        ],
        out_specs=slim_spec,
        compiler_params=pltpu.CompilerParams(vmem_limit_bytes=SELECT_VMEM),
        name="norm",
    )(
        own_head,
        pre,
        other,
        output_weight,
        norm_gain.reshape(1, channels),
        norm_shift.reshape(1, channels),
    )
    side = sides[0]
    updated = updated.reshape(tile_rows, tile_cols, side, side, channels).transpose(0, 2, 1, 3, 4)
    return updated.reshape(tile_rows * side, tile_cols * side, channels)


def solution(mesh):
    in_specs = (
        P("row", "col", None),
        P("row", "col", "head"),
        P("row", "col", "head"),
        P("row", "col", "head"),
        P("row", "col", "head"),
        P("row", "col", None, None),
        P("row", "col", "head"),
        P(None, "head"),
        P("head"),
        P(),
        P(),
        P("head"),
        P("head"),
    )
    out_specs = P("row", "col", "head")
    return jax.shard_map(on_device, mesh=mesh, in_specs=in_specs, out_specs=out_specs, check_vma=False)
```

```python
import functools
import jax
import jax.numpy as jnp
from jax import lax
from jax.experimental import pallas as pl
from jax.experimental.pallas import tpu as pltpu
from jax.sharding import PartitionSpec as P

LEVELS = 4
POINTS = 4
ANY = pl.ANY
SMEM = pltpu.SMEM
VMEM = pltpu.VMEM
SELECT_VMEM = 4 * 1024 * 1024
PREP_VMEM = 8 * 1024 * 1024
ATTEND_VMEM = 12 * 1024 * 1024
GROUPS = (2, 4)


def to_blocks(source, tile_rows, tile_cols, tile_side):
    channels = source.shape[2]
    shaped = source.reshape(tile_rows, tile_side, tile_cols, tile_side, channels)
    return shaped.transpose(0, 2, 1, 3, 4).reshape(
        tile_rows * tile_cols, tile_side * tile_side, channels
    )


def hat(position, center):
    return jnp.maximum(1.0 - jnp.abs(position - center), 0.0)


def iota(shape, dim):
    return lax.broadcasted_iota(jnp.int32, shape, dim)


def prep_kernel(
    dims,
    query_ref,
    logit_ref,
    bias_ref,
    sample_ref,
    weight0,
    weight1,
    weight2,
    down_ref,
    attend_ref,
    code_ref,
    col_ref,
    hot_ref,
):
    _, _, sizes, sides, per_block, heads, _, _ = dims
    block = pl.program_id(0)
    pixels = sizes[0]
    base2 = per_block * sizes[2]
    lanes = LEVELS * POINTS
    logits = lax.dot_general(
        query_ref[...], logit_ref[...], (((1,), (1,)), ((), ())), preferred_element_type=jnp.float32
    )
    logits = (logits + bias_ref[...]).T
    for head in range(heads):
        part = logits[head * lanes : (head + 1) * lanes, :]
        part = jnp.exp(part - jnp.max(part, axis=0, keepdims=True))
        attend_ref[head * lanes : (head + 1) * lanes, :] = part / jnp.sum(part, axis=0, keepdims=True)
    packed = sample_ref[...].T
    level_of = iota(packed.shape, 0) // POINTS % LEVELS
    slot = packed >> 24
    pos_row = (packed >> 12) & 4095
    pos_col = packed & 4095
    deep = jnp.where(level_of == 0, sides[0] * 256 // GROUPS[0], sides[1] * 256 // GROUPS[1])
    group = jnp.zeros_like(packed)
    for bound in range(1, max(GROUPS)):
        group = group + jnp.where(pos_row >= bound * deep, 1, 0)
    group = jnp.where(level_of < 2, group, 0)
    code_ref[...] = slot + group * per_block
    down_ref[0] = (pos_row - group * deep).astype(jnp.float32) * (1.0 / 256.0)
    col_ref[...] = pos_col.astype(jnp.float32) * (1.0 / 256.0)

    def line_of(head, level, point):
        row = (head * LEVELS + level) * POINTS + point
        return slice(row, row + 1)

    def hot_of(head, level, point, rows):
        line = line_of(head, level, point)
        return jnp.where(code_ref[line, :] == iota((rows, pixels), 0), attend_ref[line, :], 0.0)

    weight2[0, :, base2:, :] = jnp.zeros((heads, weight2.shape[2] - base2, pixels), jnp.bfloat16)
    for head in range(heads):
        for level in range(2):
            side = sides[level]
            weight = (weight0, weight1)[level]
            step = 16 // side
            rows = GROUPS[level] * per_block
            for point in range(POINTS):
                hot_ref[point, :rows, :] = hot_of(head, level, point, rows)
                across = hat(
                    col_ref[line_of(head, level, point), :], iota((side, pixels), 0).astype(jnp.float32)
                )
                for index in range(0, rows, step):
                    stack = [hot_ref[point, row : row + 1, :] * across for row in range(index, index + step)]
                    piece = stack[0] if step == 1 else jnp.concatenate(stack, axis=0)
                    weight[0, head, point, index * side : (index + step) * side, :] = piece.astype(
                        jnp.bfloat16
                    )
        for level in (2, 3):
            side = sides[level]
            size = sizes[level]
            step = max(1, 8 // size)
            tall = size * step
            place = iota((tall, pixels), 0)
            parts = []
            for point in range(POINTS):
                line = line_of(head, level, point)
                parts.append(
                    hat(down_ref[0, line, :], (place % size // side).astype(jnp.float32))
                    * hat(col_ref[line, :], (place % side).astype(jnp.float32))
                )
                if step == 1:
                    hot_ref[point, :per_block, :] = hot_of(head, level, point, per_block)
                else:
                    line = line_of(head, level, point)
                    parts[-1] = parts[-1] * attend_ref[line, :]
                    hot_ref[point, :tall, :] = jnp.broadcast_to(
                        code_ref[line, :], (tall, pixels)
                    ).astype(jnp.float32) - (place // size).astype(jnp.float32)
            stack = []
            for index in range(0, per_block, step):
                mixed = jnp.zeros((tall, pixels), jnp.float32)
                for point in range(POINTS):
                    if step == 1:
                        mixed = mixed + hot_ref[point, index : index + 1, :] * parts[point]
                    else:
                        mixed = mixed + jnp.where(hot_ref[point, :tall, :] == float(index), parts[point], 0.0)
                stack.append(mixed)
            if level == 2:
                for index, mixed in enumerate(stack):
                    weight2[0, head, index * tall : (index + 1) * tall, :] = mixed.astype(jnp.bfloat16)
            else:
                depth = per_block * size
                first = pl.multiple_of(base2 + block * depth, depth)
                weight2[0, head, pl.ds(first, depth), :] = jnp.concatenate(stack, axis=0).astype(
                    jnp.bfloat16
                )


def load_kernel(*refs):
    count = len(refs) // 2
    sem = refs[-1]
    moves = [
        pltpu.make_async_copy(refs[number], refs[count + number], sem.at[number]) for number in range(count)
    ]
    for move in moves:
        move.start()
    for move in moves:
        move.wait()


def select_kernel(dims, ids_ref, zero_ref, one_ref, two_ref, three_ref, out_ref, sem):
    peers, capacity, sizes = dims
    refs = (zero_ref, one_ref, two_ref)

    def copies(peer, make):
        base = 0
        for level in range(LEVELS - 1):
            size = sizes[level]
            for slot in range(capacity):
                index = jnp.maximum(ids_ref[peer, level * capacity + slot], 0)
                make(refs[level].at[index], out_ref.at[peer, base : base + size, :])
                base += size
        make(three_ref, out_ref.at[peer, base : base + three_ref.shape[0], :])

    def start(peer, carry):
        copies(peer, lambda src, dst: pltpu.make_async_copy(src, dst, sem).start())
        return carry

    def finish(peer, carry):
        copies(peer, lambda src, dst: pltpu.make_async_copy(src, dst, sem).wait())
        return carry

    lax.fori_loop(0, peers, start, 0)
    lax.fori_loop(0, peers, finish, 0)


def pick(values, my_column):
    chosen = jnp.int32(values[0])
    for column in range(1, len(values)):
        chosen = jnp.where(my_column == column, values[column], chosen)
    return chosen


def relay_select_kernel(dims, order, place_ref, request_ref, asked_ref, *refs):
    partners, candidates, capacity, sizes, blocks = dims
    ids = refs[:partners]
    sources = refs[partners : partners + candidates]
    outs = refs[partners + candidates :]
    columns, numbers = order
    column = pick(columns, place_ref[1])
    which = pick(numbers, place_ref[1])
    for number, source in enumerate(sources):

        @pl.when(which == number)
        def _(source=source):
            for partner in range(partners):
                base = 0
                start = 0
                for level in range(LEVELS - 1):
                    size = sizes[level]
                    for rank in range(capacity):
                        index = jnp.maximum(ids[partner][column, level * capacity + rank], 0)
                        outs[partner][base : base + size, :] = source[
                            pl.ds(pl.multiple_of(start + index * size, size), size), :
                        ]
                        base += size
                    start += blocks * size
                small = blocks * sizes[3]
                outs[partner][base : base + small, :] = source[start : start + small, :]


def gather_direct(dims, request_ref, fetched_ref, tiles, tile3, sem):
    peers, capacity, sizes, _, _, _, _, _ = dims
    small = tile3.shape[1]
    base3 = capacity * sum(sizes[:3])
    pltpu.make_async_copy(fetched_ref.at[:, base3 : base3 + small, :], tile3, sem.at[LEVELS - 1]).start()

    def start(peer, carry):
        base = 0
        for level in range(LEVELS - 1):
            size = sizes[level]
            for rank in range(capacity):
                fetch_one(
                    request_ref[peer, level * capacity + rank],
                    fetched_ref.at[peer, base : base + size, :],
                    tiles[level],
                    sem.at[level],
                )
                base += size
        return carry

    lax.fori_loop(0, peers, start, 0)
    for level in range(LEVELS - 1):
        pltpu.make_async_copy(tiles[level], tiles[level], sem.at[level]).wait()
    pltpu.make_async_copy(tile3, tile3, sem.at[LEVELS - 1]).wait()


def fetch_one(request, source, tile, sem):
    @pl.when(request >= 0)
    def _():
        pltpu.make_async_copy(source, tile.at[request], sem).start()


def gather_relay(dims, relay, request_ref, place_ref, asked_ref, near_refs, packs_refs, tiles, tile3):
    _, capacity, sizes, _, _, _, _, blocks = dims
    rows, columns, partner_of = relay
    small = tile3.shape[1]
    my_row = place_ref[0]
    my_column = place_ref[1]

    def put(owner, level, rank, source, start):
        request = request_ref[owner, level * capacity + rank]
        size = sizes[level]
        tiles[level][jnp.maximum(request, 0)] = source[pl.ds(start, size), :]

    for name, source in zip(NEAR, near_refs, strict=True):
        held = [-1] * columns
        for buffers, owners in SLOTS:
            for column in range(columns):
                if buffers[column] == name:
                    held[column] = owners[column]
        column = pick(held, my_column)

        @pl.when(column >= 0)
        def _(source=source, column=column):
            owner = my_row * columns + column
            start = 0
            for level in range(LEVELS - 1):
                size = sizes[level]
                for rank in range(capacity):
                    index = jnp.maximum(asked_ref[owner, level * capacity + rank], 0)
                    put(owner, level, rank, source, pl.multiple_of(start + index * size, size))
                start += blocks * size
            tile3[owner] = source[start : start + small, :]

    for number, source in enumerate(packs_refs):
        slot, partner = divmod(number, rows - 1)
        owner = partner_of(my_row, partner + 1) * columns + pick(SLOTS[slot][1], my_column)
        base = 0
        for level in range(LEVELS - 1):
            for rank in range(capacity):
                put(owner, level, rank, source, base)
                base += sizes[level]
        tile3[owner] = source[base : base + small, :]


def attend_kernel(dims, grid, gather, count, *refs):
    sources = refs[:count]
    (
        weight0,
        weight1,
        weight2,
        down_ref,
        lists_ref,
        out_ref,
        tile0,
        tile1,
        tile2,
        tile3,
        left0,
        left1,
        left2,
        sem,
    ) = refs[count:]
    peers, capacity, sizes, sides, per_block, heads, head_dim, blocks = dims
    pixels = sizes[0]
    channels = heads * head_dim
    small = tile3.shape[1]
    base2 = per_block * sizes[2]
    side0, side1 = sides[0], sides[1]

    gather(sources, (tile0, tile1, tile2), tile3, sem)
    left0[...] = jnp.zeros_like(left0)
    flat = tile3[...].reshape(peers * small, channels)
    size3 = sizes[3]
    wide = blocks * per_block * size3
    lane = iota((1, wide), 1)
    target = lane % size3
    tile_rows, tile_cols, grid_cols, col_count, capacity = grid
    for request in range(blocks * per_block):
        block, entry = divmod(request, per_block)
        tile = lists_ref[block // tile_cols, block % tile_cols, LEVELS - 1, entry]
        tile_row = tile // grid_cols
        tile_col = tile % grid_cols
        owner = tile_row // tile_rows * col_count + tile_col // tile_cols
        first = owner * small + (tile_row % tile_rows * tile_cols + tile_col % tile_cols) * size3
        target = target + jnp.where(lane // size3 == request, first, 0)
    chosen = (iota((peers * small, wide), 0) == target).astype(jnp.bfloat16)
    picked = lax.dot_general(flat, chosen, (((0,), (0,)), ((), ())), preferred_element_type=jnp.float32)
    left2[:, base2:] = picked.astype(jnp.bfloat16)

    def one(block, carry):
        mine = pl.ds(block * per_block, per_block)
        reach0 = side0 // GROUPS[0]
        for line in range(side0):
            piece = tile0[mine, line * side0 : (line + 1) * side0, :]
            turned = piece.reshape(per_block * side0, channels).T
            for group in range(GROUPS[0]):
                offset = line - group * reach0
                if 0 <= offset <= reach0:
                    for head in range(heads):
                        left0[
                            head,
                            offset * head_dim : (offset + 1) * head_dim,
                            group * per_block * side0 : (group + 1) * per_block * side0,
                        ] = turned[head * head_dim : (head + 1) * head_dim, :]
        wide1 = tile1[mine].astype(jnp.float32)
        reach1 = side1 // GROUPS[1]
        for offset in range(reach1 + 1):
            stack = []
            for group in range(GROUPS[1]):
                line = min(group * reach1 + offset, side1 - 1)
                stack.append(
                    wide1[:, line * side1 : (line + 1) * side1, :].reshape(per_block * side1, channels)
                )
            turned = jnp.concatenate(stack, axis=0).astype(jnp.bfloat16).T
            for head in range(heads):
                left1[head, offset * head_dim : (offset + 1) * head_dim, :] = turned[
                    head * head_dim : (head + 1) * head_dim, :
                ]
        left2[:, :base2] = tile2[mine].reshape(per_block * sizes[2], channels).T

        for head in range(heads):
            total = jnp.dot(
                left2[head * head_dim : (head + 1) * head_dim, :],
                weight2[block, head],
                preferred_element_type=jnp.float32,
            )
            for level in range(2):
                left = (left0, left1)[level]
                weight = (weight0, weight1)[level]
                for point in range(POINTS):
                    row = (head * LEVELS + level) * POINTS + point
                    product = jnp.dot(left[head], weight[block, head, point], preferred_element_type=jnp.float32)
                    down = down_ref[block, row : row + 1, :]
                    for offset in range(sides[level] // GROUPS[level] + 1):
                        total = total + product[offset * head_dim : (offset + 1) * head_dim, :] * hat(
                            down, float(offset)
                        )
            out_ref[
                pl.ds(pl.multiple_of(block * pixels, pixels), pixels), head * head_dim : (head + 1) * head_dim
            ] = total.T.astype(jnp.bfloat16)
        return carry

    lax.fori_loop(0, blocks, one, 0)


def own_kernel(head_ref, query_ref, own_ref, weight_ref, bias_ref, out_ref):
    channels = own_ref.shape[1]
    rows = weight_ref[pl.ds(pl.multiple_of(head_ref[0] * channels, channels), channels), :]
    pre = query_ref[...].astype(jnp.float32) + bias_ref[...]
    out_ref[...] = pre + jnp.dot(own_ref[...], rows, preferred_element_type=jnp.float32)


def norm_kernel(head_ref, pre_ref, other_ref, weight_ref, gain_ref, shift_ref, out_ref):
    own_head = head_ref[0]
    channels = out_ref.shape[1]
    rows = weight_ref[pl.ds(pl.multiple_of((1 - own_head) * channels, channels), channels), :]
    pre = pre_ref[...] + jnp.dot(other_ref[...], rows, preferred_element_type=jnp.float32)
    centered = pre - jnp.mean(pre, axis=1, keepdims=True)
    variance = jnp.mean(centered * centered, axis=1, keepdims=True)
    own = jnp.where(own_head == 0, centered[:, :channels], centered[:, channels:])
    out_ref[...] = (own * lax.rsqrt(variance + 1e-05) * gain_ref[...] + shift_ref[...]).astype(jnp.bfloat16)


def tables(lists, grid):
    tile_rows, tile_cols, grid_cols, col_count, _ = grid
    count, blocks, level_count, per_block = lists.shape
    requests = blocks * per_block
    wanted = lists.transpose(0, 2, 1, 3).reshape(count, level_count, requests)
    grid_row = wanted // grid_cols
    grid_col = wanted % grid_cols
    owner = grid_row // tile_rows * col_count + grid_col // tile_cols
    local = grid_row % tile_rows * tile_cols + grid_col % tile_cols
    order = jnp.arange(requests, dtype=jnp.int32)
    earlier = (owner[..., :, None] == owner[..., None, :]) & (order[None, :] < order[:, None])
    rank = jnp.sum(earlier.astype(jnp.int32), axis=3)
    return owner, local, rank


def entries(owner, rank, owners, capacity, value):
    slot = jnp.arange(capacity, dtype=jnp.int32)
    hit = (owner[:, None, :, None, :] == owners[None, :, None, None, None]) & (
        rank[:, None, :, None, :] == slot[None, None, None, :, None]
    )
    found = jnp.sum(jnp.where(hit, 1 + value[:, None, :, None, :], 0), axis=4) - 1
    return found.reshape(owner.shape[0], owners.shape[0], -1)


LINE = 4
SELECT_COST = pl.CostEstimate(flops=500_000_000, bytes_accessed=1_000_000, transcendentals=0)
PREP_COST = pl.CostEstimate(flops=2_000_000_000, bytes_accessed=4_000_000, transcendentals=0)
STEPS = (
    ("first", None, ((0, 1), (1, 0), (2, 3), (3, 2))),
    ("cross", None, ((1, 2), (2, 1))),
    ("out", "cross", ((1, 0), (2, 3))),
    ("over", "first", ((1, 2), (2, 1))),
    ("last", "over", ((1, 0), (2, 3))),
)
NEAR = ("own", "first", "cross", "out", "over", "last")
SLOTS = (
    (("own",) * 4, (0, 1, 2, 3)),
    (("first",) * 4, (1, 0, 3, 2)),
    (("out", "cross", "cross", "out"), (2, 2, 1, 1)),
    (("last", "over", "over", "last"), (3, 3, 0, 0)),
)


def relay_tiles(dims, row_count, col_count, pack, flat_sets, lists, grid):
    peers, capacity, sizes, _, per_block, heads, head_dim, blocks = dims
    channels = heads * head_dim
    my_row = lax.axis_index("row")
    my_column = lax.axis_index("col")
    power = row_count & (row_count - 1) == 0

    def partner_of(row, number):
        return row ^ number if power else (row + number) % row_count

    def source_of(row, number):
        return row ^ number if power else (row + row_count - number) % row_count

    held = {"own": jnp.concatenate(flat_sets, axis=0)}

    def move(name):
        source, pairs = {step[0]: step[1:] for step in STEPS}[name]
        held[name] = lax.ppermute(held[source or "own"], "col", pairs)

    move("first")
    move("cross")
    place = jnp.stack([my_row, my_column]).astype(jnp.int32)
    owner, local, rank = tables(lists.reshape(1, blocks, LEVELS, per_block), grid)
    order = jnp.arange(blocks * per_block, dtype=jnp.int32)
    code = entries(owner, rank, jnp.arange(peers, dtype=jnp.int32), capacity, order * blocks + local)[0]
    asked = jnp.where(code >= 0, code % blocks, -1)
    request = jnp.where(code >= 0, code // blocks, -1)
    by_row = asked.reshape(row_count, col_count, asked.shape[1])
    ids = []
    for number in range(1, row_count):
        mine = jnp.sum(
            jnp.where(
                (jnp.arange(row_count) == partner_of(my_row, number))[:, None, None], by_row, 0
            ),
            axis=0,
        )
        ids.append(
            lax.ppermute(mine, "row", [(row, partner_of(row, number)) for row in range(row_count)])
        )

    packs = []
    for slot, (buffers, columns) in enumerate(SLOTS):
        if slot == 1:
            move("out")
            move("over")
        if slot == 2:
            move("last")
        names = sorted(set(buffers))
        numbers = [names.index(name) for name in buffers]
        sent = pl.pallas_call(
            functools.partial(
                relay_select_kernel, (row_count - 1, len(names), capacity, sizes, blocks), (columns, numbers)
            ),
            out_shape=[jax.ShapeDtypeStruct((pack, channels), jnp.bfloat16)] * (row_count - 1),
            in_specs=[pl.BlockSpec(memory_space=SMEM)] * (row_count + 2)
            + [pl.BlockSpec(memory_space=VMEM)] * len(names),
            out_specs=[pl.BlockSpec(memory_space=VMEM)] * (row_count - 1),
            compiler_params=pltpu.CompilerParams(vmem_limit_bytes=SELECT_VMEM),
            cost_estimate=SELECT_COST,
        )(place, request, asked, *ids, *[held[name] for name in names])
        for number in range(1, row_count):
            packs.append(
                lax.ppermute(
                    sent[number - 1], "row", [(row, source_of(row, number)) for row in range(row_count)]
                )
            )

    near = [held[name] for name in NEAR]
    sources = (request, place, asked, *near, *packs)
    spaces = (SMEM, SMEM, SMEM) + (VMEM,) * (len(near) + len(packs))

    def gather(refs, tiles, tile3, sem):
        gather_relay(
            dims,
            (row_count, col_count, partner_of),
            refs[0],
            refs[1],
            refs[2],
            refs[3 : 3 + len(near)],
            refs[3 + len(near) :],
            tiles,
            tile3,
        )

    return gather, sources, spaces


def direct_tiles(dims, pack, tile_sets, flat_sets, lists, grid):
    peers, capacity, sizes, _, per_block, heads, head_dim, blocks = dims
    channels = heads * head_dim
    owner, local, rank = tables(lists.reshape(1, blocks, LEVELS, per_block), grid)
    owners = jnp.arange(peers, dtype=jnp.int32)
    order = jnp.broadcast_to(jnp.arange(blocks * per_block, dtype=jnp.int32), owner.shape)
    asked = entries(owner, rank, owners, capacity, local)[0]
    request = entries(owner, rank, owners, capacity, order)[0]
    received = lax.all_to_all(asked, ("row", "col"), split_axis=0, concat_axis=0, tiled=True)
    packs = pl.pallas_call(
        functools.partial(select_kernel, (peers, capacity, sizes)),
        out_shape=jax.ShapeDtypeStruct((peers, pack, channels), jnp.bfloat16),
        in_specs=[pl.BlockSpec(memory_space=SMEM)] + [pl.BlockSpec(memory_space=VMEM)] * 4,
        out_specs=pl.BlockSpec(memory_space=ANY),
        scratch_shapes=[pltpu.SemaphoreType.DMA],
        name="select",
    )(received, tile_sets[0], tile_sets[1], tile_sets[2], flat_sets[3])
    fetched = lax.all_to_all(packs, ("row", "col"), split_axis=0, concat_axis=0, tiled=True)

    def gather(refs, tiles, tile3, sem):
        gather_direct(dims, refs[0], refs[1], tiles, tile3, sem)

    return gather, (request, fetched), (SMEM, ANY)


def on_device(
    queries,
    level_zero,
    level_one,
    level_two,
    level_three,
    tile_lists,
    samples,
    logit_weight,
    logit_bias,
    output_weight,
    output_bias,
    norm_gain,
    norm_shift,
):
    level_blocks = (level_zero, level_one, level_two, level_three)
    row_count = lax.axis_size("row")
    col_count = lax.axis_size("col")
    peers = row_count * col_count
    tile_rows, tile_cols, level_count, per_block = tile_lists.shape
    blocks = tile_rows * tile_cols
    requests = blocks * per_block
    capacity = max(2, (requests + peers - 1) // peers)
    grid_cols = tile_cols * col_count
    channels = level_zero.shape[2]
    width_all = queries.shape[2]
    lanes = samples.shape[2]
    heads = lanes // (LEVELS * POINTS)
    head_dim = channels // heads
    sides = tuple(block.shape[0] // tile_rows for block in level_blocks)
    sizes = tuple(side * side for side in sides)
    pixels = sizes[0]
    tile_sets = [
        to_blocks(level_blocks[level], tile_rows, tile_cols, sides[level]) for level in range(level_count)
    ]

    small = blocks * sizes[3]
    pack = capacity * sum(sizes[:3]) + small
    dims = (peers, capacity, sizes, sides, per_block, heads, head_dim, blocks)
    grid = (tile_rows, tile_cols, grid_cols, col_count, capacity)
    flat_sets = [
        tile_sets[level].reshape(blocks * sizes[level], channels) for level in range(level_count)
    ]
    if peers * capacity <= requests and col_count == LINE:
        gather, sources, spaces = relay_tiles(
            dims, row_count, col_count, pack, flat_sets, tile_lists, grid
        )
    else:
        gather, sources, spaces = direct_tiles(
            dims, pack, tile_sets, flat_sets, tile_lists, grid
        )

    queries_blocked = to_blocks(queries, tile_rows, tile_cols, sides[0]).reshape(blocks * pixels, width_all)
    samples_blocked = to_blocks(samples, tile_rows, tile_cols, sides[0]).reshape(blocks * pixels, lanes)
    depth0 = GROUPS[0] * per_block * sides[0]
    depth1 = GROUPS[1] * per_block * sides[1]
    depth2 = per_block * sizes[2] + requests * sizes[3]
    whole = pl.BlockSpec(memory_space=VMEM)
    staged = (queries_blocked, samples_blocked, logit_weight.T)
    queries_blocked, samples_blocked, logit_turned = pl.pallas_call(
        load_kernel,
        out_shape=[jax.ShapeDtypeStruct(array.shape, array.dtype) for array in staged],
        in_specs=[pl.BlockSpec(memory_space=ANY)] * len(staged),
        out_specs=[whole] * len(staged),
        scratch_shapes=[pltpu.SemaphoreType.DMA((len(staged),))],
        compiler_params=pltpu.CompilerParams(vmem_limit_bytes=SELECT_VMEM),
        name="load",
    )(*staged)
    weights = pl.pallas_call(
        functools.partial(prep_kernel, dims),
        out_shape=[
            jax.ShapeDtypeStruct((blocks, heads, POINTS, depth0, pixels), jnp.bfloat16),
            jax.ShapeDtypeStruct((blocks, heads, POINTS, depth1, pixels), jnp.bfloat16),
            jax.ShapeDtypeStruct((blocks, heads, depth2, pixels), jnp.bfloat16),
            jax.ShapeDtypeStruct((blocks, lanes, pixels), jnp.float32),
        ],
        grid=(blocks,),
        in_specs=[
            pl.BlockSpec((pixels, width_all), lambda i: (i, 0)),
            pl.BlockSpec((lanes, width_all), lambda i: (0, 0)),
            pl.BlockSpec((1, lanes), lambda i: (0, 0)),
            pl.BlockSpec((pixels, lanes), lambda i: (i, 0)),
        ],
        out_specs=[
            pl.BlockSpec((1, heads, POINTS, depth0, pixels), lambda i: (i, 0, 0, 0, 0)),
            pl.BlockSpec((1, heads, POINTS, depth1, pixels), lambda i: (i, 0, 0, 0, 0)),
            pl.BlockSpec((1, heads, depth2, pixels), lambda i: (i, 0, 0, 0)),
            pl.BlockSpec((1, lanes, pixels), lambda i: (i, 0, 0)),
        ],
        scratch_shapes=[
            VMEM((lanes, pixels), jnp.float32),
            VMEM((lanes, pixels), jnp.int32),
            VMEM((lanes, pixels), jnp.float32),
            VMEM((POINTS, max(GROUPS) * per_block, pixels), jnp.float32),
        ],
        compiler_params=pltpu.CompilerParams(vmem_limit_bytes=PREP_VMEM),
        cost_estimate=PREP_COST,
        name="prep",
    )(queries_blocked, logit_turned, logit_bias.reshape(1, lanes), samples_blocked)

    attn = pl.pallas_call(
        functools.partial(attend_kernel, dims, grid, gather, len(sources)),
        out_shape=jax.ShapeDtypeStruct((blocks * pixels, channels), jnp.bfloat16),
        in_specs=[pl.BlockSpec(memory_space=space) for space in spaces]
        + [whole] * 4
        + [pl.BlockSpec(memory_space=SMEM)],
        out_specs=whole,
        scratch_shapes=[
            VMEM((requests, sizes[0], channels), jnp.bfloat16),
            VMEM((requests, sizes[1], channels), jnp.bfloat16),
            VMEM((requests, sizes[2], channels), jnp.bfloat16),
            VMEM((peers, small, channels), jnp.bfloat16),
            VMEM((heads, (sides[0] // GROUPS[0] + 1) * head_dim, depth0), jnp.bfloat16),
            VMEM((heads, (sides[1] // GROUPS[1] + 1) * head_dim, depth1), jnp.bfloat16),
            VMEM((channels, depth2), jnp.bfloat16),
            pltpu.SemaphoreType.DMA((LEVELS,)),
        ],
        compiler_params=pltpu.CompilerParams(vmem_limit_bytes=ATTEND_VMEM),
        cost_estimate=PREP_COST,
        name="attend",
    )(*sources, *weights, tile_lists)

    own_head = lax.axis_index("head").reshape(1).astype(jnp.int32)
    other = lax.ppermute(attn, "head", [(0, 1), (1, 0)])
    wide_spec = pl.BlockSpec((pixels, width_all), lambda i: (i, 0))
    slim_spec = pl.BlockSpec((pixels, channels), lambda i: (i, 0))
    matrix_spec = pl.BlockSpec((width_all, width_all), lambda i: (0, 0))
    pre = pl.pallas_call(
        own_kernel,
        out_shape=jax.ShapeDtypeStruct((blocks * pixels, width_all), jnp.float32),
        grid=(blocks,),
        in_specs=[
            pl.BlockSpec(memory_space=SMEM),
            wide_spec,
            slim_spec,
            matrix_spec,
            pl.BlockSpec((1, width_all), lambda i: (0, 0)),
        ],
        out_specs=wide_spec,
        compiler_params=pltpu.CompilerParams(vmem_limit_bytes=SELECT_VMEM),
        name="own",
    )(own_head, queries_blocked, attn, output_weight, output_bias.reshape(1, width_all))
    updated = pl.pallas_call(
        norm_kernel,
        out_shape=jax.ShapeDtypeStruct((blocks * pixels, channels), jnp.bfloat16),
        grid=(blocks,),
        in_specs=[
            pl.BlockSpec(memory_space=SMEM),
            wide_spec,
            slim_spec,
            matrix_spec,
            pl.BlockSpec((1, channels), lambda i: (0, 0)),
            pl.BlockSpec((1, channels), lambda i: (0, 0)),
        ],
        out_specs=slim_spec,
        compiler_params=pltpu.CompilerParams(vmem_limit_bytes=SELECT_VMEM),
        name="norm",
    )(
        own_head,
        pre,
        other,
        output_weight,
        norm_gain.reshape(1, channels),
        norm_shift.reshape(1, channels),
    )
    side = sides[0]
    updated = updated.reshape(tile_rows, tile_cols, side, side, channels).transpose(0, 2, 1, 3, 4)
    return updated.reshape(tile_rows * side, tile_cols * side, channels)


def solution(mesh):
    in_specs = (
        P("row", "col", None),
        P("row", "col", "head"),
        P("row", "col", "head"),
        P("row", "col", "head"),
        P("row", "col", "head"),
        P("row", "col", None, None),
        P("row", "col", "head"),
        P(None, "head"),
        P("head"),
        P(),
        P(),
        P("head"),
        P("head"),
    )
    out_specs = P("row", "col", "head")
    return jax.shard_map(on_device, mesh=mesh, in_specs=in_specs, out_specs=out_specs, check_vma=False)
```

```python
import functools
import jax
import jax.numpy as jnp
from jax import lax
from jax.experimental import pallas as pl
from jax.experimental.pallas import tpu as pltpu
from jax.sharding import PartitionSpec as P

LEVELS = 4
POINTS = 4
ANY = pl.ANY
SMEM = pltpu.SMEM
VMEM = pltpu.VMEM
SELECT_VMEM = 4 * 1024 * 1024
PREP_VMEM = 8 * 1024 * 1024
ATTEND_VMEM = 12 * 1024 * 1024
GROUPS = (2, 4)


def to_blocks(source, tile_rows, tile_cols, tile_side):
    channels = source.shape[2]
    shaped = source.reshape(tile_rows, tile_side, tile_cols, tile_side, channels)
    return shaped.transpose(0, 2, 1, 3, 4).reshape(
        tile_rows * tile_cols, tile_side * tile_side, channels
    )


def hat(position, center):
    return jnp.maximum(1.0 - jnp.abs(position - center), 0.0)


def iota(shape, dim):
    return lax.broadcasted_iota(jnp.int32, shape, dim)


def prep_kernel(
    dims,
    query_ref,
    logit_ref,
    bias_ref,
    sample_ref,
    weight0,
    weight1,
    weight2,
    down_ref,
    attend_ref,
    code_ref,
    col_ref,
    hot_ref,
):
    _, _, sizes, sides, per_block, heads, _, _ = dims
    block = pl.program_id(0)
    pixels = sizes[0]
    base2 = per_block * sizes[2]
    lanes = LEVELS * POINTS
    logits = lax.dot_general(
        query_ref[...], logit_ref[...], (((1,), (1,)), ((), ())), preferred_element_type=jnp.float32
    )
    logits = (logits + bias_ref[...]).T
    for head in range(heads):
        part = logits[head * lanes : (head + 1) * lanes, :]
        part = jnp.exp(part - jnp.max(part, axis=0, keepdims=True))
        attend_ref[head * lanes : (head + 1) * lanes, :] = part / jnp.sum(part, axis=0, keepdims=True)
    packed = sample_ref[...].T
    level_of = iota(packed.shape, 0) // POINTS % LEVELS
    slot = packed >> 24
    pos_row = (packed >> 12) & 4095
    pos_col = packed & 4095
    deep = jnp.where(level_of == 0, sides[0] * 256 // GROUPS[0], sides[1] * 256 // GROUPS[1])
    group = jnp.zeros_like(packed)
    for bound in range(1, max(GROUPS)):
        group = group + jnp.where(pos_row >= bound * deep, 1, 0)
    group = jnp.where(level_of < 2, group, 0)
    code_ref[...] = slot + group * per_block
    down_ref[0] = (pos_row - group * deep).astype(jnp.float32) * (1.0 / 256.0)
    col_ref[...] = pos_col.astype(jnp.float32) * (1.0 / 256.0)

    def line_of(head, level, point):
        row = (head * LEVELS + level) * POINTS + point
        return slice(row, row + 1)

    def hot_of(head, level, point, rows):
        line = line_of(head, level, point)
        return jnp.where(code_ref[line, :] == iota((rows, pixels), 0), attend_ref[line, :], 0.0)

    weight2[0, :, base2:, :] = jnp.zeros((heads, weight2.shape[2] - base2, pixels), jnp.bfloat16)
    for head in range(heads):
        for level in range(2):
            side = sides[level]
            weight = (weight0, weight1)[level]
            step = 16 // side
            rows = GROUPS[level] * per_block
            for point in range(POINTS):
                hot_ref[point, :rows, :] = hot_of(head, level, point, rows)
                across = hat(
                    col_ref[line_of(head, level, point), :], iota((side, pixels), 0).astype(jnp.float32)
                )
                for index in range(0, rows, step):
                    stack = [hot_ref[point, row : row + 1, :] * across for row in range(index, index + step)]
                    piece = stack[0] if step == 1 else jnp.concatenate(stack, axis=0)
                    weight[0, head, point, index * side : (index + step) * side, :] = piece.astype(
                        jnp.bfloat16
                    )
        for level in (2, 3):
            side = sides[level]
            size = sizes[level]
            step = max(1, 8 // size)
            tall = size * step
            place = iota((tall, pixels), 0)
            parts = []
            for point in range(POINTS):
                line = line_of(head, level, point)
                parts.append(
                    hat(down_ref[0, line, :], (place % size // side).astype(jnp.float32))
                    * hat(col_ref[line, :], (place % side).astype(jnp.float32))
                )
                if step == 1:
                    hot_ref[point, :per_block, :] = hot_of(head, level, point, per_block)
                else:
                    line = line_of(head, level, point)
                    parts[-1] = parts[-1] * attend_ref[line, :]
                    hot_ref[point, :tall, :] = jnp.broadcast_to(
                        code_ref[line, :], (tall, pixels)
                    ).astype(jnp.float32) - (place // size).astype(jnp.float32)
            stack = []
            for index in range(0, per_block, step):
                mixed = jnp.zeros((tall, pixels), jnp.float32)
                for point in range(POINTS):
                    if step == 1:
                        mixed = mixed + hot_ref[point, index : index + 1, :] * parts[point]
                    else:
                        mixed = mixed + jnp.where(hot_ref[point, :tall, :] == float(index), parts[point], 0.0)
                stack.append(mixed)
            if level == 2:
                for index, mixed in enumerate(stack):
                    weight2[0, head, index * tall : (index + 1) * tall, :] = mixed.astype(jnp.bfloat16)
            else:
                depth = per_block * size
                first = pl.multiple_of(base2 + block * depth, depth)
                weight2[0, head, pl.ds(first, depth), :] = jnp.concatenate(stack, axis=0).astype(
                    jnp.bfloat16
                )


def load_kernel(*refs):
    count = len(refs) // 2
    sem = refs[-1]
    moves = [
        pltpu.make_async_copy(refs[number], refs[count + number], sem.at[number]) for number in range(count)
    ]
    for move in moves:
        move.start()
    for move in moves:
        move.wait()


def select_kernel(dims, ids_ref, zero_ref, one_ref, two_ref, three_ref, out_ref, sem):
    peers, capacity, sizes = dims
    refs = (zero_ref, one_ref, two_ref)

    def copies(peer, make):
        base = 0
        for level in range(LEVELS - 1):
            size = sizes[level]
            for slot in range(capacity):
                index = jnp.maximum(ids_ref[peer, level * capacity + slot], 0)
                make(refs[level].at[index], out_ref.at[peer, base : base + size, :])
                base += size
        make(three_ref, out_ref.at[peer, base : base + three_ref.shape[0], :])

    def start(peer, carry):
        copies(peer, lambda src, dst: pltpu.make_async_copy(src, dst, sem).start())
        return carry

    def finish(peer, carry):
        copies(peer, lambda src, dst: pltpu.make_async_copy(src, dst, sem).wait())
        return carry

    lax.fori_loop(0, peers, start, 0)
    lax.fori_loop(0, peers, finish, 0)


def pick(values, my_column):
    chosen = jnp.int32(values[0])
    for column in range(1, len(values)):
        chosen = jnp.where(my_column == column, values[column], chosen)
    return chosen


def relay_select_kernel(dims, order, table_ref, *refs):
    partners, candidates, capacity, sizes, blocks = dims
    sources = refs[:candidates]
    outs = refs[candidates:]
    columns, numbers = order
    my_column = table_ref[0, 1]
    column = pick(columns, my_column)
    which = pick(numbers, my_column)
    for number, source in enumerate(sources):

        @pl.when(which == number)
        def _(source=source):
            for partner in range(partners):
                base = 0
                start = 0
                for level in range(LEVELS - 1):
                    size = sizes[level]
                    for rank in range(capacity):
                        index = jnp.maximum(
                            table_ref[1 + partner * LINE + column, level * capacity + rank], 0
                        )
                        outs[partner][base : base + size, :] = source[
                            pl.ds(pl.multiple_of(start + index * size, size), size), :
                        ]
                        base += size
                    start += blocks * size
                small = blocks * sizes[3]
                outs[partner][base : base + small, :] = source[start : start + small, :]


def gather_direct(dims, request_ref, fetched_ref, tiles, tile3, sem):
    peers, capacity, sizes, _, _, _, _, _ = dims
    small = tile3.shape[1]
    base3 = capacity * sum(sizes[:3])
    pltpu.make_async_copy(fetched_ref.at[:, base3 : base3 + small, :], tile3, sem.at[LEVELS - 1]).start()

    def start(peer, carry):
        base = 0
        for level in range(LEVELS - 1):
            size = sizes[level]
            for rank in range(capacity):
                fetch_one(
                    request_ref[peer, level * capacity + rank],
                    fetched_ref.at[peer, base : base + size, :],
                    tiles[level],
                    sem.at[level],
                )
                base += size
        return carry

    lax.fori_loop(0, peers, start, 0)
    for level in range(LEVELS - 1):
        pltpu.make_async_copy(tiles[level], tiles[level], sem.at[level]).wait()
    pltpu.make_async_copy(tile3, tile3, sem.at[LEVELS - 1]).wait()


def fetch_one(request, source, tile, sem):
    @pl.when(request >= 0)
    def _():
        pltpu.make_async_copy(source, tile.at[request], sem).start()


def gather_relay(dims, relay, table_ref, near_refs, packs_refs, tiles, tile3):
    peers, capacity, sizes, _, _, _, _, blocks = dims
    rows, columns, partner_of = relay
    small = tile3.shape[1]
    my_row = table_ref[0, 0]
    my_column = table_ref[0, 1]
    requests = 1 + (rows - 1) * columns
    asked = requests + peers

    def put(owner, level, rank, source, start):
        request = table_ref[requests + owner, level * capacity + rank]
        size = sizes[level]
        tiles[level][jnp.maximum(request, 0)] = source[pl.ds(start, size), :]

    for name, source in zip(NEAR, near_refs, strict=True):
        held = [-1] * columns
        for buffers, owners in SLOTS:
            for column in range(columns):
                if buffers[column] == name:
                    held[column] = owners[column]
        column = pick(held, my_column)

        @pl.when(column >= 0)
        def _(source=source, column=column):
            owner = my_row * columns + column
            start = 0
            for level in range(LEVELS - 1):
                size = sizes[level]
                for rank in range(capacity):
                    index = jnp.maximum(table_ref[asked + owner, level * capacity + rank], 0)
                    put(owner, level, rank, source, pl.multiple_of(start + index * size, size))
                start += blocks * size
            tile3[owner] = source[start : start + small, :]

    for number, source in enumerate(packs_refs):
        slot, partner = divmod(number, rows - 1)
        owner = partner_of(my_row, partner + 1) * columns + pick(SLOTS[slot][1], my_column)
        base = 0
        for level in range(LEVELS - 1):
            for rank in range(capacity):
                put(owner, level, rank, source, base)
                base += sizes[level]
        tile3[owner] = source[base : base + small, :]


def attend_kernel(dims, grid, gather, count, *refs):
    sources = refs[:count]
    (
        weight0,
        weight1,
        weight2,
        down_ref,
        lists_ref,
        out_ref,
        tile0,
        tile1,
        tile2,
        tile3,
        left0,
        left1,
        left2,
        sem,
    ) = refs[count:]
    peers, capacity, sizes, sides, per_block, heads, head_dim, blocks = dims
    pixels = sizes[0]
    channels = heads * head_dim
    small = tile3.shape[1]
    base2 = per_block * sizes[2]
    side0, side1 = sides[0], sides[1]

    gather(sources, (tile0, tile1, tile2), tile3, sem)
    left0[...] = jnp.zeros_like(left0)
    flat = tile3[...].reshape(peers * small, channels)
    size3 = sizes[3]
    wide = blocks * per_block * size3
    lane = iota((1, wide), 1)
    target = lane % size3
    tile_rows, tile_cols, grid_cols, col_count, capacity = grid
    for request in range(blocks * per_block):
        block, entry = divmod(request, per_block)
        tile = lists_ref[block // tile_cols, block % tile_cols, LEVELS - 1, entry]
        tile_row = tile // grid_cols
        tile_col = tile % grid_cols
        owner = tile_row // tile_rows * col_count + tile_col // tile_cols
        first = owner * small + (tile_row % tile_rows * tile_cols + tile_col % tile_cols) * size3
        target = target + jnp.where(lane // size3 == request, first, 0)
    chosen = (iota((peers * small, wide), 0) == target).astype(jnp.bfloat16)
    picked = lax.dot_general(flat, chosen, (((0,), (0,)), ((), ())), preferred_element_type=jnp.float32)
    left2[:, base2:] = picked.astype(jnp.bfloat16)

    def one(block, carry):
        mine = pl.ds(block * per_block, per_block)
        reach0 = side0 // GROUPS[0]
        for line in range(side0):
            piece = tile0[mine, line * side0 : (line + 1) * side0, :]
            turned = piece.reshape(per_block * side0, channels).T
            for group in range(GROUPS[0]):
                offset = line - group * reach0
                if 0 <= offset <= reach0:
                    for head in range(heads):
                        left0[
                            head,
                            offset * head_dim : (offset + 1) * head_dim,
                            group * per_block * side0 : (group + 1) * per_block * side0,
                        ] = turned[head * head_dim : (head + 1) * head_dim, :]
        wide1 = tile1[mine].astype(jnp.float32)
        reach1 = side1 // GROUPS[1]
        for offset in range(reach1 + 1):
            stack = []
            for group in range(GROUPS[1]):
                line = min(group * reach1 + offset, side1 - 1)
                stack.append(
                    wide1[:, line * side1 : (line + 1) * side1, :].reshape(per_block * side1, channels)
                )
            turned = jnp.concatenate(stack, axis=0).astype(jnp.bfloat16).T
            for head in range(heads):
                left1[head, offset * head_dim : (offset + 1) * head_dim, :] = turned[
                    head * head_dim : (head + 1) * head_dim, :
                ]
        left2[:, :base2] = tile2[mine].reshape(per_block * sizes[2], channels).T

        for head in range(heads):
            total = jnp.dot(
                left2[head * head_dim : (head + 1) * head_dim, :],
                weight2[block, head],
                preferred_element_type=jnp.float32,
            )
            for level in range(2):
                left = (left0, left1)[level]
                weight = (weight0, weight1)[level]
                for point in range(POINTS):
                    row = (head * LEVELS + level) * POINTS + point
                    product = jnp.dot(left[head], weight[block, head, point], preferred_element_type=jnp.float32)
                    down = down_ref[block, row : row + 1, :]
                    for offset in range(sides[level] // GROUPS[level] + 1):
                        total = total + product[offset * head_dim : (offset + 1) * head_dim, :] * hat(
                            down, float(offset)
                        )
            out_ref[
                pl.ds(pl.multiple_of(block * pixels, pixels), pixels), head * head_dim : (head + 1) * head_dim
            ] = total.T.astype(jnp.bfloat16)
        return carry

    lax.fori_loop(0, blocks, one, 0)


def own_kernel(head_ref, query_ref, own_ref, weight_ref, bias_ref, out_ref):
    channels = own_ref.shape[1]
    rows = weight_ref[pl.ds(pl.multiple_of(head_ref[0] * channels, channels), channels), :]
    pre = query_ref[...].astype(jnp.float32) + bias_ref[...]
    out_ref[...] = pre + jnp.dot(own_ref[...], rows, preferred_element_type=jnp.float32)


def norm_kernel(head_ref, pre_ref, other_ref, weight_ref, gain_ref, shift_ref, out_ref):
    own_head = head_ref[0]
    pixels, channels = out_ref.shape
    here = pl.ds(pl.multiple_of(pl.program_id(0) * pixels, pixels), pixels)
    rows = weight_ref[pl.ds(pl.multiple_of((1 - own_head) * channels, channels), channels), :]
    pre = pre_ref[here, :] + jnp.dot(other_ref[here, :], rows, preferred_element_type=jnp.float32)
    centered = pre - jnp.mean(pre, axis=1, keepdims=True)
    variance = jnp.mean(centered * centered, axis=1, keepdims=True)
    own = jnp.where(own_head == 0, centered[:, :channels], centered[:, channels:])
    out_ref[...] = (own * lax.rsqrt(variance + 1e-05) * gain_ref[...] + shift_ref[...]).astype(jnp.bfloat16)


def tables(lists, grid):
    tile_rows, tile_cols, grid_cols, col_count, _ = grid
    count, blocks, level_count, per_block = lists.shape
    requests = blocks * per_block
    wanted = lists.transpose(0, 2, 1, 3).reshape(count, level_count, requests)
    grid_row = wanted // grid_cols
    grid_col = wanted % grid_cols
    owner = grid_row // tile_rows * col_count + grid_col // tile_cols
    local = grid_row % tile_rows * tile_cols + grid_col % tile_cols
    order = jnp.arange(requests, dtype=jnp.int32)
    earlier = (owner[..., :, None] == owner[..., None, :]) & (order[None, :] < order[:, None])
    rank = jnp.sum(earlier.astype(jnp.int32), axis=3)
    return owner, local, rank


def entries(owner, rank, owners, capacity, value):
    slot = jnp.arange(capacity, dtype=jnp.int32)
    hit = (owner[:, None, :, None, :] == owners[None, :, None, None, None]) & (
        rank[:, None, :, None, :] == slot[None, None, None, :, None]
    )
    found = jnp.sum(jnp.where(hit, 1 + value[:, None, :, None, :], 0), axis=4) - 1
    return found.reshape(owner.shape[0], owners.shape[0], -1)


LINE = 4
SELECT_COST = pl.CostEstimate(flops=500_000_000, bytes_accessed=1_000_000, transcendentals=0)
PREP_COST = pl.CostEstimate(flops=2_000_000_000, bytes_accessed=4_000_000, transcendentals=0)
STEPS = (
    ("first", None, ((0, 1), (1, 0), (2, 3), (3, 2))),
    ("cross", None, ((1, 2), (2, 1))),
    ("out", "cross", ((1, 0), (2, 3))),
    ("over", "first", ((1, 2), (2, 1))),
    ("last", "over", ((1, 0), (2, 3))),
)
NEAR = ("own", "first", "cross", "out", "over", "last")
SLOTS = (
    (("own",) * 4, (0, 1, 2, 3)),
    (("first",) * 4, (1, 0, 3, 2)),
    (("out", "cross", "cross", "out"), (2, 2, 1, 1)),
    (("last", "over", "over", "last"), (3, 3, 0, 0)),
)


def relay_tiles(dims, row_count, col_count, pack, flat_sets, lists, grid):
    peers, capacity, sizes, _, per_block, heads, head_dim, blocks = dims
    channels = heads * head_dim
    my_row = lax.axis_index("row")
    my_column = lax.axis_index("col")
    power = row_count & (row_count - 1) == 0

    def partner_of(row, number):
        return row ^ number if power else (row + number) % row_count

    def source_of(row, number):
        return row ^ number if power else (row + row_count - number) % row_count

    held = {"own": jnp.concatenate(flat_sets, axis=0)}

    def move(name):
        source, pairs = {step[0]: step[1:] for step in STEPS}[name]
        held[name] = lax.ppermute(held[source or "own"], "col", pairs)

    move("first")
    move("cross")
    owner, local, rank = tables(lists.reshape(1, blocks, LEVELS, per_block), grid)
    order = jnp.arange(blocks * per_block, dtype=jnp.int32)
    code = entries(owner, rank, jnp.arange(peers, dtype=jnp.int32), capacity, order * blocks + local)[0]
    asked = jnp.where(code >= 0, code % blocks, -1)
    request = jnp.where(code >= 0, code // blocks, -1)
    by_row = asked.reshape(row_count, col_count, asked.shape[1])
    ids = []
    for number in range(1, row_count):
        mine = jnp.sum(
            jnp.where(
                (jnp.arange(row_count) == partner_of(my_row, number))[:, None, None], by_row, 0
            ),
            axis=0,
        )
        ids.append(
            lax.ppermute(mine, "row", [(row, partner_of(row, number)) for row in range(row_count)])
        )

    width = asked.shape[1]
    lane = jnp.arange(width)[None, :]
    place = jnp.where(lane == 0, my_row, my_column).astype(jnp.int32)
    table = jnp.concatenate([place, *ids, request, asked], axis=0)
    packs = []
    for slot, (buffers, columns) in enumerate(SLOTS):
        if slot == 1:
            move("out")
            move("over")
        if slot == 2:
            move("last")
        names = sorted(set(buffers))
        numbers = [names.index(name) for name in buffers]
        sent = pl.pallas_call(
            functools.partial(
                relay_select_kernel, (row_count - 1, len(names), capacity, sizes, blocks), (columns, numbers)
            ),
            out_shape=[jax.ShapeDtypeStruct((pack, channels), jnp.bfloat16)] * (row_count - 1),
            in_specs=[pl.BlockSpec(memory_space=SMEM)] + [pl.BlockSpec(memory_space=VMEM)] * len(names),
            out_specs=[pl.BlockSpec(memory_space=VMEM)] * (row_count - 1),
            compiler_params=pltpu.CompilerParams(vmem_limit_bytes=SELECT_VMEM),
            cost_estimate=SELECT_COST,
        )(table, *[held[name] for name in names])
        for number in range(1, row_count):
            packs.append(
                lax.ppermute(
                    sent[number - 1], "row", [(row, source_of(row, number)) for row in range(row_count)]
                )
            )

    near = [held[name] for name in NEAR]
    sources = (table, *near, *packs)
    spaces = (SMEM,) + (VMEM,) * (len(near) + len(packs))

    def gather(refs, tiles, tile3, sem):
        gather_relay(
            dims,
            (row_count, col_count, partner_of),
            refs[0],
            refs[1 : 1 + len(near)],
            refs[1 + len(near) :],
            tiles,
            tile3,
        )

    return gather, sources, spaces


def direct_tiles(dims, pack, tile_sets, flat_sets, lists, grid):
    peers, capacity, sizes, _, per_block, heads, head_dim, blocks = dims
    channels = heads * head_dim
    owner, local, rank = tables(lists.reshape(1, blocks, LEVELS, per_block), grid)
    owners = jnp.arange(peers, dtype=jnp.int32)
    order = jnp.broadcast_to(jnp.arange(blocks * per_block, dtype=jnp.int32), owner.shape)
    asked = entries(owner, rank, owners, capacity, local)[0]
    request = entries(owner, rank, owners, capacity, order)[0]
    received = lax.all_to_all(asked, ("row", "col"), split_axis=0, concat_axis=0, tiled=True)
    packs = pl.pallas_call(
        functools.partial(select_kernel, (peers, capacity, sizes)),
        out_shape=jax.ShapeDtypeStruct((peers, pack, channels), jnp.bfloat16),
        in_specs=[pl.BlockSpec(memory_space=SMEM)] + [pl.BlockSpec(memory_space=VMEM)] * 4,
        out_specs=pl.BlockSpec(memory_space=ANY),
        scratch_shapes=[pltpu.SemaphoreType.DMA],
        name="select",
    )(received, tile_sets[0], tile_sets[1], tile_sets[2], flat_sets[3])
    fetched = lax.all_to_all(packs, ("row", "col"), split_axis=0, concat_axis=0, tiled=True)

    def gather(refs, tiles, tile3, sem):
        gather_direct(dims, refs[0], refs[1], tiles, tile3, sem)

    return gather, (request, fetched), (SMEM, ANY)


def on_device(
    queries,
    level_zero,
    level_one,
    level_two,
    level_three,
    tile_lists,
    samples,
    logit_weight,
    logit_bias,
    output_weight,
    output_bias,
    norm_gain,
    norm_shift,
):
    level_blocks = (level_zero, level_one, level_two, level_three)
    row_count = lax.axis_size("row")
    col_count = lax.axis_size("col")
    peers = row_count * col_count
    tile_rows, tile_cols, level_count, per_block = tile_lists.shape
    blocks = tile_rows * tile_cols
    requests = blocks * per_block
    capacity = max(2, (requests + peers - 1) // peers)
    grid_cols = tile_cols * col_count
    channels = level_zero.shape[2]
    width_all = queries.shape[2]
    lanes = samples.shape[2]
    heads = lanes // (LEVELS * POINTS)
    head_dim = channels // heads
    sides = tuple(block.shape[0] // tile_rows for block in level_blocks)
    sizes = tuple(side * side for side in sides)
    pixels = sizes[0]
    tile_sets = [
        to_blocks(level_blocks[level], tile_rows, tile_cols, sides[level]) for level in range(level_count)
    ]

    small = blocks * sizes[3]
    pack = capacity * sum(sizes[:3]) + small
    dims = (peers, capacity, sizes, sides, per_block, heads, head_dim, blocks)
    grid = (tile_rows, tile_cols, grid_cols, col_count, capacity)
    flat_sets = [
        tile_sets[level].reshape(blocks * sizes[level], channels) for level in range(level_count)
    ]
    if peers * capacity <= requests and col_count == LINE:
        gather, sources, spaces = relay_tiles(
            dims, row_count, col_count, pack, flat_sets, tile_lists, grid
        )
    else:
        gather, sources, spaces = direct_tiles(
            dims, pack, tile_sets, flat_sets, tile_lists, grid
        )

    queries_blocked = to_blocks(queries, tile_rows, tile_cols, sides[0]).reshape(blocks * pixels, width_all)
    samples_blocked = to_blocks(samples, tile_rows, tile_cols, sides[0]).reshape(blocks * pixels, lanes)
    depth0 = GROUPS[0] * per_block * sides[0]
    depth1 = GROUPS[1] * per_block * sides[1]
    depth2 = per_block * sizes[2] + requests * sizes[3]
    whole = pl.BlockSpec(memory_space=VMEM)
    staged = (queries_blocked, samples_blocked, logit_weight.T)
    queries_blocked, samples_blocked, logit_turned = pl.pallas_call(
        load_kernel,
        out_shape=[jax.ShapeDtypeStruct(array.shape, array.dtype) for array in staged],
        in_specs=[pl.BlockSpec(memory_space=ANY)] * len(staged),
        out_specs=[whole] * len(staged),
        scratch_shapes=[pltpu.SemaphoreType.DMA((len(staged),))],
        compiler_params=pltpu.CompilerParams(vmem_limit_bytes=SELECT_VMEM),
        name="load",
    )(*staged)
    weights = pl.pallas_call(
        functools.partial(prep_kernel, dims),
        out_shape=[
            jax.ShapeDtypeStruct((blocks, heads, POINTS, depth0, pixels), jnp.bfloat16),
            jax.ShapeDtypeStruct((blocks, heads, POINTS, depth1, pixels), jnp.bfloat16),
            jax.ShapeDtypeStruct((blocks, heads, depth2, pixels), jnp.bfloat16),
            jax.ShapeDtypeStruct((blocks, lanes, pixels), jnp.float32),
        ],
        grid=(blocks,),
        in_specs=[
            pl.BlockSpec((pixels, width_all), lambda i: (i, 0)),
            pl.BlockSpec((lanes, width_all), lambda i: (0, 0)),
            pl.BlockSpec((1, lanes), lambda i: (0, 0)),
            pl.BlockSpec((pixels, lanes), lambda i: (i, 0)),
        ],
        out_specs=[
            pl.BlockSpec((1, heads, POINTS, depth0, pixels), lambda i: (i, 0, 0, 0, 0)),
            pl.BlockSpec((1, heads, POINTS, depth1, pixels), lambda i: (i, 0, 0, 0, 0)),
            pl.BlockSpec((1, heads, depth2, pixels), lambda i: (i, 0, 0, 0)),
            pl.BlockSpec((1, lanes, pixels), lambda i: (i, 0, 0)),
        ],
        scratch_shapes=[
            VMEM((lanes, pixels), jnp.float32),
            VMEM((lanes, pixels), jnp.int32),
            VMEM((lanes, pixels), jnp.float32),
            VMEM((POINTS, max(GROUPS) * per_block, pixels), jnp.float32),
        ],
        compiler_params=pltpu.CompilerParams(vmem_limit_bytes=PREP_VMEM),
        cost_estimate=PREP_COST,
        name="prep",
    )(queries_blocked, logit_turned, logit_bias.reshape(1, lanes), samples_blocked)

    attn = pl.pallas_call(
        functools.partial(attend_kernel, dims, grid, gather, len(sources)),
        out_shape=jax.ShapeDtypeStruct((blocks * pixels, channels), jnp.bfloat16),
        in_specs=[pl.BlockSpec(memory_space=space) for space in spaces]
        + [whole] * 4
        + [pl.BlockSpec(memory_space=SMEM)],
        out_specs=whole,
        scratch_shapes=[
            VMEM((requests, sizes[0], channels), jnp.bfloat16),
            VMEM((requests, sizes[1], channels), jnp.bfloat16),
            VMEM((requests, sizes[2], channels), jnp.bfloat16),
            VMEM((peers, small, channels), jnp.bfloat16),
            VMEM((heads, (sides[0] // GROUPS[0] + 1) * head_dim, depth0), jnp.bfloat16),
            VMEM((heads, (sides[1] // GROUPS[1] + 1) * head_dim, depth1), jnp.bfloat16),
            VMEM((channels, depth2), jnp.bfloat16),
            pltpu.SemaphoreType.DMA((LEVELS,)),
        ],
        compiler_params=pltpu.CompilerParams(vmem_limit_bytes=ATTEND_VMEM),
        cost_estimate=PREP_COST,
        name="attend",
    )(*sources, *weights, tile_lists)

    own_head = lax.axis_index("head").reshape(1).astype(jnp.int32)
    other = lax.ppermute(attn, "head", [(0, 1), (1, 0)])
    wide_spec = pl.BlockSpec((pixels, width_all), lambda i: (i, 0))
    slim_spec = pl.BlockSpec((pixels, channels), lambda i: (i, 0))
    matrix_spec = pl.BlockSpec((width_all, width_all), lambda i: (0, 0))
    pre = pl.pallas_call(
        own_kernel,
        out_shape=jax.ShapeDtypeStruct((blocks * pixels, width_all), jnp.float32),
        grid=(blocks,),
        in_specs=[
            pl.BlockSpec(memory_space=SMEM),
            wide_spec,
            slim_spec,
            matrix_spec,
            pl.BlockSpec((1, width_all), lambda i: (0, 0)),
        ],
        out_specs=wide_spec,
        compiler_params=pltpu.CompilerParams(vmem_limit_bytes=SELECT_VMEM),
        name="own",
    )(own_head, queries_blocked, attn, output_weight, output_bias.reshape(1, width_all))
    updated = pl.pallas_call(
        norm_kernel,
        out_shape=jax.ShapeDtypeStruct((blocks * pixels, channels), jnp.bfloat16),
        grid=(blocks,),
        in_specs=[pl.BlockSpec(memory_space=SMEM)] + [whole] * 5,
        out_specs=slim_spec,
        compiler_params=pltpu.CompilerParams(vmem_limit_bytes=SELECT_VMEM),
        name="norm",
    )(
        own_head,
        pre,
        other,
        output_weight,
        norm_gain.reshape(1, channels),
        norm_shift.reshape(1, channels),
    )
    side = sides[0]
    updated = updated.reshape(tile_rows, tile_cols, side, side, channels).transpose(0, 2, 1, 3, 4)
    return updated.reshape(tile_rows * side, tile_cols * side, channels)


def solution(mesh):
    in_specs = (
        P("row", "col", None),
        P("row", "col", "head"),
        P("row", "col", "head"),
        P("row", "col", "head"),
        P("row", "col", "head"),
        P("row", "col", None, None),
        P("row", "col", "head"),
        P(None, "head"),
        P("head"),
        P(),
        P(),
        P("head"),
        P("head"),
    )
    out_specs = P("row", "col", "head")
    return jax.shard_map(on_device, mesh=mesh, in_specs=in_specs, out_specs=out_specs, check_vma=False)
```

```python
import functools
import jax
import jax.numpy as jnp
from jax import lax
from jax.experimental import pallas as pl
from jax.experimental.pallas import tpu as pltpu
from jax.sharding import PartitionSpec as P

LEVELS = 4
POINTS = 4
ANY = pl.ANY
SMEM = pltpu.SMEM
VMEM = pltpu.VMEM
SELECT_VMEM = 4 * 1024 * 1024
PREP_VMEM = 8 * 1024 * 1024
ATTEND_VMEM = 12 * 1024 * 1024
GROUPS = (2, 2)


def to_blocks(source, tile_rows, tile_cols, tile_side):
    channels = source.shape[2]
    shaped = source.reshape(tile_rows, tile_side, tile_cols, tile_side, channels)
    return shaped.transpose(0, 2, 1, 3, 4).reshape(
        tile_rows * tile_cols, tile_side * tile_side, channels
    )


def hat(position, center):
    return jnp.maximum(1.0 - jnp.abs(position - center), 0.0)


def iota(shape, dim):
    return lax.broadcasted_iota(jnp.int32, shape, dim)


def prep_kernel(
    dims,
    query_ref,
    logit_ref,
    bias_ref,
    sample_ref,
    weight0,
    weight1,
    weight2,
    down_ref,
    attend_ref,
    code_ref,
    col_ref,
    hot_ref,
):
    _, _, sizes, sides, per_block, heads, _, _ = dims
    block = pl.program_id(0)
    pixels = sizes[0]
    base2 = per_block * sizes[2]
    lanes = LEVELS * POINTS
    logits = lax.dot_general(
        query_ref[...], logit_ref[...], (((1,), (1,)), ((), ())), preferred_element_type=jnp.float32
    )
    logits = (logits + bias_ref[...]).T
    for head in range(heads):
        part = logits[head * lanes : (head + 1) * lanes, :]
        part = jnp.exp(part - jnp.max(part, axis=0, keepdims=True))
        attend_ref[head * lanes : (head + 1) * lanes, :] = part / jnp.sum(part, axis=0, keepdims=True)
    packed = sample_ref[...].T
    level_of = iota(packed.shape, 0) // POINTS % LEVELS
    slot = packed >> 24
    pos_row = (packed >> 12) & 4095
    pos_col = packed & 4095
    deep = jnp.where(level_of == 0, sides[0] * 256 // GROUPS[0], sides[1] * 256 // GROUPS[1])
    group = jnp.zeros_like(packed)
    for bound in range(1, max(GROUPS)):
        group = group + jnp.where(pos_row >= bound * deep, 1, 0)
    group = jnp.where(level_of < 2, group, 0)
    code_ref[...] = slot + group * per_block
    down_ref[0] = (pos_row - group * deep).astype(jnp.float32) * (1.0 / 256.0)
    col_ref[...] = pos_col.astype(jnp.float32) * (1.0 / 256.0)

    def line_of(head, level, point):
        row = (head * LEVELS + level) * POINTS + point
        return slice(row, row + 1)

    def hot_of(head, level, point, rows):
        line = line_of(head, level, point)
        return jnp.where(code_ref[line, :] == iota((rows, pixels), 0), attend_ref[line, :], 0.0)

    weight2[0, :, base2:, :] = jnp.zeros((heads, weight2.shape[2] - base2, pixels), jnp.bfloat16)
    for head in range(heads):
        for level in range(2):
            side = sides[level]
            weight = (weight0, weight1)[level]
            step = 16 // side
            rows = GROUPS[level] * per_block
            for point in range(POINTS):
                hot_ref[point, :rows, :] = hot_of(head, level, point, rows)
                across = hat(
                    col_ref[line_of(head, level, point), :], (iota((16, pixels), 0) % side).astype(jnp.float32)
                )
                for index in range(0, rows, step):
                    stack = [
                        jnp.broadcast_to(hot_ref[point, row : row + 1, :], (side, pixels))
                        for row in range(index, index + step)
                    ]
                    piece = stack[0] if step == 1 else jnp.concatenate(stack, axis=0)
                    piece = (piece * across).astype(jnp.bfloat16)
                    weight[0, head, point, index * side : (index + step) * side, :] = piece
        for level in (2, 3):
            side = sides[level]
            size = sizes[level]
            step = max(1, 8 // size)
            tall = size * step
            place = iota((tall, pixels), 0)
            parts = []
            for point in range(POINTS):
                line = line_of(head, level, point)
                parts.append(
                    hat(down_ref[0, line, :], (place % size // side).astype(jnp.float32))
                    * hat(col_ref[line, :], (place % side).astype(jnp.float32))
                )
                if step == 1:
                    hot_ref[point, :per_block, :] = hot_of(head, level, point, per_block)
                else:
                    line = line_of(head, level, point)
                    parts[-1] = parts[-1] * attend_ref[line, :]
                    hot_ref[point, :tall, :] = jnp.broadcast_to(
                        code_ref[line, :], (tall, pixels)
                    ).astype(jnp.float32) - (place // size).astype(jnp.float32)
            stack = []
            for index in range(0, per_block, step):
                mixed = jnp.zeros((tall, pixels), jnp.float32)
                for point in range(POINTS):
                    if step == 1:
                        mixed = mixed + hot_ref[point, index : index + 1, :] * parts[point]
                    else:
                        mixed = mixed + jnp.where(hot_ref[point, :tall, :] == float(index), parts[point], 0.0)
                stack.append(mixed)
            if level == 2:
                for index, mixed in enumerate(stack):
                    weight2[0, head, index * tall : (index + 1) * tall, :] = mixed.astype(jnp.bfloat16)
            else:
                depth = per_block * size
                first = pl.multiple_of(base2 + block * depth, depth)
                weight2[0, head, pl.ds(first, depth), :] = jnp.concatenate(stack, axis=0).astype(
                    jnp.bfloat16
                )


def load_kernel(*refs):
    count = len(refs) // 2
    sem = refs[-1]
    moves = [
        pltpu.make_async_copy(refs[number], refs[count + number], sem.at[number]) for number in range(count)
    ]
    for move in moves:
        move.start()
    for move in moves:
        move.wait()


def select_kernel(dims, ids_ref, zero_ref, one_ref, two_ref, three_ref, out_ref, sem):
    peers, capacity, sizes = dims
    refs = (zero_ref, one_ref, two_ref)

    def copies(peer, make):
        base = 0
        for level in range(LEVELS - 1):
            size = sizes[level]
            for slot in range(capacity):
                index = jnp.maximum(ids_ref[peer, level * capacity + slot], 0)
                make(refs[level].at[index], out_ref.at[peer, base : base + size, :])
                base += size
        make(three_ref, out_ref.at[peer, base : base + three_ref.shape[0], :])

    def start(peer, carry):
        copies(peer, lambda src, dst: pltpu.make_async_copy(src, dst, sem).start())
        return carry

    def finish(peer, carry):
        copies(peer, lambda src, dst: pltpu.make_async_copy(src, dst, sem).wait())
        return carry

    lax.fori_loop(0, peers, start, 0)
    lax.fori_loop(0, peers, finish, 0)


def pick(values, my_column):
    chosen = jnp.int32(values[0])
    for column in range(1, len(values)):
        chosen = jnp.where(my_column == column, values[column], chosen)
    return chosen


def relay_select_kernel(dims, order, table_ref, *refs):
    partners, candidates, capacity, sizes, blocks = dims
    sources = refs[:candidates]
    outs = refs[candidates:]
    columns, numbers = order
    my_column = table_ref[0, 1]
    column = pick(columns, my_column)
    which = pick(numbers, my_column)
    for number, source in enumerate(sources):

        @pl.when(which == number)
        def _(source=source):
            for partner in range(partners):
                base = 0
                start = 0
                for level in range(LEVELS - 1):
                    size = sizes[level]
                    for rank in range(capacity):
                        index = jnp.maximum(
                            table_ref[1 + partner * LINE + column, level * capacity + rank], 0
                        )
                        outs[partner][base : base + size, :] = source[
                            pl.ds(pl.multiple_of(start + index * size, size), size), :
                        ]
                        base += size
                    start += blocks * size
                small = blocks * sizes[3]
                outs[partner][base : base + small, :] = source[start : start + small, :]


def gather_direct(dims, request_ref, fetched_ref, tiles, tile3, sem):
    peers, capacity, sizes, _, _, _, _, _ = dims
    small = tile3.shape[1]
    base3 = capacity * sum(sizes[:3])
    pltpu.make_async_copy(fetched_ref.at[:, base3 : base3 + small, :], tile3, sem.at[LEVELS - 1]).start()

    def start(peer, carry):
        base = 0
        for level in range(LEVELS - 1):
            size = sizes[level]
            for rank in range(capacity):
                fetch_one(
                    request_ref[peer, level * capacity + rank],
                    fetched_ref.at[peer, base : base + size, :],
                    tiles[level],
                    sem.at[level],
                )
                base += size
        return carry

    lax.fori_loop(0, peers, start, 0)
    for level in range(LEVELS - 1):
        pltpu.make_async_copy(tiles[level], tiles[level], sem.at[level]).wait()
    pltpu.make_async_copy(tile3, tile3, sem.at[LEVELS - 1]).wait()


def fetch_one(request, source, tile, sem):
    @pl.when(request >= 0)
    def _():
        pltpu.make_async_copy(source, tile.at[request], sem).start()


def gather_relay(dims, relay, table_ref, near_refs, packs_refs, tiles, tile3):
    peers, capacity, sizes, _, _, _, _, blocks = dims
    rows, columns, partner_of = relay
    small = tile3.shape[1]
    my_row = table_ref[0, 0]
    my_column = table_ref[0, 1]
    requests = 1 + (rows - 1) * columns
    asked = requests + peers

    def put(owner, level, rank, source, start):
        request = table_ref[requests + owner, level * capacity + rank]
        size = sizes[level]
        tiles[level][jnp.maximum(request, 0)] = source[pl.ds(start, size), :]

    for name, source in zip(NEAR, near_refs, strict=True):
        held = [-1] * columns
        for buffers, owners in SLOTS:
            for column in range(columns):
                if buffers[column] == name:
                    held[column] = owners[column]
        column = pick(held, my_column)

        @pl.when(column >= 0)
        def _(source=source, column=column):
            owner = my_row * columns + column
            start = 0
            for level in range(LEVELS - 1):
                size = sizes[level]
                for rank in range(capacity):
                    index = jnp.maximum(table_ref[asked + owner, level * capacity + rank], 0)
                    put(owner, level, rank, source, pl.multiple_of(start + index * size, size))
                start += blocks * size
            tile3[owner] = source[start : start + small, :]

    for number, source in enumerate(packs_refs):
        slot, partner = divmod(number, rows - 1)
        owner = partner_of(my_row, partner + 1) * columns + pick(SLOTS[slot][1], my_column)
        base = 0
        for level in range(LEVELS - 1):
            for rank in range(capacity):
                put(owner, level, rank, source, base)
                base += sizes[level]
        tile3[owner] = source[base : base + small, :]


def attend_kernel(dims, grid, gather, count, *refs):
    sources = refs[:count]
    (
        weight0,
        weight1,
        weight2,
        down_ref,
        lists_ref,
        out_ref,
        tile0,
        tile1,
        tile2,
        tile3,
        left0,
        left1,
        left2,
        sem,
    ) = refs[count:]
    peers, capacity, sizes, sides, per_block, heads, head_dim, blocks = dims
    pixels = sizes[0]
    channels = heads * head_dim
    small = tile3.shape[1]
    base2 = per_block * sizes[2]
    side0, side1 = sides[0], sides[1]

    gather(sources, (tile0, tile1, tile2), tile3, sem)
    left0[...] = jnp.zeros_like(left0)
    flat = tile3[...].reshape(peers * small, channels)
    size3 = sizes[3]
    wide = blocks * per_block * size3
    lane = iota((1, wide), 1)
    target = lane % size3
    tile_rows, tile_cols, grid_cols, col_count, capacity = grid
    for request in range(blocks * per_block):
        block, entry = divmod(request, per_block)
        tile = lists_ref[block // tile_cols, block % tile_cols, LEVELS - 1, entry]
        tile_row = lax.div(tile, grid_cols)
        tile_col = tile - tile_row * grid_cols
        high = lax.div(tile_row, tile_rows)
        wide_col = lax.div(tile_col, tile_cols)
        owner = high * col_count + wide_col
        place = (tile_row - high * tile_rows) * tile_cols + tile_col - wide_col * tile_cols
        first = owner * small + place * size3
        target = target + jnp.where(lane // size3 == request, first, 0)
    chosen = (iota((peers * small, wide), 0) == target).astype(jnp.bfloat16)
    picked = lax.dot_general(flat, chosen, (((0,), (0,)), ((), ())), preferred_element_type=jnp.float32)
    left2[:, base2:] = picked.astype(jnp.bfloat16)

    def one(block, carry):
        mine = pl.ds(block * per_block, per_block)
        reach0 = side0 // GROUPS[0]
        for line in range(side0):
            piece = tile0[mine, line * side0 : (line + 1) * side0, :]
            turned = piece.reshape(per_block * side0, channels).T
            for group in range(GROUPS[0]):
                offset = line - group * reach0
                if 0 <= offset <= reach0:
                    for head in range(heads):
                        left0[
                            head,
                            offset * head_dim : (offset + 1) * head_dim,
                            group * per_block * side0 : (group + 1) * per_block * side0,
                        ] = turned[head * head_dim : (head + 1) * head_dim, :]
        wide1 = tile1[mine].astype(jnp.float32)
        reach1 = side1 // GROUPS[1]
        for offset in range(reach1 + 1):
            stack = []
            for group in range(GROUPS[1]):
                line = min(group * reach1 + offset, side1 - 1)
                stack.append(
                    wide1[:, line * side1 : (line + 1) * side1, :].reshape(per_block * side1, channels)
                )
            turned = jnp.concatenate(stack, axis=0).astype(jnp.bfloat16).T
            for head in range(heads):
                left1[head, offset * head_dim : (offset + 1) * head_dim, :] = turned[
                    head * head_dim : (head + 1) * head_dim, :
                ]
        left2[:, :base2] = tile2[mine].reshape(per_block * sizes[2], channels).T

        for head in range(heads):
            total = jnp.dot(
                left2[head * head_dim : (head + 1) * head_dim, :],
                weight2[block, head],
                preferred_element_type=jnp.float32,
            )
            for level in range(2):
                left = (left0, left1)[level]
                weight = (weight0, weight1)[level]
                for point in range(POINTS):
                    row = (head * LEVELS + level) * POINTS + point
                    product = jnp.dot(left[head], weight[block, head, point], preferred_element_type=jnp.float32)
                    down = down_ref[block, row : row + 1, :]
                    for offset in range(sides[level] // GROUPS[level] + 1):
                        total = total + product[offset * head_dim : (offset + 1) * head_dim, :] * hat(
                            down, float(offset)
                        )
            out_ref[
                pl.ds(pl.multiple_of(block * pixels, pixels), pixels), head * head_dim : (head + 1) * head_dim
            ] = total.T.astype(jnp.bfloat16)
        return carry

    lax.fori_loop(0, blocks, one, 0)


def own_kernel(head_ref, query_ref, own_ref, weight_ref, bias_ref, out_ref):
    channels = own_ref.shape[1]
    rows = weight_ref[pl.ds(pl.multiple_of(head_ref[0] * channels, channels), channels), :]
    pre = query_ref[...].astype(jnp.float32) + bias_ref[...]
    out_ref[...] = pre + jnp.dot(own_ref[...], rows, preferred_element_type=jnp.float32)


def norm_kernel(head_ref, pre_ref, other_ref, weight_ref, gain_ref, shift_ref, out_ref):
    own_head = head_ref[0]
    pixels, channels = out_ref.shape
    here = pl.ds(pl.multiple_of(pl.program_id(0) * pixels, pixels), pixels)
    rows = weight_ref[pl.ds(pl.multiple_of((1 - own_head) * channels, channels), channels), :]
    pre = pre_ref[here, :] + jnp.dot(other_ref[here, :], rows, preferred_element_type=jnp.float32)
    centered = pre - jnp.mean(pre, axis=1, keepdims=True)
    variance = jnp.mean(centered * centered, axis=1, keepdims=True)
    own = jnp.where(own_head == 0, centered[:, :channels], centered[:, channels:])
    out_ref[...] = (own * lax.rsqrt(variance + 1e-05) * gain_ref[...] + shift_ref[...]).astype(jnp.bfloat16)


def tables(lists, grid):
    tile_rows, tile_cols, grid_cols, col_count, _ = grid
    _, blocks, _, per_block = lists.shape
    requests = blocks * per_block
    wanted = jnp.concatenate([lists[:, block] for block in range(blocks)], axis=2)
    grid_row = wanted // grid_cols
    grid_col = wanted % grid_cols
    owner = grid_row // tile_rows * col_count + grid_col // tile_cols
    local = grid_row % tile_rows * tile_cols + grid_col % tile_cols
    order = jnp.arange(requests, dtype=jnp.int32)
    earlier = (owner[..., :, None] == owner[..., None, :]) & (order[None, :] < order[:, None])
    rank = jnp.sum(earlier.astype(jnp.int32), axis=3)
    return owner, local, rank


def entries(owner, rank, owners, capacity, value):
    slot = jnp.arange(capacity, dtype=jnp.int32)
    hit = (owner[:, None, :, None, :] == owners[None, :, None, None, None]) & (
        rank[:, None, :, None, :] == slot[None, None, None, :, None]
    )
    found = jnp.sum(jnp.where(hit, 1 + value[:, None, :, None, :], 0), axis=4) - 1
    return found.reshape(owner.shape[0], owners.shape[0], -1)


LINE = 4
SELECT_COST = pl.CostEstimate(flops=500_000_000, bytes_accessed=1_000_000, transcendentals=0)
PREP_COST = pl.CostEstimate(flops=2_000_000_000, bytes_accessed=4_000_000, transcendentals=0)
STEPS = (
    ("first", None, ((0, 1), (1, 0), (2, 3), (3, 2))),
    ("cross", None, ((1, 2), (2, 1))),
    ("out", "cross", ((1, 0), (2, 3))),
    ("over", "first", ((1, 2), (2, 1))),
    ("last", "over", ((1, 0), (2, 3))),
)
NEAR = ("own", "first", "cross", "out", "over", "last")
SLOTS = (
    (("own",) * 4, (0, 1, 2, 3)),
    (("first",) * 4, (1, 0, 3, 2)),
    (("out", "cross", "cross", "out"), (2, 2, 1, 1)),
    (("last", "over", "over", "last"), (3, 3, 0, 0)),
)


def relay_tiles(dims, row_count, col_count, pack, flat_sets, lists, grid):
    peers, capacity, sizes, _, per_block, heads, head_dim, blocks = dims
    channels = heads * head_dim
    my_row = lax.axis_index("row")
    my_column = lax.axis_index("col")
    power = row_count & (row_count - 1) == 0

    def partner_of(row, number):
        return row ^ number if power else (row + number) % row_count

    def source_of(row, number):
        return row ^ number if power else (row + row_count - number) % row_count

    held = {"own": jnp.concatenate(flat_sets, axis=0)}

    def move(name):
        source, pairs = {step[0]: step[1:] for step in STEPS}[name]
        held[name] = lax.ppermute(held[source or "own"], "col", pairs)

    move("first")
    move("cross")
    owner, local, rank = tables(lists.reshape(1, blocks, LEVELS, per_block), grid)
    order = jnp.arange(blocks * per_block, dtype=jnp.int32)
    code = entries(owner, rank, jnp.arange(peers, dtype=jnp.int32), capacity, order * blocks + local)[0]
    asked = jnp.where(code >= 0, code % blocks, -1)
    request = jnp.where(code >= 0, code // blocks, -1)
    by_row = asked.reshape(row_count, col_count, asked.shape[1])
    ids = []
    for number in range(1, row_count):
        mine = jnp.sum(
            jnp.where(
                (jnp.arange(row_count) == partner_of(my_row, number))[:, None, None], by_row, 0
            ),
            axis=0,
        )
        ids.append(
            lax.ppermute(mine, "row", [(row, partner_of(row, number)) for row in range(row_count)])
        )

    width = asked.shape[1]
    lane = jnp.arange(width)[None, :]
    place = jnp.where(lane == 0, my_row, my_column).astype(jnp.int32)
    table = jnp.concatenate([place, *ids, request, asked], axis=0)
    packs = []
    for slot, (buffers, columns) in enumerate(SLOTS):
        if slot == 1:
            move("out")
            move("over")
        if slot == 2:
            move("last")
        names = sorted(set(buffers))
        numbers = [names.index(name) for name in buffers]
        sent = pl.pallas_call(
            functools.partial(
                relay_select_kernel, (row_count - 1, len(names), capacity, sizes, blocks), (columns, numbers)
            ),
            out_shape=[jax.ShapeDtypeStruct((pack, channels), jnp.bfloat16)] * (row_count - 1),
            in_specs=[pl.BlockSpec(memory_space=SMEM)] + [pl.BlockSpec(memory_space=VMEM)] * len(names),
            out_specs=[pl.BlockSpec(memory_space=VMEM)] * (row_count - 1),
            compiler_params=pltpu.CompilerParams(vmem_limit_bytes=SELECT_VMEM),
            cost_estimate=SELECT_COST,
        )(table, *[held[name] for name in names])
        for number in range(1, row_count):
            packs.append(
                lax.ppermute(
                    sent[number - 1], "row", [(row, source_of(row, number)) for row in range(row_count)]
                )
            )

    near = [held[name] for name in NEAR]
    sources = (table, *near, *packs)
    spaces = (SMEM,) + (VMEM,) * (len(near) + len(packs))

    def gather(refs, tiles, tile3, sem):
        gather_relay(
            dims,
            (row_count, col_count, partner_of),
            refs[0],
            refs[1 : 1 + len(near)],
            refs[1 + len(near) :],
            tiles,
            tile3,
        )

    return gather, sources, spaces


def direct_tiles(dims, pack, tile_sets, flat_sets, lists, grid):
    peers, capacity, sizes, _, per_block, heads, head_dim, blocks = dims
    channels = heads * head_dim
    owner, local, rank = tables(lists.reshape(1, blocks, LEVELS, per_block), grid)
    owners = jnp.arange(peers, dtype=jnp.int32)
    order = jnp.broadcast_to(jnp.arange(blocks * per_block, dtype=jnp.int32), owner.shape)
    asked = entries(owner, rank, owners, capacity, local)[0]
    request = entries(owner, rank, owners, capacity, order)[0]
    received = lax.all_to_all(asked, ("row", "col"), split_axis=0, concat_axis=0, tiled=True)
    packs = pl.pallas_call(
        functools.partial(select_kernel, (peers, capacity, sizes)),
        out_shape=jax.ShapeDtypeStruct((peers, pack, channels), jnp.bfloat16),
        in_specs=[pl.BlockSpec(memory_space=SMEM)] + [pl.BlockSpec(memory_space=VMEM)] * 4,
        out_specs=pl.BlockSpec(memory_space=ANY),
        scratch_shapes=[pltpu.SemaphoreType.DMA],
        name="select",
    )(received, tile_sets[0], tile_sets[1], tile_sets[2], flat_sets[3])
    fetched = lax.all_to_all(packs, ("row", "col"), split_axis=0, concat_axis=0, tiled=True)

    def gather(refs, tiles, tile3, sem):
        gather_direct(dims, refs[0], refs[1], tiles, tile3, sem)

    return gather, (request, fetched), (SMEM, ANY)


def on_device(
    queries,
    level_zero,
    level_one,
    level_two,
    level_three,
    tile_lists,
    samples,
    logit_weight,
    logit_bias,
    output_weight,
    output_bias,
    norm_gain,
    norm_shift,
):
    level_blocks = (level_zero, level_one, level_two, level_three)
    row_count = lax.axis_size("row")
    col_count = lax.axis_size("col")
    peers = row_count * col_count
    tile_rows, tile_cols, level_count, per_block = tile_lists.shape
    blocks = tile_rows * tile_cols
    requests = blocks * per_block
    capacity = max(2, (requests + peers - 1) // peers)
    grid_cols = tile_cols * col_count
    channels = level_zero.shape[2]
    width_all = queries.shape[2]
    lanes = samples.shape[2]
    heads = lanes // (LEVELS * POINTS)
    head_dim = channels // heads
    sides = tuple(block.shape[0] // tile_rows for block in level_blocks)
    sizes = tuple(side * side for side in sides)
    pixels = sizes[0]
    tile_sets = [
        to_blocks(level_blocks[level], tile_rows, tile_cols, sides[level]) for level in range(level_count)
    ]

    small = blocks * sizes[3]
    pack = capacity * sum(sizes[:3]) + small
    dims = (peers, capacity, sizes, sides, per_block, heads, head_dim, blocks)
    grid = (tile_rows, tile_cols, grid_cols, col_count, capacity)
    flat_sets = [
        tile_sets[level].reshape(blocks * sizes[level], channels) for level in range(level_count)
    ]
    if peers * capacity <= requests and col_count == LINE:
        gather, sources, spaces = relay_tiles(
            dims, row_count, col_count, pack, flat_sets, tile_lists, grid
        )
    else:
        gather, sources, spaces = direct_tiles(
            dims, pack, tile_sets, flat_sets, tile_lists, grid
        )

    queries_blocked = to_blocks(queries, tile_rows, tile_cols, sides[0]).reshape(blocks * pixels, width_all)
    samples_blocked = to_blocks(samples, tile_rows, tile_cols, sides[0]).reshape(blocks * pixels, lanes)
    depth0 = GROUPS[0] * per_block * sides[0]
    depth1 = GROUPS[1] * per_block * sides[1]
    depth2 = per_block * sizes[2] + requests * sizes[3]
    whole = pl.BlockSpec(memory_space=VMEM)
    staged = (queries_blocked, samples_blocked, logit_weight.T)
    queries_blocked, samples_blocked, logit_turned = pl.pallas_call(
        load_kernel,
        out_shape=[jax.ShapeDtypeStruct(array.shape, array.dtype) for array in staged],
        in_specs=[pl.BlockSpec(memory_space=ANY)] * len(staged),
        out_specs=[whole] * len(staged),
        scratch_shapes=[pltpu.SemaphoreType.DMA((len(staged),))],
        compiler_params=pltpu.CompilerParams(vmem_limit_bytes=SELECT_VMEM),
        name="load",
    )(*staged)
    weights = pl.pallas_call(
        functools.partial(prep_kernel, dims),
        out_shape=[
            jax.ShapeDtypeStruct((blocks, heads, POINTS, depth0, pixels), jnp.bfloat16),
            jax.ShapeDtypeStruct((blocks, heads, POINTS, depth1, pixels), jnp.bfloat16),
            jax.ShapeDtypeStruct((blocks, heads, depth2, pixels), jnp.bfloat16),
            jax.ShapeDtypeStruct((blocks, lanes, pixels), jnp.float32),
        ],
        grid=(blocks,),
        in_specs=[
            pl.BlockSpec((pixels, width_all), lambda i: (i, 0)),
            pl.BlockSpec((lanes, width_all), lambda i: (0, 0)),
            pl.BlockSpec((1, lanes), lambda i: (0, 0)),
            pl.BlockSpec((pixels, lanes), lambda i: (i, 0)),
        ],
        out_specs=[
            pl.BlockSpec((1, heads, POINTS, depth0, pixels), lambda i: (i, 0, 0, 0, 0)),
            pl.BlockSpec((1, heads, POINTS, depth1, pixels), lambda i: (i, 0, 0, 0, 0)),
            pl.BlockSpec((1, heads, depth2, pixels), lambda i: (i, 0, 0, 0)),
            pl.BlockSpec((1, lanes, pixels), lambda i: (i, 0, 0)),
        ],
        scratch_shapes=[
            VMEM((lanes, pixels), jnp.float32),
            VMEM((lanes, pixels), jnp.int32),
            VMEM((lanes, pixels), jnp.float32),
            VMEM((POINTS, max(GROUPS) * per_block, pixels), jnp.float32),
        ],
        compiler_params=pltpu.CompilerParams(vmem_limit_bytes=PREP_VMEM),
        cost_estimate=PREP_COST,
        name="prep",
    )(queries_blocked, logit_turned, logit_bias.reshape(1, lanes), samples_blocked)

    attn = pl.pallas_call(
        functools.partial(attend_kernel, dims, grid, gather, len(sources)),
        out_shape=jax.ShapeDtypeStruct((blocks * pixels, channels), jnp.bfloat16),
        in_specs=[pl.BlockSpec(memory_space=space) for space in spaces]
        + [whole] * 4
        + [pl.BlockSpec(memory_space=SMEM)],
        out_specs=whole,
        scratch_shapes=[
            VMEM((requests, sizes[0], channels), jnp.bfloat16),
            VMEM((requests, sizes[1], channels), jnp.bfloat16),
            VMEM((requests, sizes[2], channels), jnp.bfloat16),
            VMEM((peers, small, channels), jnp.bfloat16),
            VMEM((heads, (sides[0] // GROUPS[0] + 1) * head_dim, depth0), jnp.bfloat16),
            VMEM((heads, (sides[1] // GROUPS[1] + 1) * head_dim, depth1), jnp.bfloat16),
            VMEM((channels, depth2), jnp.bfloat16),
            pltpu.SemaphoreType.DMA((LEVELS,)),
        ],
        compiler_params=pltpu.CompilerParams(vmem_limit_bytes=ATTEND_VMEM),
        cost_estimate=PREP_COST,
        name="attend",
    )(*sources, *weights, tile_lists)

    own_head = lax.axis_index("head").reshape(1).astype(jnp.int32)
    other = lax.ppermute(attn, "head", [(0, 1), (1, 0)])
    wide_spec = pl.BlockSpec((pixels, width_all), lambda i: (i, 0))
    slim_spec = pl.BlockSpec((pixels, channels), lambda i: (i, 0))
    matrix_spec = pl.BlockSpec((width_all, width_all), lambda i: (0, 0))
    pre = pl.pallas_call(
        own_kernel,
        out_shape=jax.ShapeDtypeStruct((blocks * pixels, width_all), jnp.float32),
        grid=(blocks,),
        in_specs=[
            pl.BlockSpec(memory_space=SMEM),
            wide_spec,
            slim_spec,
            matrix_spec,
            pl.BlockSpec((1, width_all), lambda i: (0, 0)),
        ],
        out_specs=wide_spec,
        compiler_params=pltpu.CompilerParams(vmem_limit_bytes=SELECT_VMEM),
        name="own",
    )(own_head, queries_blocked, attn, output_weight, output_bias.reshape(1, width_all))
    updated = pl.pallas_call(
        norm_kernel,
        out_shape=jax.ShapeDtypeStruct((blocks * pixels, channels), jnp.bfloat16),
        grid=(blocks,),
        in_specs=[pl.BlockSpec(memory_space=SMEM)] + [whole] * 5,
        out_specs=slim_spec,
        compiler_params=pltpu.CompilerParams(vmem_limit_bytes=SELECT_VMEM),
        name="norm",
    )(
        own_head,
        pre,
        other,
        output_weight,
        norm_gain.reshape(1, channels),
        norm_shift.reshape(1, channels),
    )
    side = sides[0]
    updated = updated.reshape(tile_rows, tile_cols, side, side, channels).transpose(0, 2, 1, 3, 4)
    return updated.reshape(tile_rows * side, tile_cols * side, channels)


def solution(mesh):
    in_specs = (
        P("row", "col", None),
        P("row", "col", "head"),
        P("row", "col", "head"),
        P("row", "col", "head"),
        P("row", "col", "head"),
        P("row", "col", None, None),
        P("row", "col", "head"),
        P(None, "head"),
        P("head"),
        P(),
        P(),
        P("head"),
        P("head"),
    )
    out_specs = P("row", "col", "head")
    return jax.shard_map(on_device, mesh=mesh, in_specs=in_specs, out_specs=out_specs, check_vma=False)
```

```python
import functools
import jax
import jax.numpy as jnp
from jax import lax
from jax.experimental import pallas as pl
from jax.experimental.pallas import tpu as pltpu
from jax.sharding import PartitionSpec as P

LEVELS = 4
POINTS = 4
ANY = pl.ANY
SMEM = pltpu.SMEM
VMEM = pltpu.VMEM
SELECT_VMEM = 4 * 1024 * 1024
PREP_VMEM = 8 * 1024 * 1024
ATTEND_VMEM = 12 * 1024 * 1024
GROUPS = (2, 2)


def to_blocks(source, tile_rows, tile_cols, tile_side):
    channels = source.shape[2]
    shaped = source.reshape(tile_rows, tile_side, tile_cols, tile_side, channels)
    return shaped.transpose(0, 2, 1, 3, 4).reshape(
        tile_rows * tile_cols, tile_side * tile_side, channels
    )


def hat(position, center):
    return jnp.maximum(1.0 - jnp.abs(position - center), 0.0)


def iota(shape, dim):
    return lax.broadcasted_iota(jnp.int32, shape, dim)


def prep_kernel(
    dims,
    query_ref,
    logit_ref,
    bias_ref,
    sample_ref,
    weight0,
    weight1,
    weight2,
    down_ref,
    attend_ref,
    code_ref,
    col_ref,
    hot_ref,
):
    _, _, sizes, sides, per_block, heads, _, _ = dims
    block = pl.program_id(0)
    pixels = sizes[0]
    base2 = per_block * sizes[2]
    lanes = LEVELS * POINTS
    logits = lax.dot_general(
        query_ref[...], logit_ref[...], (((1,), (1,)), ((), ())), preferred_element_type=jnp.float32
    )
    logits = (logits + bias_ref[...]).T
    for head in range(heads):
        part = logits[head * lanes : (head + 1) * lanes, :]
        part = jnp.exp(part - jnp.max(part, axis=0, keepdims=True))
        attend_ref[head * lanes : (head + 1) * lanes, :] = part / jnp.sum(part, axis=0, keepdims=True)
    packed = sample_ref[...].T
    level_of = iota(packed.shape, 0) // POINTS % LEVELS
    slot = packed >> 24
    pos_row = (packed >> 12) & 4095
    pos_col = packed & 4095
    deep = jnp.where(level_of == 0, sides[0] * 256 // GROUPS[0], sides[1] * 256 // GROUPS[1])
    group = jnp.zeros_like(packed)
    for bound in range(1, max(GROUPS)):
        group = group + jnp.where(pos_row >= bound * deep, 1, 0)
    group = jnp.where(level_of < 2, group, 0)
    code_ref[...] = slot + group * per_block
    down_ref[0] = (pos_row - group * deep).astype(jnp.float32) * (1.0 / 256.0)
    col_ref[...] = pos_col.astype(jnp.float32) * (1.0 / 256.0)

    def line_of(head, level, point):
        row = (head * LEVELS + level) * POINTS + point
        return slice(row, row + 1)

    def hot_of(head, level, point, rows):
        line = line_of(head, level, point)
        return jnp.where(code_ref[line, :] == iota((rows, pixels), 0), attend_ref[line, :], 0.0)

    weight2[0, :, base2:, :] = jnp.zeros((heads, weight2.shape[2] - base2, pixels), jnp.bfloat16)
    for head in range(heads):
        for level in range(2):
            side = sides[level]
            weight = (weight0, weight1)[level]
            step = 16 // side
            rows = GROUPS[level] * per_block
            for point in range(POINTS):
                hot_ref[point, :rows, :] = hot_of(head, level, point, rows)
                across = hat(
                    col_ref[line_of(head, level, point), :], (iota((16, pixels), 0) % side).astype(jnp.float32)
                )
                for index in range(0, rows, step):
                    stack = [
                        jnp.broadcast_to(hot_ref[point, row : row + 1, :], (side, pixels))
                        for row in range(index, index + step)
                    ]
                    piece = stack[0] if step == 1 else jnp.concatenate(stack, axis=0)
                    piece = (piece * across).astype(jnp.bfloat16)
                    weight[0, head, point, index * side : (index + step) * side, :] = piece
        for level in (2, 3):
            side = sides[level]
            size = sizes[level]
            step = max(1, 8 // size)
            tall = size * step
            place = iota((tall, pixels), 0)
            parts = []
            for point in range(POINTS):
                line = line_of(head, level, point)
                parts.append(
                    hat(down_ref[0, line, :], (place % size // side).astype(jnp.float32))
                    * hat(col_ref[line, :], (place % side).astype(jnp.float32))
                )
                if step == 1:
                    hot_ref[point, :per_block, :] = hot_of(head, level, point, per_block)
                else:
                    line = line_of(head, level, point)
                    parts[-1] = parts[-1] * attend_ref[line, :]
                    hot_ref[point, :tall, :] = jnp.broadcast_to(
                        code_ref[line, :], (tall, pixels)
                    ).astype(jnp.float32) - (place // size).astype(jnp.float32)
            stack = []
            for index in range(0, per_block, step):
                mixed = jnp.zeros((tall, pixels), jnp.float32)
                for point in range(POINTS):
                    if step == 1:
                        mixed = mixed + hot_ref[point, index : index + 1, :] * parts[point]
                    else:
                        mixed = mixed + jnp.where(hot_ref[point, :tall, :] == float(index), parts[point], 0.0)
                stack.append(mixed)
            if level == 2:
                for index, mixed in enumerate(stack):
                    weight2[0, head, index * tall : (index + 1) * tall, :] = mixed.astype(jnp.bfloat16)
            else:
                depth = per_block * size
                first = pl.multiple_of(base2 + block * depth, depth)
                weight2[0, head, pl.ds(first, depth), :] = jnp.concatenate(stack, axis=0).astype(
                    jnp.bfloat16
                )


def load_kernel(*refs):
    count = len(refs) // 2
    sem = refs[-1]
    moves = [
        pltpu.make_async_copy(refs[number], refs[count + number], sem.at[number]) for number in range(count)
    ]
    for move in moves:
        move.start()
    for move in moves:
        move.wait()


def select_kernel(dims, ids_ref, zero_ref, one_ref, two_ref, three_ref, out_ref, sem):
    peers, capacity, sizes = dims
    refs = (zero_ref, one_ref, two_ref)

    def copies(peer, make):
        base = 0
        for level in range(LEVELS - 1):
            size = sizes[level]
            for slot in range(capacity):
                index = jnp.maximum(ids_ref[peer, level * capacity + slot], 0)
                make(refs[level].at[index], out_ref.at[peer, base : base + size, :])
                base += size
        make(three_ref, out_ref.at[peer, base : base + three_ref.shape[0], :])

    def start(peer, carry):
        copies(peer, lambda src, dst: pltpu.make_async_copy(src, dst, sem).start())
        return carry

    def finish(peer, carry):
        copies(peer, lambda src, dst: pltpu.make_async_copy(src, dst, sem).wait())
        return carry

    lax.fori_loop(0, peers, start, 0)
    lax.fori_loop(0, peers, finish, 0)


def pick(values, my_column):
    chosen = jnp.int32(values[0])
    for column in range(1, len(values)):
        chosen = jnp.where(my_column == column, values[column], chosen)
    return chosen


def relay_select_kernel(dims, order, table_ref, *refs):
    partners, candidates, capacity, sizes, blocks = dims
    sources = refs[:candidates]
    outs = refs[candidates:]
    columns, numbers = order
    my_column = table_ref[0, 1]
    column = pick(columns, my_column)
    which = pick(numbers, my_column)
    for number, source in enumerate(sources):

        @pl.when(which == number)
        def _(source=source):
            for partner in range(partners):
                base = 0
                start = 0
                for level in range(LEVELS - 1):
                    size = sizes[level]
                    for rank in range(capacity):
                        index = jnp.maximum(
                            table_ref[1 + partner * LINE + column, level * capacity + rank], 0
                        )
                        outs[partner][base : base + size, :] = source[
                            pl.ds(pl.multiple_of(start + index * size, size), size), :
                        ]
                        base += size
                    start += blocks * size
                small = blocks * sizes[3]
                outs[partner][base : base + small, :] = source[start : start + small, :]


def gather_direct(dims, request_ref, fetched_ref, tiles, tile3, sem):
    peers, capacity, sizes, _, _, _, _, _ = dims
    small = tile3.shape[1]
    base3 = capacity * sum(sizes[:3])
    pltpu.make_async_copy(fetched_ref.at[:, base3 : base3 + small, :], tile3, sem.at[LEVELS - 1]).start()

    def start(peer, carry):
        base = 0
        for level in range(LEVELS - 1):
            size = sizes[level]
            for rank in range(capacity):
                fetch_one(
                    request_ref[peer, level * capacity + rank],
                    fetched_ref.at[peer, base : base + size, :],
                    tiles[level],
                    sem.at[level],
                )
                base += size
        return carry

    lax.fori_loop(0, peers, start, 0)
    for level in range(LEVELS - 1):
        pltpu.make_async_copy(tiles[level], tiles[level], sem.at[level]).wait()
    pltpu.make_async_copy(tile3, tile3, sem.at[LEVELS - 1]).wait()


def fetch_one(request, source, tile, sem):
    @pl.when(request >= 0)
    def _():
        pltpu.make_async_copy(source, tile.at[request], sem).start()


def gather_relay(dims, relay, table_ref, near_refs, packs_refs, tiles, tile3):
    peers, capacity, sizes, _, _, _, _, blocks = dims
    rows, columns, partner_of = relay
    small = tile3.shape[1]
    my_row = table_ref[0, 0]
    my_column = table_ref[0, 1]
    requests = 1 + (rows - 1) * columns
    asked = requests + peers

    def put(owner, level, rank, source, start):
        request = table_ref[requests + owner, level * capacity + rank]
        size = sizes[level]
        tiles[level][jnp.maximum(request, 0)] = source[pl.ds(start, size), :]

    for name, source in zip(NEAR, near_refs, strict=True):
        held = [-1] * columns
        for buffers, owners in SLOTS:
            for column in range(columns):
                if buffers[column] == name:
                    held[column] = owners[column]
        column = pick(held, my_column)

        @pl.when(column >= 0)
        def _(source=source, column=column):
            owner = my_row * columns + column
            start = 0
            for level in range(LEVELS - 1):
                size = sizes[level]
                for rank in range(capacity):
                    index = jnp.maximum(table_ref[asked + owner, level * capacity + rank], 0)
                    put(owner, level, rank, source, pl.multiple_of(start + index * size, size))
                start += blocks * size
            tile3[owner] = source[start : start + small, :]

    for number, source in enumerate(packs_refs):
        slot, partner = divmod(number, rows - 1)
        owner = partner_of(my_row, partner + 1) * columns + pick(SLOTS[slot][1], my_column)
        base = 0
        for level in range(LEVELS - 1):
            for rank in range(capacity):
                put(owner, level, rank, source, base)
                base += sizes[level]
        tile3[owner] = source[base : base + small, :]


def attend_kernel(dims, grid, gather, count, *refs):
    sources = refs[:count]
    (
        weight0,
        weight1,
        weight2,
        down_ref,
        lists_ref,
        out_ref,
        tile0,
        tile1,
        tile2,
        tile3,
        left0,
        left1,
        left2,
        turn_ref,
        sem,
    ) = refs[count:]
    peers, capacity, sizes, sides, per_block, heads, head_dim, blocks = dims
    pixels = sizes[0]
    channels = heads * head_dim
    small = tile3.shape[1]
    base2 = per_block * sizes[2]
    side0, side1 = sides[0], sides[1]

    gather(sources, (tile0, tile1, tile2), tile3, sem)
    left0[:, side0 // GROUPS[0] * head_dim :, :] = jnp.zeros(
        (heads, head_dim, left0.shape[2]), jnp.bfloat16
    )
    flat = tile3[...].reshape(peers * small, channels)
    size3 = sizes[3]
    wide = blocks * per_block * size3
    lane = iota((1, wide), 1)
    target = lane % size3
    tile_rows, tile_cols, grid_cols, col_count, capacity = grid
    for request in range(blocks * per_block):
        block, entry = divmod(request, per_block)
        tile = lists_ref[block // tile_cols, block % tile_cols, LEVELS - 1, entry]
        tile_row = lax.div(tile, grid_cols)
        tile_col = tile - tile_row * grid_cols
        high = lax.div(tile_row, tile_rows)
        wide_col = lax.div(tile_col, tile_cols)
        owner = high * col_count + wide_col
        place = (tile_row - high * tile_rows) * tile_cols + tile_col - wide_col * tile_cols
        first = owner * small + place * size3
        target = target + jnp.where(lane // size3 == request, first, 0)
    chosen = (iota((peers * small, wide), 0) == target).astype(jnp.bfloat16)
    picked = lax.dot_general(flat, chosen, (((0,), (0,)), ((), ())), preferred_element_type=jnp.float32)
    left2[:, base2:] = picked.astype(jnp.bfloat16)

    def one(block, carry):
        mine = pl.ds(block * per_block, per_block)
        reach0 = side0 // GROUPS[0]
        for line in range(side0):
            piece = tile0[mine, line * side0 : (line + 1) * side0, :]
            turned = piece.reshape(per_block * side0, channels).T
            for group in range(GROUPS[0]):
                offset = line - group * reach0
                if 0 <= offset <= reach0:
                    for head in range(heads):
                        left0[
                            head,
                            offset * head_dim : (offset + 1) * head_dim,
                            group * per_block * side0 : (group + 1) * per_block * side0,
                        ] = turned[head * head_dim : (head + 1) * head_dim, :]
        wide1 = tile1[mine].astype(jnp.float32)
        reach1 = side1 // GROUPS[1]
        for offset in range(reach1 + 1):
            stack = []
            for group in range(GROUPS[1]):
                line = min(group * reach1 + offset, side1 - 1)
                stack.append(
                    wide1[:, line * side1 : (line + 1) * side1, :].reshape(per_block * side1, channels)
                )
            turned = jnp.concatenate(stack, axis=0).astype(jnp.bfloat16).T
            for head in range(heads):
                left1[head, offset * head_dim : (offset + 1) * head_dim, :] = turned[
                    head * head_dim : (head + 1) * head_dim, :
                ]
        left2[:, :base2] = tile2[mine].reshape(per_block * sizes[2], channels).T

        def per_head(head, carry):
            rows = pl.ds(head * head_dim, head_dim)
            total = jnp.dot(left2[rows, :], weight2[block, head], preferred_element_type=jnp.float32)
            for level in range(2):
                left = (left0, left1)[level]
                weight = (weight0, weight1)[level]
                for point in range(POINTS):
                    row = (head * LEVELS + level) * POINTS + point
                    product = jnp.dot(left[head], weight[block, head, point], preferred_element_type=jnp.float32)
                    down = down_ref[block, pl.ds(row, 1), :]
                    for offset in range(sides[level] // GROUPS[level] + 1):
                        total = total + product[offset * head_dim : (offset + 1) * head_dim, :] * hat(
                            down, float(offset)
                        )
            turn_ref[rows, :] = total
            return carry

        for head in range(heads):
            per_head(head, 0)
        out_ref[pl.ds(pl.multiple_of(block * pixels, pixels), pixels), :] = turn_ref[...].T.astype(jnp.bfloat16)
        return carry

    lax.fori_loop(0, blocks, one, 0)


def own_kernel(head_ref, query_ref, own_ref, weight_ref, bias_ref, out_ref):
    channels = own_ref.shape[1]
    rows = weight_ref[pl.ds(pl.multiple_of(head_ref[0] * channels, channels), channels), :]
    pre = query_ref[...].astype(jnp.float32) + bias_ref[...]
    out_ref[...] = pre + jnp.dot(own_ref[...], rows, preferred_element_type=jnp.float32)


def norm_kernel(head_ref, pre_ref, other_ref, weight_ref, gain_ref, shift_ref, out_ref):
    own_head = head_ref[0]
    pixels, channels = out_ref.shape
    here = pl.ds(pl.multiple_of(pl.program_id(0) * pixels, pixels), pixels)
    rows = weight_ref[pl.ds(pl.multiple_of((1 - own_head) * channels, channels), channels), :]
    pre = pre_ref[here, :] + jnp.dot(other_ref[here, :], rows, preferred_element_type=jnp.float32)
    centered = pre - jnp.mean(pre, axis=1, keepdims=True)
    variance = jnp.mean(centered * centered, axis=1, keepdims=True)
    own = jnp.where(own_head == 0, centered[:, :channels], centered[:, channels:])
    out_ref[...] = (own * lax.rsqrt(variance + 1e-05) * gain_ref[...] + shift_ref[...]).astype(jnp.bfloat16)


def tables(lists, grid):
    tile_rows, tile_cols, grid_cols, col_count, _ = grid
    _, blocks, _, per_block = lists.shape
    requests = blocks * per_block
    wanted = jnp.concatenate([lists[:, block] for block in range(blocks)], axis=2)
    grid_row = wanted // grid_cols
    grid_col = wanted % grid_cols
    owner = grid_row // tile_rows * col_count + grid_col // tile_cols
    local = grid_row % tile_rows * tile_cols + grid_col % tile_cols
    order = jnp.arange(requests, dtype=jnp.int32)
    earlier = (owner[..., :, None] == owner[..., None, :]) & (order[None, :] < order[:, None])
    rank = jnp.sum(earlier.astype(jnp.int32), axis=3)
    return owner, local, rank


def entries(owner, rank, owners, capacity, value):
    slot = jnp.arange(capacity, dtype=jnp.int32)
    hit = (owner[:, None, :, None, :] == owners[None, :, None, None, None]) & (
        rank[:, None, :, None, :] == slot[None, None, None, :, None]
    )
    found = jnp.sum(jnp.where(hit, 1 + value[:, None, :, None, :], 0), axis=4) - 1
    return found.reshape(owner.shape[0], owners.shape[0], -1)


LINE = 4
SELECT_COST = pl.CostEstimate(flops=500_000_000, bytes_accessed=1_000_000, transcendentals=0)
PREP_COST = pl.CostEstimate(flops=2_000_000_000, bytes_accessed=4_000_000, transcendentals=0)
STEPS = (
    ("first", None, ((0, 1), (1, 0), (2, 3), (3, 2))),
    ("cross", None, ((1, 2), (2, 1))),
    ("out", "cross", ((1, 0), (2, 3))),
    ("over", "first", ((1, 2), (2, 1))),
    ("last", "over", ((1, 0), (2, 3))),
)
NEAR = ("own", "first", "cross", "out", "over", "last")
SLOTS = (
    (("own",) * 4, (0, 1, 2, 3)),
    (("first",) * 4, (1, 0, 3, 2)),
    (("out", "cross", "cross", "out"), (2, 2, 1, 1)),
    (("last", "over", "over", "last"), (3, 3, 0, 0)),
)


def relay_tiles(dims, row_count, col_count, pack, flat_sets, lists, grid):
    peers, capacity, sizes, _, per_block, heads, head_dim, blocks = dims
    channels = heads * head_dim
    my_row = lax.axis_index("row")
    my_column = lax.axis_index("col")
    power = row_count & (row_count - 1) == 0

    def partner_of(row, number):
        return row ^ number if power else (row + number) % row_count

    def source_of(row, number):
        return row ^ number if power else (row + row_count - number) % row_count

    held = {"own": jnp.concatenate(flat_sets, axis=0)}

    def move(name):
        source, pairs = {step[0]: step[1:] for step in STEPS}[name]
        held[name] = lax.ppermute(held[source or "own"], "col", pairs)

    move("first")
    move("cross")
    owner, local, rank = tables(lists.reshape(1, blocks, LEVELS, per_block), grid)
    order = jnp.arange(blocks * per_block, dtype=jnp.int32)
    code = entries(owner, rank, jnp.arange(peers, dtype=jnp.int32), capacity, order * blocks + local)[0]
    asked = jnp.where(code >= 0, code % blocks, -1)
    request = jnp.where(code >= 0, code // blocks, -1)
    by_row = asked.reshape(row_count, col_count, asked.shape[1])
    ids = []
    for number in range(1, row_count):
        mine = jnp.sum(
            jnp.where(
                (jnp.arange(row_count) == partner_of(my_row, number))[:, None, None], by_row, 0
            ),
            axis=0,
        )
        ids.append(
            lax.ppermute(mine, "row", [(row, partner_of(row, number)) for row in range(row_count)])
        )

    width = asked.shape[1]
    lane = jnp.arange(width)[None, :]
    place = jnp.where(lane == 0, my_row, my_column).astype(jnp.int32)
    table = jnp.concatenate([place, *ids, request, asked], axis=0)
    packs = []
    for slot, (buffers, columns) in enumerate(SLOTS):
        if slot == 1:
            move("out")
            move("over")
        if slot == 2:
            move("last")
        names = sorted(set(buffers))
        numbers = [names.index(name) for name in buffers]
        sent = pl.pallas_call(
            functools.partial(
                relay_select_kernel, (row_count - 1, len(names), capacity, sizes, blocks), (columns, numbers)
            ),
            out_shape=[jax.ShapeDtypeStruct((pack, channels), jnp.bfloat16)] * (row_count - 1),
            in_specs=[pl.BlockSpec(memory_space=SMEM)] + [pl.BlockSpec(memory_space=VMEM)] * len(names),
            out_specs=[pl.BlockSpec(memory_space=VMEM)] * (row_count - 1),
            compiler_params=pltpu.CompilerParams(vmem_limit_bytes=SELECT_VMEM),
            cost_estimate=SELECT_COST,
        )(table, *[held[name] for name in names])
        for number in range(1, row_count):
            packs.append(
                lax.ppermute(
                    sent[number - 1], "row", [(row, source_of(row, number)) for row in range(row_count)]
                )
            )

    near = [held[name] for name in NEAR]
    sources = (table, *near, *packs)
    spaces = (SMEM,) + (VMEM,) * (len(near) + len(packs))

    def gather(refs, tiles, tile3, sem):
        gather_relay(
            dims,
            (row_count, col_count, partner_of),
            refs[0],
            refs[1 : 1 + len(near)],
            refs[1 + len(near) :],
            tiles,
            tile3,
        )

    return gather, sources, spaces


def direct_tiles(dims, pack, tile_sets, flat_sets, lists, grid):
    peers, capacity, sizes, _, per_block, heads, head_dim, blocks = dims
    channels = heads * head_dim
    owner, local, rank = tables(lists.reshape(1, blocks, LEVELS, per_block), grid)
    owners = jnp.arange(peers, dtype=jnp.int32)
    order = jnp.broadcast_to(jnp.arange(blocks * per_block, dtype=jnp.int32), owner.shape)
    asked = entries(owner, rank, owners, capacity, local)[0]
    request = entries(owner, rank, owners, capacity, order)[0]
    received = lax.all_to_all(asked, ("row", "col"), split_axis=0, concat_axis=0, tiled=True)
    packs = pl.pallas_call(
        functools.partial(select_kernel, (peers, capacity, sizes)),
        out_shape=jax.ShapeDtypeStruct((peers, pack, channels), jnp.bfloat16),
        in_specs=[pl.BlockSpec(memory_space=SMEM)] + [pl.BlockSpec(memory_space=VMEM)] * 4,
        out_specs=pl.BlockSpec(memory_space=ANY),
        scratch_shapes=[pltpu.SemaphoreType.DMA],
        name="select",
    )(received, tile_sets[0], tile_sets[1], tile_sets[2], flat_sets[3])
    fetched = lax.all_to_all(packs, ("row", "col"), split_axis=0, concat_axis=0, tiled=True)

    def gather(refs, tiles, tile3, sem):
        gather_direct(dims, refs[0], refs[1], tiles, tile3, sem)

    return gather, (request, fetched), (SMEM, ANY)


def on_device(
    queries,
    level_zero,
    level_one,
    level_two,
    level_three,
    tile_lists,
    samples,
    logit_weight,
    logit_bias,
    output_weight,
    output_bias,
    norm_gain,
    norm_shift,
):
    level_blocks = (level_zero, level_one, level_two, level_three)
    row_count = lax.axis_size("row")
    col_count = lax.axis_size("col")
    peers = row_count * col_count
    tile_rows, tile_cols, level_count, per_block = tile_lists.shape
    blocks = tile_rows * tile_cols
    requests = blocks * per_block
    capacity = max(2, (requests + peers - 1) // peers)
    grid_cols = tile_cols * col_count
    channels = level_zero.shape[2]
    width_all = queries.shape[2]
    lanes = samples.shape[2]
    heads = lanes // (LEVELS * POINTS)
    head_dim = channels // heads
    sides = tuple(block.shape[0] // tile_rows for block in level_blocks)
    sizes = tuple(side * side for side in sides)
    pixels = sizes[0]
    tile_sets = [
        to_blocks(level_blocks[level], tile_rows, tile_cols, sides[level]) for level in range(level_count)
    ]

    small = blocks * sizes[3]
    pack = capacity * sum(sizes[:3]) + small
    dims = (peers, capacity, sizes, sides, per_block, heads, head_dim, blocks)
    grid = (tile_rows, tile_cols, grid_cols, col_count, capacity)
    flat_sets = [
        tile_sets[level].reshape(blocks * sizes[level], channels) for level in range(level_count)
    ]
    if peers * capacity <= requests and col_count == LINE:
        gather, sources, spaces = relay_tiles(
            dims, row_count, col_count, pack, flat_sets, tile_lists, grid
        )
    else:
        gather, sources, spaces = direct_tiles(
            dims, pack, tile_sets, flat_sets, tile_lists, grid
        )

    queries_blocked = to_blocks(queries, tile_rows, tile_cols, sides[0]).reshape(blocks * pixels, width_all)
    samples_blocked = to_blocks(samples, tile_rows, tile_cols, sides[0]).reshape(blocks * pixels, lanes)
    depth0 = GROUPS[0] * per_block * sides[0]
    depth1 = GROUPS[1] * per_block * sides[1]
    depth2 = per_block * sizes[2] + requests * sizes[3]
    whole = pl.BlockSpec(memory_space=VMEM)
    staged = (queries_blocked, samples_blocked, logit_weight.T)
    queries_blocked, samples_blocked, logit_turned = pl.pallas_call(
        load_kernel,
        out_shape=[jax.ShapeDtypeStruct(array.shape, array.dtype) for array in staged],
        in_specs=[pl.BlockSpec(memory_space=ANY)] * len(staged),
        out_specs=[whole] * len(staged),
        scratch_shapes=[pltpu.SemaphoreType.DMA((len(staged),))],
        compiler_params=pltpu.CompilerParams(vmem_limit_bytes=SELECT_VMEM),
        name="load",
    )(*staged)
    weights = pl.pallas_call(
        functools.partial(prep_kernel, dims),
        out_shape=[
            jax.ShapeDtypeStruct((blocks, heads, POINTS, depth0, pixels), jnp.bfloat16),
            jax.ShapeDtypeStruct((blocks, heads, POINTS, depth1, pixels), jnp.bfloat16),
            jax.ShapeDtypeStruct((blocks, heads, depth2, pixels), jnp.bfloat16),
            jax.ShapeDtypeStruct((blocks, lanes, pixels), jnp.float32),
        ],
        grid=(blocks,),
        in_specs=[
            pl.BlockSpec((pixels, width_all), lambda i: (i, 0)),
            pl.BlockSpec((lanes, width_all), lambda i: (0, 0)),
            pl.BlockSpec((1, lanes), lambda i: (0, 0)),
            pl.BlockSpec((pixels, lanes), lambda i: (i, 0)),
        ],
        out_specs=[
            pl.BlockSpec((1, heads, POINTS, depth0, pixels), lambda i: (i, 0, 0, 0, 0)),
            pl.BlockSpec((1, heads, POINTS, depth1, pixels), lambda i: (i, 0, 0, 0, 0)),
            pl.BlockSpec((1, heads, depth2, pixels), lambda i: (i, 0, 0, 0)),
            pl.BlockSpec((1, lanes, pixels), lambda i: (i, 0, 0)),
        ],
        scratch_shapes=[
            VMEM((lanes, pixels), jnp.float32),
            VMEM((lanes, pixels), jnp.int32),
            VMEM((lanes, pixels), jnp.float32),
            VMEM((POINTS, max(GROUPS) * per_block, pixels), jnp.float32),
        ],
        compiler_params=pltpu.CompilerParams(vmem_limit_bytes=PREP_VMEM),
        cost_estimate=PREP_COST,
        name="prep",
    )(queries_blocked, logit_turned, logit_bias.reshape(1, lanes), samples_blocked)

    attn = pl.pallas_call(
        functools.partial(attend_kernel, dims, grid, gather, len(sources)),
        out_shape=jax.ShapeDtypeStruct((blocks * pixels, channels), jnp.bfloat16),
        in_specs=[pl.BlockSpec(memory_space=space) for space in spaces]
        + [whole] * 4
        + [pl.BlockSpec(memory_space=SMEM)],
        out_specs=whole,
        scratch_shapes=[
            VMEM((requests, sizes[0], channels), jnp.bfloat16),
            VMEM((requests, sizes[1], channels), jnp.bfloat16),
            VMEM((requests, sizes[2], channels), jnp.bfloat16),
            VMEM((peers, small, channels), jnp.bfloat16),
            VMEM((heads, (sides[0] // GROUPS[0] + 1) * head_dim, depth0), jnp.bfloat16),
            VMEM((heads, (sides[1] // GROUPS[1] + 1) * head_dim, depth1), jnp.bfloat16),
            VMEM((channels, depth2), jnp.bfloat16),
            VMEM((channels, pixels), jnp.float32),
            pltpu.SemaphoreType.DMA((LEVELS,)),
        ],
        compiler_params=pltpu.CompilerParams(vmem_limit_bytes=ATTEND_VMEM),
        cost_estimate=PREP_COST,
        name="attend",
    )(*sources, *weights, tile_lists)

    own_head = lax.axis_index("head").reshape(1).astype(jnp.int32)
    other = lax.ppermute(attn, "head", [(0, 1), (1, 0)])
    wide_spec = pl.BlockSpec((pixels, width_all), lambda i: (i, 0))
    slim_spec = pl.BlockSpec((pixels, channels), lambda i: (i, 0))
    matrix_spec = pl.BlockSpec((width_all, width_all), lambda i: (0, 0))
    pre = pl.pallas_call(
        own_kernel,
        out_shape=jax.ShapeDtypeStruct((blocks * pixels, width_all), jnp.float32),
        grid=(blocks,),
        in_specs=[
            pl.BlockSpec(memory_space=SMEM),
            wide_spec,
            slim_spec,
            matrix_spec,
            pl.BlockSpec((1, width_all), lambda i: (0, 0)),
        ],
        out_specs=wide_spec,
        compiler_params=pltpu.CompilerParams(vmem_limit_bytes=SELECT_VMEM),
        name="own",
    )(own_head, queries_blocked, attn, output_weight, output_bias.reshape(1, width_all))
    updated = pl.pallas_call(
        norm_kernel,
        out_shape=jax.ShapeDtypeStruct((blocks * pixels, channels), jnp.bfloat16),
        grid=(blocks,),
        in_specs=[pl.BlockSpec(memory_space=SMEM)] + [whole] * 5,
        out_specs=slim_spec,
        compiler_params=pltpu.CompilerParams(vmem_limit_bytes=SELECT_VMEM),
        name="norm",
    )(
        own_head,
        pre,
        other,
        output_weight,
        norm_gain.reshape(1, channels),
        norm_shift.reshape(1, channels),
    )
    side = sides[0]
    updated = updated.reshape(tile_rows, tile_cols, side, side, channels).transpose(0, 2, 1, 3, 4)
    return updated.reshape(tile_rows * side, tile_cols * side, channels)


def solution(mesh):
    in_specs = (
        P("row", "col", None),
        P("row", "col", "head"),
        P("row", "col", "head"),
        P("row", "col", "head"),
        P("row", "col", "head"),
        P("row", "col", None, None),
        P("row", "col", "head"),
        P(None, "head"),
        P("head"),
        P(),
        P(),
        P("head"),
        P("head"),
    )
    out_specs = P("row", "col", "head")
    return jax.shard_map(on_device, mesh=mesh, in_specs=in_specs, out_specs=out_specs, check_vma=False)
```

```python
import functools
import jax
import jax.numpy as jnp
from jax import lax
from jax.experimental import pallas as pl
from jax.experimental.pallas import tpu as pltpu
from jax.sharding import PartitionSpec as P

LEVELS = 4
POINTS = 4
ANY = pl.ANY
SMEM = pltpu.SMEM
VMEM = pltpu.VMEM
SELECT_VMEM = 4 * 1024 * 1024
PREP_VMEM = 8 * 1024 * 1024
ATTEND_VMEM = 12 * 1024 * 1024
GROUPS = (2, 2)


def to_blocks(source, tile_rows, tile_cols, tile_side):
    channels = source.shape[2]
    shaped = source.reshape(tile_rows, tile_side, tile_cols, tile_side, channels)
    return shaped.transpose(0, 2, 1, 3, 4).reshape(
        tile_rows * tile_cols, tile_side * tile_side, channels
    )


def hat(position, center):
    return jnp.maximum(1.0 - jnp.abs(position - center), 0.0)


def iota(shape, dim):
    return lax.broadcasted_iota(jnp.int32, shape, dim)


def prep_kernel(
    dims,
    query_ref,
    logit_ref,
    bias_ref,
    sample_ref,
    weight0,
    weight1,
    weight2,
    down_ref,
    attend_ref,
    code_ref,
    col_ref,
    hot_ref,
):
    _, _, sizes, sides, per_block, heads, _, _ = dims
    block = pl.program_id(0)
    pixels = sizes[0]
    base2 = per_block * sizes[2]
    lanes = LEVELS * POINTS
    logits = lax.dot_general(
        query_ref[...], logit_ref[...], (((1,), (1,)), ((), ())), preferred_element_type=jnp.float32
    )
    logits = (logits + bias_ref[...]).T
    for head in range(heads):
        part = logits[head * lanes : (head + 1) * lanes, :]
        part = jnp.exp(part - jnp.max(part, axis=0, keepdims=True))
        attend_ref[head * lanes : (head + 1) * lanes, :] = part / jnp.sum(part, axis=0, keepdims=True)
    packed = sample_ref[...].T
    level_of = iota(packed.shape, 0) // POINTS % LEVELS
    slot = packed >> 24
    pos_row = (packed >> 12) & 4095
    pos_col = packed & 4095
    deep = jnp.where(level_of == 0, sides[0] * 256 // GROUPS[0], sides[1] * 256 // GROUPS[1])
    group = jnp.zeros_like(packed)
    for bound in range(1, max(GROUPS)):
        group = group + jnp.where(pos_row >= bound * deep, 1, 0)
    group = jnp.where(level_of < 2, group, 0)
    code_ref[...] = slot + group * per_block
    down_ref[0] = (pos_row - group * deep).astype(jnp.float32) * (1.0 / 256.0)
    col_ref[...] = pos_col.astype(jnp.float32) * (1.0 / 256.0)

    def line_of(head, level, point):
        row = (head * LEVELS + level) * POINTS + point
        return slice(row, row + 1)

    def hot_of(head, level, point, rows):
        line = line_of(head, level, point)
        return jnp.where(code_ref[line, :] == iota((rows, pixels), 0), attend_ref[line, :], 0.0)

    weight2[0, :, base2:, :] = jnp.zeros((heads, weight2.shape[2] - base2, pixels), jnp.bfloat16)
    for head in range(heads):
        for level in range(2):
            side = sides[level]
            weight = (weight0, weight1)[level]
            step = 16 // side
            rows = GROUPS[level] * per_block
            for point in range(POINTS):
                hot_ref[point, :rows, :] = hot_of(head, level, point, rows)
                across = hat(
                    col_ref[line_of(head, level, point), :], (iota((16, pixels), 0) % side).astype(jnp.float32)
                )
                for index in range(0, rows, step):
                    stack = [
                        jnp.broadcast_to(hot_ref[point, row : row + 1, :], (side, pixels))
                        for row in range(index, index + step)
                    ]
                    piece = stack[0] if step == 1 else jnp.concatenate(stack, axis=0)
                    piece = (piece * across).astype(jnp.bfloat16)
                    weight[0, head, point, index * side : (index + step) * side, :] = piece
        for level in (2, 3):
            side = sides[level]
            size = sizes[level]
            step = max(1, 8 // size)
            tall = size * step
            place = iota((tall, pixels), 0)
            parts = []
            for point in range(POINTS):
                line = line_of(head, level, point)
                parts.append(
                    hat(down_ref[0, line, :], (place % size // side).astype(jnp.float32))
                    * hat(col_ref[line, :], (place % side).astype(jnp.float32))
                )
                if step == 1:
                    hot_ref[point, :per_block, :] = hot_of(head, level, point, per_block)
                else:
                    line = line_of(head, level, point)
                    parts[-1] = parts[-1] * attend_ref[line, :]
                    hot_ref[point, :tall, :] = jnp.broadcast_to(
                        code_ref[line, :], (tall, pixels)
                    ).astype(jnp.float32) - (place // size).astype(jnp.float32)
            stack = []
            for index in range(0, per_block, step):
                mixed = jnp.zeros((tall, pixels), jnp.float32)
                for point in range(POINTS):
                    if step == 1:
                        mixed = mixed + hot_ref[point, index : index + 1, :] * parts[point]
                    else:
                        mixed = mixed + jnp.where(hot_ref[point, :tall, :] == float(index), parts[point], 0.0)
                stack.append(mixed)
            if level == 2:
                for index, mixed in enumerate(stack):
                    weight2[0, head, index * tall : (index + 1) * tall, :] = mixed.astype(jnp.bfloat16)
            else:
                depth = per_block * size
                first = pl.multiple_of(base2 + block * depth, depth)
                weight2[0, head, pl.ds(first, depth), :] = jnp.concatenate(stack, axis=0).astype(
                    jnp.bfloat16
                )


def load_kernel(*refs):
    count = len(refs) // 2
    sem = refs[-1]
    moves = [
        pltpu.make_async_copy(refs[number], refs[count + number], sem.at[number]) for number in range(count)
    ]
    for move in moves:
        move.start()
    for move in moves:
        move.wait()


def select_kernel(dims, ids_ref, zero_ref, one_ref, two_ref, three_ref, out_ref, sem):
    peers, capacity, sizes = dims
    refs = (zero_ref, one_ref, two_ref)

    def copies(peer, make):
        base = 0
        for level in range(LEVELS - 1):
            size = sizes[level]
            for slot in range(capacity):
                index = jnp.maximum(ids_ref[peer, level * capacity + slot], 0)
                make(refs[level].at[index], out_ref.at[peer, base : base + size, :])
                base += size
        make(three_ref, out_ref.at[peer, base : base + three_ref.shape[0], :])

    def start(peer, carry):
        copies(peer, lambda src, dst: pltpu.make_async_copy(src, dst, sem).start())
        return carry

    def finish(peer, carry):
        copies(peer, lambda src, dst: pltpu.make_async_copy(src, dst, sem).wait())
        return carry

    lax.fori_loop(0, peers, start, 0)
    lax.fori_loop(0, peers, finish, 0)


def pick(values, my_column):
    chosen = jnp.int32(values[0])
    for column in range(1, len(values)):
        chosen = jnp.where(my_column == column, values[column], chosen)
    return chosen


def relay_select_kernel(dims, order, table_ref, *refs):
    partners, candidates, capacity, sizes, blocks = dims
    sources = refs[:candidates]
    outs = refs[candidates:]
    columns, numbers = order
    my_column = table_ref[0, 1]
    column = pick(columns, my_column)
    which = pick(numbers, my_column)
    for number, source in enumerate(sources):

        @pl.when(which == number)
        def _(source=source):
            for partner in range(partners):
                base = 0
                start = 0
                for level in range(LEVELS - 1):
                    size = sizes[level]
                    for rank in range(capacity):
                        index = jnp.maximum(
                            table_ref[1 + partner * LINE + column, level * capacity + rank], 0
                        )
                        outs[partner][base : base + size, :] = source[
                            pl.ds(pl.multiple_of(start + index * size, size), size), :
                        ]
                        base += size
                    start += blocks * size
                small = blocks * sizes[3]
                outs[partner][base : base + small, :] = source[start : start + small, :]


def gather_direct(dims, request_ref, fetched_ref, tiles, tile3, sem):
    peers, capacity, sizes, _, _, _, _, _ = dims
    small = tile3.shape[1]
    base3 = capacity * sum(sizes[:3])
    pltpu.make_async_copy(fetched_ref.at[:, base3 : base3 + small, :], tile3, sem.at[LEVELS - 1]).start()

    def start(peer, carry):
        base = 0
        for level in range(LEVELS - 1):
            size = sizes[level]
            for rank in range(capacity):
                fetch_one(
                    request_ref[peer, level * capacity + rank],
                    fetched_ref.at[peer, base : base + size, :],
                    tiles[level],
                    sem.at[level],
                )
                base += size
        return carry

    lax.fori_loop(0, peers, start, 0)
    for level in range(LEVELS - 1):
        pltpu.make_async_copy(tiles[level], tiles[level], sem.at[level]).wait()
    pltpu.make_async_copy(tile3, tile3, sem.at[LEVELS - 1]).wait()


def fetch_one(request, source, tile, sem):
    @pl.when(request >= 0)
    def _():
        pltpu.make_async_copy(source, tile.at[request], sem).start()


def gather_relay(dims, relay, table_ref, near_refs, packs_refs, tiles, tile3):
    peers, capacity, sizes, _, _, _, _, blocks = dims
    rows, columns, partner_of = relay
    small = tile3.shape[1]
    my_row = table_ref[0, 0]
    my_column = table_ref[0, 1]
    requests = 1 + (rows - 1) * columns
    asked = requests + peers

    def put(owner, level, rank, source, start):
        request = table_ref[requests + owner, level * capacity + rank]
        size = sizes[level]
        tiles[level][jnp.maximum(request, 0)] = source[pl.ds(start, size), :]

    for name, source in zip(NEAR, near_refs, strict=True):
        held = [-1] * columns
        for buffers, owners in SLOTS:
            for column in range(columns):
                if buffers[column] == name:
                    held[column] = owners[column]
        column = pick(held, my_column)

        @pl.when(column >= 0)
        def _(source=source, column=column):
            owner = my_row * columns + column
            start = 0
            for level in range(LEVELS - 1):
                size = sizes[level]
                for rank in range(capacity):
                    index = jnp.maximum(table_ref[asked + owner, level * capacity + rank], 0)
                    put(owner, level, rank, source, pl.multiple_of(start + index * size, size))
                start += blocks * size
            tile3[owner] = source[start : start + small, :]

    for number, source in enumerate(packs_refs):
        slot, partner = divmod(number, rows - 1)
        owner = partner_of(my_row, partner + 1) * columns + pick(SLOTS[slot][1], my_column)
        base = 0
        for level in range(LEVELS - 1):
            for rank in range(capacity):
                put(owner, level, rank, source, base)
                base += sizes[level]
        tile3[owner] = source[base : base + small, :]


def attend_kernel(dims, grid, gather, count, *refs):
    sources = refs[:count]
    (
        weight0,
        weight1,
        weight2,
        down_ref,
        lists_ref,
        out_ref,
        tile0,
        tile1,
        tile2,
        tile3,
        left0,
        left1,
        left2,
        turn_ref,
        sem,
    ) = refs[count:]
    peers, capacity, sizes, sides, per_block, heads, head_dim, blocks = dims
    pixels = sizes[0]
    channels = heads * head_dim
    small = tile3.shape[1]
    base2 = per_block * sizes[2]
    side0, side1 = sides[0], sides[1]

    gather(sources, (tile0, tile1, tile2), tile3, sem)
    left0[:, side0 // GROUPS[0] * head_dim :, :] = jnp.zeros(
        (heads, head_dim, left0.shape[2]), jnp.bfloat16
    )
    flat = tile3[...].reshape(peers * small, channels)
    size3 = sizes[3]
    wide = blocks * per_block * size3
    lane = iota((1, wide), 1)
    target = lane % size3
    tile_rows, tile_cols, grid_cols, col_count, capacity = grid
    for request in range(blocks * per_block):
        block, entry = divmod(request, per_block)
        tile = lists_ref[block // tile_cols, block % tile_cols, LEVELS - 1, entry]
        tile_row = lax.div(tile, grid_cols)
        tile_col = tile - tile_row * grid_cols
        high = lax.div(tile_row, tile_rows)
        wide_col = lax.div(tile_col, tile_cols)
        owner = high * col_count + wide_col
        place = (tile_row - high * tile_rows) * tile_cols + tile_col - wide_col * tile_cols
        first = owner * small + place * size3
        target = target + jnp.where(lane // size3 == request, first, 0)
    chosen = (iota((peers * small, wide), 0) == target).astype(jnp.bfloat16)
    picked = lax.dot_general(flat, chosen, (((0,), (0,)), ((), ())), preferred_element_type=jnp.float32)
    left2[:, base2:] = picked.astype(jnp.bfloat16)

    def one(block, carry):
        mine = pl.ds(block * per_block, per_block)
        reach0 = side0 // GROUPS[0]
        for line in range(side0):
            piece = tile0[mine, line * side0 : (line + 1) * side0, :]
            turned = piece.reshape(per_block * side0, channels).T
            for group in range(GROUPS[0]):
                offset = line - group * reach0
                if 0 <= offset <= reach0:
                    for head in range(heads):
                        left0[
                            head,
                            offset * head_dim : (offset + 1) * head_dim,
                            group * per_block * side0 : (group + 1) * per_block * side0,
                        ] = turned[head * head_dim : (head + 1) * head_dim, :]
        wide1 = tile1[mine].astype(jnp.float32)
        reach1 = side1 // GROUPS[1]
        for offset in range(reach1 + 1):
            stack = []
            for group in range(GROUPS[1]):
                line = min(group * reach1 + offset, side1 - 1)
                stack.append(
                    wide1[:, line * side1 : (line + 1) * side1, :].reshape(per_block * side1, channels)
                )
            turned = jnp.concatenate(stack, axis=0).astype(jnp.bfloat16).T
            for head in range(heads):
                left1[head, offset * head_dim : (offset + 1) * head_dim, :] = turned[
                    head * head_dim : (head + 1) * head_dim, :
                ]
        left2[:, :base2] = tile2[mine].reshape(per_block * sizes[2], channels).T

        def per_head(head, carry):
            rows = pl.ds(head * head_dim, head_dim)
            total = jnp.dot(left2[rows, :], weight2[block, head], preferred_element_type=jnp.float32)
            for level in range(2):
                left = (left0, left1)[level]
                weight = (weight0, weight1)[level]
                for point in range(POINTS):
                    row = (head * LEVELS + level) * POINTS + point
                    product = jnp.dot(left[head], weight[block, head, point], preferred_element_type=jnp.float32)
                    down = down_ref[block, pl.ds(row, 1), :]
                    for offset in range(sides[level] // GROUPS[level] + 1):
                        total = total + product[offset * head_dim : (offset + 1) * head_dim, :] * hat(
                            down, float(offset)
                        )
            turn_ref[rows, :] = total
            return carry

        for head in range(heads):
            per_head(head, 0)
        out_ref[pl.ds(pl.multiple_of(block * pixels, pixels), pixels), :] = turn_ref[...].T.astype(jnp.bfloat16)
        return carry

    lax.fori_loop(0, blocks, one, 0)


def own_kernel(head_ref, query_ref, own_ref, weight_ref, bias_ref, out_ref):
    channels = own_ref.shape[1]
    rows = weight_ref[pl.ds(pl.multiple_of(head_ref[0] * channels, channels), channels), :]
    pre = query_ref[...].astype(jnp.float32) + bias_ref[...]
    out_ref[...] = pre + jnp.dot(own_ref[...], rows, preferred_element_type=jnp.float32)


def norm_kernel(head_ref, pre_ref, other_ref, weight_ref, gain_ref, shift_ref, out_ref):
    own_head = head_ref[0]
    pixels, channels = out_ref.shape
    here = pl.ds(pl.multiple_of(pl.program_id(0) * pixels, pixels), pixels)
    rows = weight_ref[pl.ds(pl.multiple_of((1 - own_head) * channels, channels), channels), :]
    pre = pre_ref[here, :] + jnp.dot(other_ref[here, :], rows, preferred_element_type=jnp.float32)
    centered = pre - jnp.mean(pre, axis=1, keepdims=True)
    variance = jnp.mean(centered * centered, axis=1, keepdims=True)
    own = jnp.where(own_head == 0, centered[:, :channels], centered[:, channels:])
    out_ref[...] = (own * lax.rsqrt(variance + 1e-05) * gain_ref[...] + shift_ref[...]).astype(jnp.bfloat16)


def tables(lists, grid):
    tile_rows, tile_cols, grid_cols, col_count, _ = grid
    _, blocks, _, per_block = lists.shape
    requests = blocks * per_block
    wanted = jnp.concatenate([lists[:, block] for block in range(blocks)], axis=2)
    grid_row = wanted // grid_cols
    grid_col = wanted % grid_cols
    owner = grid_row // tile_rows * col_count + grid_col // tile_cols
    local = grid_row % tile_rows * tile_cols + grid_col % tile_cols
    order = jnp.arange(requests, dtype=jnp.int32)
    earlier = (owner[..., :, None] == owner[..., None, :]) & (order[None, :] < order[:, None])
    rank = jnp.sum(earlier.astype(jnp.int32), axis=3)
    return owner, local, rank


def entries(owner, rank, owners, capacity, value):
    slot = jnp.arange(capacity, dtype=jnp.int32)
    hit = (owner[:, None, :, None, :] == owners[None, :, None, None, None]) & (
        rank[:, None, :, None, :] == slot[None, None, None, :, None]
    )
    found = jnp.sum(jnp.where(hit, 1 + value[:, None, :, None, :], 0), axis=4) - 1
    return found.reshape(owner.shape[0], owners.shape[0], -1)


LINE = 4
SELECT_COST = pl.CostEstimate(flops=500_000_000, bytes_accessed=1_000_000, transcendentals=0)
PREP_COST = pl.CostEstimate(flops=2_000_000_000, bytes_accessed=4_000_000, transcendentals=0)
STEPS = (
    ("first", None, ((0, 1), (1, 0), (2, 3), (3, 2))),
    ("cross", None, ((1, 2), (2, 1))),
    ("out", "cross", ((1, 0), (2, 3))),
    ("over", "first", ((1, 2), (2, 1))),
    ("last", "over", ((1, 0), (2, 3))),
)
NEAR = ("own", "first", "cross", "out", "over", "last")
SLOTS = (
    (("own",) * 4, (0, 1, 2, 3)),
    (("first",) * 4, (1, 0, 3, 2)),
    (("out", "cross", "cross", "out"), (2, 2, 1, 1)),
    (("last", "over", "over", "last"), (3, 3, 0, 0)),
)


def relay_tiles(dims, row_count, col_count, pack, flat_sets, lists, grid):
    peers, capacity, sizes, _, per_block, heads, head_dim, blocks = dims
    channels = heads * head_dim
    my_row = lax.axis_index("row")
    my_column = lax.axis_index("col")
    power = row_count & (row_count - 1) == 0

    def partner_of(row, number):
        return row ^ number if power else (row + number) % row_count

    def source_of(row, number):
        return row ^ number if power else (row + row_count - number) % row_count

    held = {"own": jnp.concatenate(flat_sets, axis=0)}

    def move(name):
        source, pairs = {step[0]: step[1:] for step in STEPS}[name]
        held[name] = lax.ppermute(held[source or "own"], "col", pairs)

    move("first")
    move("cross")
    owner, local, rank = tables(lists.reshape(1, blocks, LEVELS, per_block), grid)
    order = jnp.arange(blocks * per_block, dtype=jnp.int32)
    code = entries(owner, rank, jnp.arange(peers, dtype=jnp.int32), capacity, order * blocks + local)[0]
    asked = jnp.where(code >= 0, code % blocks, -1)
    request = jnp.where(code >= 0, code // blocks, -1)
    by_row = asked.reshape(row_count, col_count, asked.shape[1])
    ids = []
    for number in range(1, row_count):
        mine = jnp.sum(
            jnp.where(
                (jnp.arange(row_count) == partner_of(my_row, number))[:, None, None], by_row, 0
            ),
            axis=0,
        )
        ids.append(
            lax.ppermute(mine, "row", [(row, partner_of(row, number)) for row in range(row_count)])
        )

    width = asked.shape[1]
    lane = jnp.arange(width)[None, :]
    place = jnp.where(lane == 0, my_row, my_column).astype(jnp.int32)
    table = jnp.concatenate([place, *ids, request, asked], axis=0)
    packs = []
    for slot, (buffers, columns) in enumerate(SLOTS):
        if slot == 1:
            move("out")
            move("over")
        if slot == 2:
            move("last")
        names = sorted(set(buffers))
        numbers = [names.index(name) for name in buffers]
        sent = pl.pallas_call(
            functools.partial(
                relay_select_kernel, (row_count - 1, len(names), capacity, sizes, blocks), (columns, numbers)
            ),
            out_shape=[jax.ShapeDtypeStruct((pack, channels), jnp.bfloat16)] * (row_count - 1),
            in_specs=[pl.BlockSpec(memory_space=SMEM)] + [pl.BlockSpec(memory_space=VMEM)] * len(names),
            out_specs=[pl.BlockSpec(memory_space=VMEM)] * (row_count - 1),
            compiler_params=pltpu.CompilerParams(vmem_limit_bytes=SELECT_VMEM),
            cost_estimate=SELECT_COST,
        )(table, *[held[name] for name in names])
        for number in range(1, row_count):
            packs.append(
                lax.ppermute(
                    sent[number - 1], "row", [(row, source_of(row, number)) for row in range(row_count)]
                )
            )

    near = [held[name] for name in NEAR]
    sources = (table, *near, *packs)
    spaces = (SMEM,) + (VMEM,) * (len(near) + len(packs))

    def gather(refs, tiles, tile3, sem):
        gather_relay(
            dims,
            (row_count, col_count, partner_of),
            refs[0],
            refs[1 : 1 + len(near)],
            refs[1 + len(near) :],
            tiles,
            tile3,
        )

    return gather, sources, spaces


def direct_tiles(dims, pack, tile_sets, flat_sets, lists, grid):
    peers, capacity, sizes, _, per_block, heads, head_dim, blocks = dims
    channels = heads * head_dim
    owner, local, rank = tables(lists.reshape(1, blocks, LEVELS, per_block), grid)
    owners = jnp.arange(peers, dtype=jnp.int32)
    order = jnp.broadcast_to(jnp.arange(blocks * per_block, dtype=jnp.int32), owner.shape)
    asked = entries(owner, rank, owners, capacity, local)[0]
    request = entries(owner, rank, owners, capacity, order)[0]
    received = lax.all_to_all(asked, ("row", "col"), split_axis=0, concat_axis=0, tiled=True)
    packs = pl.pallas_call(
        functools.partial(select_kernel, (peers, capacity, sizes)),
        out_shape=jax.ShapeDtypeStruct((peers, pack, channels), jnp.bfloat16),
        in_specs=[pl.BlockSpec(memory_space=SMEM)] + [pl.BlockSpec(memory_space=VMEM)] * 4,
        out_specs=pl.BlockSpec(memory_space=ANY),
        scratch_shapes=[pltpu.SemaphoreType.DMA],
        name="select",
    )(received, tile_sets[0], tile_sets[1], tile_sets[2], flat_sets[3])
    fetched = lax.all_to_all(packs, ("row", "col"), split_axis=0, concat_axis=0, tiled=True)

    def gather(refs, tiles, tile3, sem):
        gather_direct(dims, refs[0], refs[1], tiles, tile3, sem)

    return gather, (request, fetched), (SMEM, ANY)


def on_device(
    queries,
    level_zero,
    level_one,
    level_two,
    level_three,
    tile_lists,
    samples,
    logit_weight,
    logit_bias,
    output_weight,
    output_bias,
    norm_gain,
    norm_shift,
):
    level_blocks = (level_zero, level_one, level_two, level_three)
    row_count = lax.axis_size("row")
    col_count = lax.axis_size("col")
    peers = row_count * col_count
    tile_rows, tile_cols, level_count, per_block = tile_lists.shape
    blocks = tile_rows * tile_cols
    requests = blocks * per_block
    capacity = max(2, (requests + peers - 1) // peers)
    grid_cols = tile_cols * col_count
    channels = level_zero.shape[2]
    width_all = queries.shape[2]
    lanes = samples.shape[2]
    heads = lanes // (LEVELS * POINTS)
    head_dim = channels // heads
    sides = tuple(block.shape[0] // tile_rows for block in level_blocks)
    sizes = tuple(side * side for side in sides)
    pixels = sizes[0]
    tile_sets = [
        to_blocks(level_blocks[level], tile_rows, tile_cols, sides[level]) for level in range(level_count)
    ]

    small = blocks * sizes[3]
    pack = capacity * sum(sizes[:3]) + small
    dims = (peers, capacity, sizes, sides, per_block, heads, head_dim, blocks)
    grid = (tile_rows, tile_cols, grid_cols, col_count, capacity)
    flat_sets = [
        tile_sets[level].reshape(blocks * sizes[level], channels) for level in range(level_count)
    ]
    if peers * capacity <= requests and col_count == LINE:
        gather, sources, spaces = relay_tiles(
            dims, row_count, col_count, pack, flat_sets, tile_lists, grid
        )
    else:
        gather, sources, spaces = direct_tiles(
            dims, pack, tile_sets, flat_sets, tile_lists, grid
        )

    queries_blocked = to_blocks(queries, tile_rows, tile_cols, sides[0]).reshape(blocks * pixels, width_all)
    samples_blocked = to_blocks(samples, tile_rows, tile_cols, sides[0]).reshape(blocks * pixels, lanes)
    depth0 = GROUPS[0] * per_block * sides[0]
    depth1 = GROUPS[1] * per_block * sides[1]
    depth2 = per_block * sizes[2] + requests * sizes[3]
    whole = pl.BlockSpec(memory_space=VMEM)
    staged = (queries_blocked, samples_blocked, logit_weight.T)
    queries_blocked, samples_blocked, logit_turned = pl.pallas_call(
        load_kernel,
        out_shape=[jax.ShapeDtypeStruct(array.shape, array.dtype) for array in staged],
        in_specs=[pl.BlockSpec(memory_space=ANY)] * len(staged),
        out_specs=[whole] * len(staged),
        scratch_shapes=[pltpu.SemaphoreType.DMA((len(staged),))],
        compiler_params=pltpu.CompilerParams(vmem_limit_bytes=SELECT_VMEM),
        name="load",
    )(*staged)
    weights = pl.pallas_call(
        functools.partial(prep_kernel, dims),
        out_shape=[
            jax.ShapeDtypeStruct((blocks, heads, POINTS, depth0, pixels), jnp.bfloat16),
            jax.ShapeDtypeStruct((blocks, heads, POINTS, depth1, pixels), jnp.bfloat16),
            jax.ShapeDtypeStruct((blocks, heads, depth2, pixels), jnp.bfloat16),
            jax.ShapeDtypeStruct((blocks, lanes, pixels), jnp.float32),
        ],
        grid=(blocks,),
        in_specs=[
            pl.BlockSpec((pixels, width_all), lambda i: (i, 0)),
            pl.BlockSpec((lanes, width_all), lambda i: (0, 0)),
            pl.BlockSpec((1, lanes), lambda i: (0, 0)),
            pl.BlockSpec((pixels, lanes), lambda i: (i, 0)),
        ],
        out_specs=[
            pl.BlockSpec((1, heads, POINTS, depth0, pixels), lambda i: (i, 0, 0, 0, 0)),
            pl.BlockSpec((1, heads, POINTS, depth1, pixels), lambda i: (i, 0, 0, 0, 0)),
            pl.BlockSpec((1, heads, depth2, pixels), lambda i: (i, 0, 0, 0)),
            pl.BlockSpec((1, lanes, pixels), lambda i: (i, 0, 0)),
        ],
        scratch_shapes=[
            VMEM((lanes, pixels), jnp.float32),
            VMEM((lanes, pixels), jnp.int32),
            VMEM((lanes, pixels), jnp.float32),
            VMEM((POINTS, max(GROUPS) * per_block, pixels), jnp.float32),
        ],
        compiler_params=pltpu.CompilerParams(vmem_limit_bytes=PREP_VMEM),
        cost_estimate=PREP_COST,
        name="prep",
    )(queries_blocked, logit_turned, logit_bias.reshape(1, lanes), samples_blocked)

    attn = pl.pallas_call(
        functools.partial(attend_kernel, dims, grid, gather, len(sources)),
        out_shape=jax.ShapeDtypeStruct((blocks * pixels, channels), jnp.bfloat16),
        in_specs=[pl.BlockSpec(memory_space=space) for space in spaces]
        + [whole] * 4
        + [pl.BlockSpec(memory_space=SMEM)],
        out_specs=whole,
        scratch_shapes=[
            VMEM((requests, sizes[0], channels), jnp.bfloat16),
            VMEM((requests, sizes[1], channels), jnp.bfloat16),
            VMEM((requests, sizes[2], channels), jnp.bfloat16),
            VMEM((peers, small, channels), jnp.bfloat16),
            VMEM((heads, (sides[0] // GROUPS[0] + 1) * head_dim, depth0), jnp.bfloat16),
            VMEM((heads, (sides[1] // GROUPS[1] + 1) * head_dim, depth1), jnp.bfloat16),
            VMEM((channels, depth2), jnp.bfloat16),
            VMEM((channels, pixels), jnp.float32),
            pltpu.SemaphoreType.DMA((LEVELS,)),
        ],
        compiler_params=pltpu.CompilerParams(vmem_limit_bytes=ATTEND_VMEM),
        cost_estimate=PREP_COST,
        name="attend",
    )(*sources, *weights, tile_lists)

    own_head = lax.axis_index("head").reshape(1).astype(jnp.int32)
    other = lax.ppermute(attn, "head", [(0, 1), (1, 0)])
    wide_spec = pl.BlockSpec((pixels, width_all), lambda i: (i, 0))
    slim_spec = pl.BlockSpec((pixels, channels), lambda i: (i, 0))
    matrix_spec = pl.BlockSpec((width_all, width_all), lambda i: (0, 0))
    pre = pl.pallas_call(
        own_kernel,
        out_shape=jax.ShapeDtypeStruct((blocks * pixels, width_all), jnp.float32),
        grid=(blocks,),
        in_specs=[
            pl.BlockSpec(memory_space=SMEM),
            wide_spec,
            slim_spec,
            matrix_spec,
            pl.BlockSpec((1, width_all), lambda i: (0, 0)),
        ],
        out_specs=wide_spec,
        compiler_params=pltpu.CompilerParams(vmem_limit_bytes=SELECT_VMEM),
        name="own",
    )(own_head, queries_blocked, attn, output_weight, output_bias.reshape(1, width_all))
    merged = 2 if blocks % 2 == 0 else 1
    updated = pl.pallas_call(
        norm_kernel,
        out_shape=jax.ShapeDtypeStruct((blocks * pixels, channels), jnp.bfloat16),
        grid=(blocks // merged,),
        in_specs=[pl.BlockSpec(memory_space=SMEM)] + [whole] * 5,
        out_specs=pl.BlockSpec((merged * pixels, channels), lambda i: (i, 0)),
        compiler_params=pltpu.CompilerParams(vmem_limit_bytes=SELECT_VMEM),
        name="norm",
    )(
        own_head,
        pre,
        other,
        output_weight,
        norm_gain.reshape(1, channels),
        norm_shift.reshape(1, channels),
    )
    side = sides[0]
    updated = updated.reshape(tile_rows, tile_cols, side, side, channels).transpose(0, 2, 1, 3, 4)
    return updated.reshape(tile_rows * side, tile_cols * side, channels)


def solution(mesh):
    in_specs = (
        P("row", "col", None),
        P("row", "col", "head"),
        P("row", "col", "head"),
        P("row", "col", "head"),
        P("row", "col", "head"),
        P("row", "col", None, None),
        P("row", "col", "head"),
        P(None, "head"),
        P("head"),
        P(),
        P(),
        P("head"),
        P("head"),
    )
    out_specs = P("row", "col", "head")
    return jax.shard_map(on_device, mesh=mesh, in_specs=in_specs, out_specs=out_specs, check_vma=False)
```
